16 devices in a mesh: sp: 16 (over z, y, x, core).
Axes of the slice: x: 2, y: 2, z: 2, core: 2. Of those that a mesh axis runs over, the one named last changes fastest.
Arguments:
- hidden: bfloat16 [64, 512, 2048], P(None, 'sp')
- norm_gain: bfloat16 [2048], replicated
- w_qkv: bfloat16 [2048, 6144], replicated
- w_out: bfloat16 [2048, 2048], replicated
- cos_tab: float32 [512, 64], P('sp')
- sin_tab: float32 [512, 64], P('sp')
- d_out: bfloat16 [64, 512, 2048], P(None, 'sp')
Outputs:
- output 1: bfloat16 [64, 512, 2048], P(None, 'sp')
- output 2: bfloat16 [64, 512, 2048], P(None, 'sp')
- output 3: float32 [2048, 6144], replicated
- output 4: float32 [2048, 2048], replicated
- output 5: float32 [2048], replicated
All inputs are finite; a program needn't handle non-finite values.
Results may differ from the reference program's by a relative error of at most 0.011258.
Values are sent between devices in bfloat16 or wider.
A program may use at most 1 GiB of HBM per device.

```python
import jax
import jax.numpy as jnp
from jax import lax

MODEL_DIM = 2048
NUM_HEADS = 16
HEAD_DIM = 128
BATCH_SEQS = 64
SEQ_LEN = 512

NORM_EPS = 1e-6
ROPE_BASE = 10000.0
SCORE_SCALE = HEAD_DIM ** -0.5


def setup_inputs(seed: int = 0) -> dict:
    subkeys = jax.random.split(jax.random.key(seed), 8)
    act_shape = (BATCH_SEQS, SEQ_LEN, MODEL_DIM)
    weight_scale = MODEL_DIM ** -0.5
    hidden = jax.random.normal(subkeys[0], act_shape, jnp.float32).astype(jnp.bfloat16)
    norm_gain = (1.5 + 0.3 * jax.random.normal(subkeys[1], (MODEL_DIM,), jnp.float32)).astype(jnp.bfloat16)
    w_qkv = (jax.random.normal(subkeys[2], (MODEL_DIM, 3 * MODEL_DIM), jnp.float32) * weight_scale).astype(jnp.bfloat16)
    w_out = (jax.random.normal(subkeys[3], (MODEL_DIM, MODEL_DIM), jnp.float32) * weight_scale).astype(jnp.bfloat16)
    half_dim = HEAD_DIM // 2
    base_freq = ROPE_BASE ** (-jnp.arange(half_dim, dtype=jnp.float32) / half_dim)
    jitter = jax.random.uniform(subkeys[4], (half_dim,), jnp.float32, 0.5, 1.5)
    angles = jnp.arange(SEQ_LEN, dtype=jnp.float32)[:, None] * (base_freq * jitter)[None, :]
    d_out = jax.random.normal(subkeys[5], act_shape, jnp.float32).astype(jnp.bfloat16)
    return {'hidden': hidden, 'norm_gain': norm_gain, 'w_qkv': w_qkv, 'w_out': w_out, 'cos_tab': jnp.cos(angles), 'sin_tab': jnp.sin(angles), 'd_out': d_out}


def rotate_half(head_vecs):
    half_dim = head_vecs.shape[-1] // 2
    return jnp.concatenate([-head_vecs[..., half_dim:], head_vecs[..., :half_dim]], axis=-1)


def head_attention(operands):
    q_head, k_head, v_head = operands
    scores = jnp.einsum('bqd,bkd->bqk', q_head.astype(jnp.float32), k_head.astype(jnp.float32)) * SCORE_SCALE
    positions = jnp.arange(SEQ_LEN)
    causal = positions[:, None] >= positions[None, :]
    scores = jnp.where(causal[None], scores, -1e30)
    probs_bf = jax.nn.softmax(scores, axis=-1).astype(jnp.bfloat16)
    return jnp.einsum('bqk,bkd->bqd', probs_bf.astype(jnp.float32), v_head.astype(jnp.float32)).astype(jnp.bfloat16)


def block_forward(hidden, gain_f32, w_qkv_f32, w_out_f32, cos_tab, sin_tab):
    hidden_f32 = hidden.astype(jnp.float32)
    inv_rms = lax.rsqrt(jnp.mean(hidden_f32 * hidden_f32, axis=-1, keepdims=True) + NORM_EPS)
    normed = (hidden_f32 * inv_rms * gain_f32).astype(jnp.bfloat16)
    flat_rows = BATCH_SEQS * SEQ_LEN
    projected = jnp.dot(normed.reshape(flat_rows, MODEL_DIM).astype(jnp.float32), w_qkv_f32)
    projected = projected.reshape(BATCH_SEQS, SEQ_LEN, 3, NUM_HEADS, HEAD_DIM)
    cos_full = jnp.concatenate([cos_tab, cos_tab], axis=-1)[:, None, :]
    sin_full = jnp.concatenate([sin_tab, sin_tab], axis=-1)[:, None, :]
    q_rot = projected[:, :, 0] * cos_full + rotate_half(projected[:, :, 0]) * sin_full
    k_rot = projected[:, :, 1] * cos_full + rotate_half(projected[:, :, 1]) * sin_full
    by_head = (jnp.transpose(q_rot.astype(jnp.bfloat16), (2, 0, 1, 3)), jnp.transpose(k_rot.astype(jnp.bfloat16), (2, 0, 1, 3)), jnp.transpose(projected[:, :, 2].astype(jnp.bfloat16), (2, 0, 1, 3)))
    attn_heads = lax.map(jax.checkpoint(head_attention), by_head)
    attn_flat = jnp.transpose(attn_heads, (1, 2, 0, 3)).reshape(flat_rows, MODEL_DIM)
    out_proj = jnp.dot(attn_flat.astype(jnp.float32), w_out_f32).reshape(BATCH_SEQS, SEQ_LEN, MODEL_DIM)
    return (hidden_f32 + out_proj).astype(jnp.bfloat16)


def reference(hidden, norm_gain, w_qkv, w_out, cos_tab, sin_tab, d_out):
    def forward_fn(hidden_in, gain_f32, w_qkv_f32, w_out_f32):
        return block_forward(hidden_in, gain_f32, w_qkv_f32, w_out_f32, cos_tab, sin_tab)
    y_out, pullback = jax.vjp(forward_fn, hidden, norm_gain.astype(jnp.float32), w_qkv.astype(jnp.float32), w_out.astype(jnp.float32))
    d_hidden, d_gain, dw_qkv, dw_out = pullback(d_out)
    return (y_out, d_hidden, dw_qkv, dw_out, d_gain)
```

```python
import functools
import jax
import jax.numpy as jnp
from jax import lax
from jax.experimental import pallas as pl
from jax.experimental.pallas import tpu as pltpu
from jax.sharding import PartitionSpec as P

NORM_EPS = 1e-6
BF = jnp.bfloat16
F32 = jnp.float32
VMEM_LIMIT = 60 * 1024 * 1024


def dot_nn(a, b):
    return lax.dot_general(a, b, (((1,), (0,)), ((), ())), preferred_element_type=F32)


def dot_nt(a, b):
    return lax.dot_general(a, b, (((1,), (1,)), ((), ())), preferred_element_type=F32)


def rotate(u, cos, sin_signed):
    return u * cos + pltpu.roll(u, 64, 1) * sin_signed


def unrotate(u, cos, sin_signed):
    return u * cos - pltpu.roll(u, 64, 1) * sin_signed


def qkv_kernel(n_rot, n_tile, hidden_ref, gain_ref, w_ref, cos_ref, sin_ref, normed_t_ref, qkv_ref, normed_ref):
    n = pl.program_id(1)

    @pl.when(n == 0)
    def _():
        h = hidden_ref[...].astype(F32)
        inv = lax.rsqrt(jnp.mean(h * h, axis=-1, keepdims=True) + NORM_EPS)
        normed = (h * inv * gain_ref[...].astype(F32)).astype(BF)
        normed_ref[...] = normed
        normed_t_ref[...] = normed.T

    proj = dot_nn(normed_ref[...], w_ref[...])

    @pl.when(n < n_rot)
    def _():
        for h in range(n_tile // 128):
            cols = slice(h * 128, (h + 1) * 128)
            qkv_ref[0, :, cols] = rotate(proj[:, cols], cos_ref[...], sin_ref[...]).astype(BF)

    @pl.when(n >= n_rot)
    def _():
        qkv_ref[0] = proj.astype(BF)


def qkv_call(hidden, gain, w_qkv, cos, sin):
    rows, dim = hidden.shape
    seq = cos.shape[0]
    tile = 512
    per = dim // tile
    return pl.pallas_call(
        functools.partial(qkv_kernel, 2 * per, tile),
        grid=(rows // seq, 3 * per),
        in_specs=[
            pl.BlockSpec((seq, dim), lambda s, n: (s, 0)),
            pl.BlockSpec((1, dim), lambda s, n: (0, 0)),
            pl.BlockSpec((dim, tile), lambda s, n: (0, n)),
            pl.BlockSpec((seq, 128), lambda s, n: (0, 0)),
            pl.BlockSpec((seq, 128), lambda s, n: (0, 0)),
        ],
        out_specs=[
            pl.BlockSpec((dim, seq), lambda s, n: (0, s)),
            pl.BlockSpec((1, seq, tile), lambda s, n: (n // per, s, n % per)),
        ],
        out_shape=[
            jax.ShapeDtypeStruct((dim, rows), BF),
            jax.ShapeDtypeStruct((3, rows, dim), BF),
        ],
        scratch_shapes=[pltpu.VMEM((seq, dim), BF)],
        compiler_params=pltpu.CompilerParams(vmem_limit_bytes=VMEM_LIMIT),
        cost_estimate=pl.CostEstimate(flops=2 * rows * dim * 3 * dim, bytes_accessed=rows * dim * 10 + 6 * dim * dim, transcendentals=0),
        name="qkv",
    )(hidden, gain, w_qkv, cos, sin)


def nt_kernel(a_ref, b_ref, o_ref):
    o_ref[...] = dot_nt(a_ref[...], b_ref[...]).astype(BF)


def nt_call(a, b):
    rows, k = a.shape
    n = b.shape[0]
    tm, tn = 1024, 512
    return pl.pallas_call(
        nt_kernel,
        grid=(rows // tm, n // tn),
        in_specs=[pl.BlockSpec((tm, k), lambda i, j: (i, 0)), pl.BlockSpec((tn, k), lambda i, j: (j, 0))],
        out_specs=pl.BlockSpec((tm, tn), lambda i, j: (i, j)),
        out_shape=jax.ShapeDtypeStruct((rows, n), BF),
        compiler_params=pltpu.CompilerParams(vmem_limit_bytes=VMEM_LIMIT),
        cost_estimate=pl.CostEstimate(flops=2 * rows * n * k, bytes_accessed=2 * (rows * k + n * k + rows * n), transcendentals=0),
        name="d_attn",
    )(a, b)


def out_kernel(a_ref, b_ref, h_ref, o_ref):
    o_ref[...] = (h_ref[...].astype(F32) + dot_nn(a_ref[...], b_ref[...])).astype(BF)


def out_call(a, b, h):
    rows, k = a.shape
    n = b.shape[1]
    tm, tn = 1024, 512
    return pl.pallas_call(
        out_kernel,
        grid=(rows // tm, n // tn),
        in_specs=[
            pl.BlockSpec((tm, k), lambda i, j: (i, 0)),
            pl.BlockSpec((k, tn), lambda i, j: (0, j)),
            pl.BlockSpec((tm, tn), lambda i, j: (i, j)),
        ],
        out_specs=pl.BlockSpec((tm, tn), lambda i, j: (i, j)),
        out_shape=jax.ShapeDtypeStruct((rows, n), BF),
        compiler_params=pltpu.CompilerParams(vmem_limit_bytes=VMEM_LIMIT),
        cost_estimate=pl.CostEstimate(flops=2 * rows * n * k, bytes_accessed=2 * (rows * k + n * k + 2 * rows * n), transcendentals=0),
        name="out_proj",
    )(a, b, h)


def attn_kernel(heads, scale, qkv_ref, do_ref, cos_ref, sin_ref, o_ref, o_t_ref, dproj_ref):
    seq = qkv_ref.shape[1]
    blk = 256
    cos = cos_ref[...]
    sin = sin_ref[...]
    for h in range(heads):
        cols = slice(h * 128, (h + 1) * 128)
        q = qkv_ref[0, :, cols]
        k = qkv_ref[1, :, cols]
        v = qkv_ref[2, :, cols]
        do = do_ref[:, cols]
        k_t = k.T
        v_t = v.T
        dk = [None] * (seq // blk)
        dv = [None] * (seq // blk)
        dq_t = []
        o_t = []
        for j in range(seq // blk):
            end = (j + 1) * blk
            q_j = q[j * blk:end]
            do_j = do[j * blk:end]
            s = dot_nt(k[:end], q_j)
            row = lax.broadcasted_iota(jnp.int32, (end, blk), 0)
            col = lax.broadcasted_iota(jnp.int32, (end, blk), 1) + j * blk
            s = jnp.where(row <= col, s * scale, -1e30)
            m = jnp.max(s, axis=0, keepdims=True)
            e = jnp.exp(s - m)
            p = e * (1.0 / jnp.sum(e, axis=0, keepdims=True))
            p_bf = p.astype(BF)
            o_t.append(dot_nn(v_t[:, :end], p_bf))
            dp = dot_nt(v[:end], do_j).astype(BF).astype(F32)
            delta = jnp.sum(p * dp, axis=0, keepdims=True)
            ds = (p * (dp - delta) * scale).astype(BF)
            dv_j = dot_nn(p_bf, do_j)
            dk_j = dot_nn(ds, q_j)
            dq_t.append(dot_nn(k_t[:, :end], ds))
            for i in range(j + 1):
                part = slice(i * blk, (i + 1) * blk)
                dv[i] = dv_j[part] if dv[i] is None else dv[i] + dv_j[part]
                dk[i] = dk_j[part] if dk[i] is None else dk[i] + dk_j[part]
        for j in range(seq // blk):
            rows = slice(j * blk, (j + 1) * blk)
            o_ref[rows, cols] = o_t[j].T.astype(BF)
            o_t_ref[cols, rows] = o_t[j].astype(BF)
            dq_j = dq_t[j].T.astype(BF).astype(F32)
            dk_j = dk[j].astype(BF).astype(F32)
            dproj_ref[0, rows, cols] = unrotate(dq_j, cos[rows], sin[rows]).astype(BF)
            dproj_ref[1, rows, cols] = unrotate(dk_j, cos[rows], sin[rows]).astype(BF)
            dproj_ref[2, rows, cols] = dv[j].astype(BF)


def attn_call(qkv, d_attn, cos, sin):
    _, rows, dim = qkv.shape
    seq = cos.shape[0]
    heads = 2
    width = heads * 128
    return pl.pallas_call(
        functools.partial(attn_kernel, heads, 128 ** -0.5),
        grid=(rows // seq, dim // width),
        in_specs=[
            pl.BlockSpec((3, seq, width), lambda s, h: (0, s, h)),
            pl.BlockSpec((seq, width), lambda s, h: (s, h)),
            pl.BlockSpec((seq, 128), lambda s, h: (0, 0)),
            pl.BlockSpec((seq, 128), lambda s, h: (0, 0)),
        ],
        out_specs=[
            pl.BlockSpec((seq, width), lambda s, h: (s, h)),
            pl.BlockSpec((width, seq), lambda s, h: (h, s)),
            pl.BlockSpec((3, seq, width), lambda s, h: (0, s, h)),
        ],
        out_shape=[
            jax.ShapeDtypeStruct((rows, dim), BF),
            jax.ShapeDtypeStruct((dim, rows), BF),
            jax.ShapeDtypeStruct((3, rows, dim), BF),
        ],
        compiler_params=pltpu.CompilerParams(vmem_limit_bytes=VMEM_LIMIT),
        cost_estimate=pl.CostEstimate(flops=12 * rows * dim * seq, bytes_accessed=rows * dim * 16, transcendentals=rows * seq * 16),
        name="attention",
    )(qkv, d_attn, cos, sin)


MESH=pl.DeviceIdType.MESH
TW=256
PARTS=((0,384),(384,320),(704,320))
NS=3
NB=8

def reduce_kernel(n_qkv, n_all, at_hbm, ot_hbm, dproj_hbm, dout_hbm, g_hbm,
                  lhs, rhs, acc, r0, r1, r2, r3,
                  ld_sem, rhs_sem, s_send, s_recv, credit, loc_sem, g_send, g_recv):
    me=lax.axis_index('sp')
    dim=at_hbm.shape[0]
    core=me%2
    mate=me+1-2*core
    recv=(r0,r1,r2,r3)

    def link(d):
        w=2+d+d*d
        bit=(me//w)%2
        return bit, me+w*(1-2*bit)

    barrier=pltpu.get_barrier_semaphore()
    for p in (mate,link(0)[1],link(1)[1],link(2)[1]):
        pl.semaphore_signal(barrier,inc=1,device_id=(p,),device_id_type=MESH)
    pl.semaphore_wait(barrier,4)

    def dims(u,p,t):
        return (u+p+t-1)%3

    def offs(u,p,size):
        o=[0]
        for t in (1,2,3):
            b,_=link(dims(u,p,t))
            o.append(o[-1]+b*(size>>t))
        return o

    def half_rows(t):
        return (dim//2)>>t

    def rs_copies(u,t):
        sl=u%NS; nb=u%NB
        if t==0:
            return [pltpu.make_async_remote_copy(
                src_ref=acc.at[nb,pl.ds(pl.multiple_of((1-core)*(dim//2),dim//2),dim//2)],
                dst_ref=r0.at[sl],send_sem=s_send.at[0,sl],recv_sem=s_recv.at[0,sl],device_id=(mate,),device_id_type=MESH)]
        out=[]
        for p,(base,size) in enumerate(PARTS):
            o=offs(u,p,size)
            n=size>>t
            b,peer=link(dims(u,p,t))
            row=core*(dim//2)+base+o[t-1]+(1-b)*n
            out.append(pltpu.make_async_remote_copy(
                src_ref=acc.at[nb,pl.ds(pl.multiple_of(row,8),n)],
                dst_ref=recv[t].at[sl,pl.ds(base>>t,n)],
                send_sem=s_send.at[t,sl],recv_sem=s_recv.at[t,sl],device_id=(peer,),device_id_type=MESH))
        return out

    def all_rows(t,u):
        sl=u%NS
        return pltpu.make_async_remote_copy(src_ref=recv[t].at[sl],dst_ref=recv[t].at[sl],
            send_sem=s_send.at[t,sl],recv_sem=s_recv.at[t,sl],device_id=(mate,),device_id_type=MESH)

    def rs_start(u,t):
        sl=u%NS
        peers=[mate] if t==0 else [link(dims(u,p,t))[1] for p in range(3)]
        @pl.when(u>=NS)
        def _():
            pl.semaphore_wait(credit.at[t,sl],len(peers))
            all_rows(t,u).wait_send()
        for c in rs_copies(u,t): c.start()

    def rs_finish(u,t):
        sl=u%NS; nb=u%NB
        all_rows(t,u).wait_recv()
        if t==0:
            rows=pl.ds(pl.multiple_of(core*(dim//2),dim//2),dim//2)
            acc[nb,rows]=acc[nb,rows]+r0[sl]
            pl.semaphore_signal(credit.at[0,sl],inc=1,device_id=(mate,),device_id_type=MESH)
        else:
            for p,(base,size) in enumerate(PARTS):
                o=offs(u,p,size)
                n=size>>t
                rows=pl.ds(pl.multiple_of(core*(dim//2)+base+o[t],8),n)
                acc[nb,rows]=acc[nb,rows]+recv[t][sl,pl.ds(base>>t,n)]
                pl.semaphore_signal(credit.at[t,sl],inc=1,device_id=(link(dims(u,p,t))[1],),device_id_type=MESH)

    def g_at(u,row,n):
        return g_hbm.at[pl.ds(pl.multiple_of(row,8),n),pl.ds(pl.multiple_of(u*TW,TW),TW)]

    def ag_copies(u,t):
        if t==0:
            r=g_at(u,core*(dim//2),dim//2)
            return [pltpu.make_async_remote_copy(src_ref=r,dst_ref=r,send_sem=g_send.at[0,u%NS],recv_sem=g_recv.at[0,u],device_id=(mate,),device_id_type=MESH)]
        out=[]
        for p,(base,size) in enumerate(PARTS):
            o=offs(u,p,size)
            n=size>>t
            row=core*(dim//2)+base+o[t]
            _,peer=link(dims(u,p,t))
            dst=g_at(u,row,n)
            src=acc.at[u%NB,pl.ds(pl.multiple_of(row,8),n)] if t==3 else dst
            out.append(pltpu.make_async_remote_copy(src_ref=src,dst_ref=dst,send_sem=g_send.at[t,u%NS],recv_sem=g_recv.at[t,u],device_id=(peer,),device_id_type=MESH))
        return out

    def ag_rows(t,u):
        r=g_hbm.at[pl.ds(0,half_rows(t)),pl.ds(0,TW)]
        return pltpu.make_async_remote_copy(src_ref=r,dst_ref=r,send_sem=g_send.at[t,u%NS],recv_sem=g_recv.at[t,u],device_id=(mate,),device_id_type=MESH)

    def ag_start(u,t):
        @pl.when(u>=NS)
        def _():
            ag_rows(t,u).wait_send()
        for c in ag_copies(u,t): c.start()

    def local_copies(u):
        out=[]
        for p,(base,size) in enumerate(PARTS):
            o=offs(u,p,size)
            n=size>>3
            row=core*(dim//2)+base+o[3]
            out.append(pltpu.make_async_copy(acc.at[u%NB,pl.ds(pl.multiple_of(row,8),n)],g_at(u,row,n),loc_sem.at[u%NS]))
        return out

    def local_wait(u):
        pltpu.make_async_copy(acc.at[0,pl.ds(0,half_rows(3))],g_hbm.at[pl.ds(0,half_rows(3)),pl.ds(0,TW)],loc_sem.at[u%NS]).wait()

    def rhs_start(u):
        per=dim//TW
        @pl.when(u<n_qkv)
        def _():
            pltpu.make_async_copy(dproj_hbm.at[u//per,:,pl.ds(pl.multiple_of((u%per)*TW,TW),TW)],rhs.at[u%2],rhs_sem.at[u%2]).start()
        @pl.when(u>=n_qkv)
        def _():
            pltpu.make_async_copy(dout_hbm.at[:,pl.ds(pl.multiple_of((u-n_qkv)*TW,TW),TW)],rhs.at[u%2],rhs_sem.at[u%2]).start()

    def rhs_wait(u):
        pltpu.make_async_copy(dout_hbm.at[:,pl.ds(0,TW)],rhs.at[u%2],rhs_sem.at[u%2]).wait()

    pltpu.make_async_copy(at_hbm,lhs.at[0],ld_sem.at[0]).start()
    pltpu.make_async_copy(ot_hbm,lhs.at[1],ld_sem.at[1]).start()
    rhs_start(0)
    pltpu.make_async_copy(at_hbm,lhs.at[0],ld_sem.at[0]).wait()
    pltpu.make_async_copy(ot_hbm,lhs.at[1],ld_sem.at[1]).wait()

    def guarded(u,fn):
        @pl.when(jnp.logical_and(u>=0,u<n_all))
        def _(): fn()

    def step(i,carry):
        def ag0(u):
            ag_rows(0,u).wait_recv()
        def ag1(u):
            ag_rows(1,u).wait_recv(); ag_start(u,0)
        def ag2(u):
            ag_rows(2,u).wait_recv(); ag_start(u,1)
        def ag3(u):
            ag_rows(3,u).wait_recv(); local_wait(u); ag_start(u,2)
        def last(u):
            rs_finish(u,3)
            for c in local_copies(u): c.start()
            ag_start(u,3)
        def mid(t):
            def f(u):
                rs_finish(u,t); rs_start(u,t+1)
            return f
        def first(u):
            @pl.when(u+1<n_all)
            def _(): rhs_start(u+1)
            rhs_wait(u)
            which=jnp.where(u<n_qkv,0,1)
            @pl.loop(0,dim//512)
            def _(b):
                rows=pl.ds(pl.multiple_of(b*512,512),512)
                acc[u%NB,rows]=dot_nn(lhs[which,rows],rhs[u%2])
            rs_start(u,0)
        for lag,fn in ((1,mid(0)),(2,mid(1)),(3,mid(2)),(4,last),(5,ag3),(6,ag2),(7,ag1),(8,ag0),(0,first)):
            guarded(i-lag,functools.partial(fn,i-lag))
        return carry
    lax.fori_loop(0,n_all+8,step,0)

    for j in range(NS):
        u=n_all-NS+j
        for t in range(4):
            all_rows(t,u).wait_send()
            pl.semaphore_wait(credit.at[t,u%NS],1 if t==0 else 3)
            ag_rows(t,u).wait_send()

def reduce_call(at,ot,dproj,dout):
    dim=at.shape[0]; rows=at.shape[1]
    n_qkv=3*dim//TW; n_all=4*dim//TW
    any_=pl.BlockSpec(memory_space=pl.ANY)
    h=dim//2
    D=pltpu.SemaphoreType.DMA
    return pl.pallas_call(
        functools.partial(reduce_kernel,n_qkv,n_all),
        in_specs=[any_]*4,out_specs=any_,
        out_shape=jax.ShapeDtypeStruct((dim,4*dim),F32),
        scratch_shapes=[pltpu.VMEM((2,dim,rows),BF),pltpu.VMEM((2,rows,TW),BF),pltpu.VMEM((NB,dim,TW),F32),
            pltpu.VMEM((NS,h,TW),F32),pltpu.VMEM((NS,h>>1,TW),F32),pltpu.VMEM((NS,h>>2,TW),F32),pltpu.VMEM((NS,h>>3,TW),F32),
            D((2,)),D((2,)),D((4,NS)),D((4,NS)),pltpu.SemaphoreType.REGULAR((4,NS)),D((NS,)),D((4,NS)),D((4,n_all))],
        compiler_params=pltpu.CompilerParams(collective_id=1,has_side_effects=True,vmem_limit_bytes=62<<20),
        cost_estimate=pl.CostEstimate(flops=8*rows*dim*dim,bytes_accessed=40*dim*dim,transcendentals=0),
        name="reduce",
    )(at,ot,dproj,dout)


def dh_kernel(steps, dproj_ref, w_ref, hidden_ref, dout_ref, gain_ref, dh_ref, dgain_ref, acc_ref):
    s, n = pl.program_id(0), pl.program_id(1)
    part = dot_nt(dproj_ref[0], w_ref[...])

    @pl.when(n == 0)
    def _():
        acc_ref[...] = part

    @pl.when(n > 0)
    def _():
        acc_ref[...] += part

    @pl.when(n == steps - 1)
    def _():
        h = hidden_ref[...].astype(F32)
        inv = lax.rsqrt(jnp.mean(h * h, axis=-1, keepdims=True) + NORM_EPS)
        dn = acc_ref[...].astype(BF).astype(F32)
        dgain = jnp.sum(dn * h * inv, axis=0, keepdims=True)
        ds = dn * gain_ref[...].astype(F32)
        dh = dout_ref[...].astype(F32) + inv * ds - h * (inv * inv * inv) * jnp.mean(ds * h, axis=-1, keepdims=True)
        dh_ref[...] = dh.astype(BF)

        @pl.when(s == 0)
        def _():
            dgain_ref[...] = dgain

        @pl.when(s > 0)
        def _():
            dgain_ref[...] += dgain


def dh_call(dproj, w_qkv, hidden, d_out, gain):
    rows, dim = hidden.shape
    tm, tk = 512, 1024
    per = dim // tk
    return pl.pallas_call(
        functools.partial(dh_kernel, 3 * per),
        grid=(rows // tm, 3 * per),
        in_specs=[
            pl.BlockSpec((1, tm, tk), lambda s, n: (n // per, s, n % per)),
            pl.BlockSpec((dim, tk), lambda s, n: (0, n)),
            pl.BlockSpec((tm, dim), lambda s, n: (s, 0)),
            pl.BlockSpec((tm, dim), lambda s, n: (s, 0)),
            pl.BlockSpec((1, dim), lambda s, n: (0, 0)),
        ],
        out_specs=[
            pl.BlockSpec((tm, dim), lambda s, n: (s, 0)),
            pl.BlockSpec((1, dim), lambda s, n: (0, 0)),
        ],
        out_shape=[jax.ShapeDtypeStruct((rows, dim), BF), jax.ShapeDtypeStruct((1, dim), F32)],
        scratch_shapes=[pltpu.VMEM((tm, dim), F32)],
        compiler_params=pltpu.CompilerParams(vmem_limit_bytes=VMEM_LIMIT),
        cost_estimate=pl.CostEstimate(flops=6 * rows * dim * dim, bytes_accessed=rows * dim * 14 + 6 * dim * dim, transcendentals=0),
        name="d_hidden",
    )(dproj, w_qkv, hidden, d_out, gain)


def solution(mesh):
    group = mesh.shape['sp']
    token_spec = P(None, 'sp', None)
    table_spec = P('sp', None)
    swap = functools.partial(lax.all_to_all, axis_name='sp', split_axis=0, concat_axis=0, tiled=True)

    def device_step(hidden, norm_gain, w_qkv, w_out, cos_tab, sin_tab, d_out):
        num_seqs, local_len, dim = hidden.shape
        mine = num_seqs // group
        seq = local_len * group
        rows = mine * seq

        def to_seqs(x):
            x = x.reshape(mine, group, local_len, dim)
            x = lax.all_to_all(x, 'sp', split_axis=1, concat_axis=1, tiled=True)
            return x.reshape(rows, dim)

        def to_tokens(x):
            x = x.reshape(mine, group, local_len, dim)
            x = lax.all_to_all(x, 'sp', split_axis=1, concat_axis=1, tiled=True)
            return x.reshape(num_seqs, local_len, dim)

        tab = lax.all_gather(jnp.concatenate([cos_tab, sin_tab], axis=1), 'sp', axis=0, tiled=True)
        cos, sin = tab[:, :64], tab[:, 64:]
        cos = jnp.concatenate([cos, cos], axis=1)
        sin = jnp.concatenate([-sin, sin], axis=1)
        gain = norm_gain.reshape(1, dim)

        h_seq = to_seqs(hidden)
        normed_t, qkv = qkv_call(h_seq, gain, w_qkv, cos, sin)
        do_seq = to_seqs(d_out)
        d_attn = nt_call(do_seq, w_out)
        attn, attn_t, dproj = attn_call(qkv, d_attn, cos, sin)
        y = to_tokens(out_call(attn, w_out, h_seq))
        dw = reduce_call(normed_t, attn_t, dproj, do_seq)
        dh, dgain = dh_call(dproj, w_qkv, h_seq, do_seq, gain)
        dh = to_tokens(dh)
        dgain = lax.psum(dgain, 'sp')
        return y, dh, dw[:, :3 * dim], dw[:, 3 * dim:], dgain.reshape(dim)

    return jax.shard_map(device_step, mesh=mesh, in_specs=(token_spec, P(None), P(None, None), P(None, None), table_spec, table_spec, token_spec), out_specs=(token_spec, token_spec, P(None, None), P(None, None), P(None)), check_vma=False)
```

```python
import functools
import jax
import jax.numpy as jnp
from jax import lax
from jax.experimental import pallas as pl
from jax.experimental.pallas import tpu as pltpu
from jax.sharding import PartitionSpec as P

NORM_EPS = 1e-6
BF = jnp.bfloat16
F32 = jnp.float32
VMEM_LIMIT = 60 * 1024 * 1024


def dot_nn(a, b):
    return lax.dot_general(a, b, (((1,), (0,)), ((), ())), preferred_element_type=F32)


def dot_nt(a, b):
    return lax.dot_general(a, b, (((1,), (1,)), ((), ())), preferred_element_type=F32)


def rotate(u, cos, sin_signed):
    return u * cos + pltpu.roll(u, 64, 1) * sin_signed


def unrotate(u, cos, sin_signed):
    return u * cos - pltpu.roll(u, 64, 1) * sin_signed


MESH = pl.DeviceIdType.MESH


def flipped(me,j):
    p=me
    for b in range(4):
        if (j>>b)&1:
            p=p+(1<<b)*(1-2*((me//(1<<b))%2))
    return p

ORDER=(2,4,8,1,3,5,9,6,10,12,7,11,13,14,15)

def exchange_kernel(hidden, d_out, tab, gain_ref, w_qkv, w_out,
                    h_seq, do_seq, tab_all, a_t, qkv, d_attn,
                    own, own_tab, hbuf, normed, normed_t, tabs,
                    h_send, h_recv, d_send, d_recv, t_send, t_recv, own_sem, ld_sem, at_sem):
    me=lax.axis_index('sp')
    group=16
    seqs=hidden.shape[0]//group
    loc=hidden.shape[1]
    dim=hidden.shape[2]
    seq=loc*group
    barrier=pltpu.get_barrier_semaphore()
    for j in range(1,group):
        pl.semaphore_signal(barrier,inc=1,device_id=(flipped(me,j),),device_id_type=MESH)
    pl.semaphore_wait(barrier,group-1)

    for j in ORDER:
        pltpu.make_async_remote_copy(src_ref=tab,dst_ref=tab_all.at[pl.ds(pl.multiple_of(me*loc,loc),loc)],send_sem=t_send,recv_sem=t_recv,
            device_id=(flipped(me,j),),device_id_type=MESH).start()
    def send(src,dst,ss,rs,c):
        for j in ORDER:
            peer=flipped(me,j)
            pltpu.make_async_remote_copy(src_ref=src.at[peer*seqs+c],
                dst_ref=dst.at[pl.ds(pl.multiple_of(c*seq+me*loc,loc),loc)],
                send_sem=ss.at[c],recv_sem=rs.at[c],device_id=(peer,),device_id_type=MESH).start()
    for c in range(seqs): send(hidden,h_seq,h_send,h_recv,c)
    for c in range(seqs): send(d_out,do_seq,d_send,d_recv,c)

    copies=[]
    for c in range(seqs):
        copies.append((hidden.at[me*seqs+c],own.at[c],h_seq.at[pl.ds(pl.multiple_of(c*seq+me*loc,loc),loc)]))
        copies.append((d_out.at[me*seqs+c],own.at[seqs+c],do_seq.at[pl.ds(pl.multiple_of(c*seq+me*loc,loc),loc)]))
    copies.append((tab,own_tab,tab_all.at[pl.ds(pl.multiple_of(me*loc,loc),loc)]))
    for n,(a,b,_) in enumerate(copies): pltpu.make_async_copy(a,b,own_sem.at[n]).start()
    for n,(a,b,d) in enumerate(copies):
        pltpu.make_async_copy(a,b,own_sem.at[n]).wait()
        pltpu.make_async_copy(b,d,own_sem.at[n]).start()
    for n,(a,b,d) in enumerate(copies):
        pltpu.make_async_copy(b,d,own_sem.at[n]).wait()

    def from_all(dst,ss,rs):
        r=dst.at[pl.ds(0,(group-1)*loc)]
        return pltpu.make_async_remote_copy(src_ref=r,dst_ref=r,send_sem=ss,recv_sem=rs,device_id=(flipped(me,1),),device_id_type=MESH)

    from_all(tab_all,t_send,t_recv).wait_recv()
    cp=pltpu.make_async_copy(tab_all,tabs,ld_sem); cp.start(); cp.wait()

    tile=512
    per=dim//tile
    def chunk(c,carry):
        rows=pl.ds(pl.multiple_of(c*seq,seq),seq)
        from_all(h_seq,h_send.at[c],h_recv.at[c]).wait_recv()
        cp=pltpu.make_async_copy(h_seq.at[rows],hbuf,ld_sem); cp.start(); cp.wait()
        @pl.when(c>0)
        def _():
            pltpu.make_async_copy(normed_t,a_t.at[:,rows],at_sem).wait()
        blk=128
        @pl.loop(0,seq//blk)
        def _(b):
            r=pl.ds(pl.multiple_of(b*blk,blk),blk)
            h=hbuf[r].astype(F32)
            inv=lax.rsqrt(jnp.mean(h*h,axis=-1,keepdims=True)+NORM_EPS)
            n=(h*inv*gain_ref[...].astype(F32)).astype(BF)
            normed[r]=n
            normed_t[:,r]=n.T
        pltpu.make_async_copy(normed_t,a_t.at[:,rows],at_sem).start()

        def body(w_ref,out_ref):
            n=pl.program_id(0)
            proj=dot_nn(normed[...],w_ref[...])
            @pl.when(n<2*per)
            def _():
                for h in range(tile//128):
                    cols=slice(h*128,(h+1)*128)
                    out_ref[0,:,cols]=rotate(proj[:,cols],tabs[:,:128],tabs[:,128:]).astype(BF)
            @pl.when(n>=2*per)
            def _():
                out_ref[0]=proj.astype(BF)
        pltpu.emit_pipeline(body,grid=(3*per,),
            in_specs=[pl.BlockSpec((dim,tile),lambda n:(0,n))],
            out_specs=[pl.BlockSpec((1,seq,tile),lambda n:(n//per,0,n%per))])(w_qkv,qkv.at[:,rows])
        return carry
    lax.fori_loop(0,seqs,chunk,0)

    def chunk2(c,carry):
        rows=pl.ds(pl.multiple_of(c*seq,seq),seq)
        from_all(do_seq,d_send.at[c],d_recv.at[c]).wait_recv()
        cp=pltpu.make_async_copy(do_seq.at[rows],hbuf,ld_sem); cp.start(); cp.wait()
        def body(w_ref,out_ref):
            out_ref[...]=dot_nt(hbuf[...],w_ref[...]).astype(BF)
        pltpu.emit_pipeline(body,grid=(per,),
            in_specs=[pl.BlockSpec((tile,dim),lambda n:(n,0))],
            out_specs=[pl.BlockSpec((seq,tile),lambda n:(0,n))])(w_out,d_attn.at[rows])
        return carry
    lax.fori_loop(0,seqs,chunk2,0)

    pltpu.make_async_copy(normed_t,a_t.at[:,pl.ds(0,seq)],at_sem).wait()
    for c in range(seqs):
        from_all(h_seq,h_send.at[c],h_recv.at[c]).wait_send()
        from_all(do_seq,d_send.at[c],d_recv.at[c]).wait_send()
    from_all(tab_all,t_send,t_recv).wait_send()

def exchange_call(hidden,d_out,tab,gain,w_qkv,w_out):
    n,loc,dim=hidden.shape
    group=16
    rows=n*loc
    seqs=n//group; seq=loc*group
    any_=pl.BlockSpec(memory_space=pl.ANY)
    D=pltpu.SemaphoreType.DMA
    S=jax.ShapeDtypeStruct
    return pl.pallas_call(
        exchange_kernel,
        in_specs=[any_,any_,any_,pl.BlockSpec(memory_space=pltpu.VMEM),any_,any_],
        out_specs=[any_]*6,
        out_shape=[S((rows,dim),BF),S((rows,dim),BF),S((seq,256),F32),S((dim,rows),BF),S((3,rows,dim),BF),S((rows,dim),BF)],
        scratch_shapes=[pltpu.VMEM((2*seqs,loc,dim),BF),pltpu.VMEM((loc,256),F32),pltpu.VMEM((seq,dim),BF),pltpu.VMEM((seq,dim),BF),pltpu.VMEM((dim,seq),BF),pltpu.VMEM((seq,256),F32),
            D((seqs,)),D((seqs,)),D((seqs,)),D((seqs,)),D,D,D((2*seqs+1,)),D,D],
        compiler_params=pltpu.CompilerParams(collective_id=0,has_side_effects=True,vmem_limit_bytes=48<<20),
        cost_estimate=pl.CostEstimate(flops=8*rows*dim*dim,bytes_accessed=40*dim*dim,transcendentals=0),
        name="exchange",
    )(hidden,d_out,tab,gain,w_qkv,w_out)


TW = 256
PARTS = ((0, 384), (384, 320), (704, 320))
NS = 3
NB = 7
BLK = 256


def attend(scale, qkv, do, tabs, o_out, o_t_out, dproj_out):
    seq = qkv.shape[1]
    for h in range(2):
        cols = slice(h * 128, (h + 1) * 128)
        q = qkv[0, :, cols]
        k = qkv[1, :, cols]
        v = qkv[2, :, cols]
        dout = do[:, cols]
        k_t = k.T
        v_t = v.T
        dk = [None] * (seq // BLK)
        dv = [None] * (seq // BLK)
        for j in range(seq // BLK):
            end = (j + 1) * BLK
            rows = slice(j * BLK, end)
            q_j = q[rows]
            do_j = dout[rows]
            s = dot_nt(k[:end], q_j)
            row = lax.broadcasted_iota(jnp.int32, (end, BLK), 0)
            col = lax.broadcasted_iota(jnp.int32, (end, BLK), 1) + j * BLK
            s = jnp.where(row <= col, s * scale, -1e30)
            m = jnp.max(s, axis=0, keepdims=True)
            e = jnp.exp(s - m)
            p = e * (1.0 / jnp.sum(e, axis=0, keepdims=True))
            p_bf = p.astype(BF)
            o_t = dot_nn(v_t[:, :end], p_bf)
            dp = dot_nt(v[:end], do_j).astype(BF).astype(F32)
            delta = jnp.sum(p * dp, axis=0, keepdims=True)
            ds = (p * (dp - delta) * scale).astype(BF)
            dv_j = dot_nn(p_bf, do_j)
            dk_j = dot_nn(ds, q_j)
            dq_t = dot_nn(k_t[:, :end], ds)
            for i in range(j + 1):
                part = slice(i * BLK, (i + 1) * BLK)
                dv[i] = dv_j[part] if dv[i] is None else dv[i] + dv_j[part]
                dk[i] = dk_j[part] if dk[i] is None else dk[i] + dk_j[part]
            o_out[rows, cols] = o_t.T.astype(BF)
            o_t_out[cols, rows] = o_t.astype(BF)
            dq = dq_t.T.astype(BF).astype(F32)
            dproj_out[0, rows, cols] = unrotate(dq, tabs[rows, :128], tabs[rows, 128:]).astype(BF)
        for j in range(seq // BLK):
            rows = slice(j * BLK, (j + 1) * BLK)
            dkj = dk[j].astype(BF).astype(F32)
            dproj_out[1, rows, cols] = unrotate(dkj, tabs[rows, :128], tabs[rows, 128:]).astype(BF)
            dproj_out[2, rows, cols] = dv[j].astype(BF)


def main_kernel(scale, a_t, qkv, d_attn, tab_all, h_seq, do_seq, w_qkv, w_out, gain_ref,
                g_hbm, o_hbm, o_t_hbm, dproj_hbm, y_hbm, dh_hbm, dgain_ref,
                lhs, dproj_v, acc, r0, r1, r2, r3, qkv_v, do_v, o_v, o_t_v, tabs, o_chunk, dn_acc, h_v, dout_v, dh_v, dg_all,
                lhs_sem, ld_sem, s_send, s_recv, credit, loc_sem, g_send, g_recv,
                in_sem, out_sem, rhs_sem, dh_sem, dg_send, dg_recv):
    me = lax.axis_index('sp')
    group = 16
    dim, rows_all = a_t.shape
    seq = tab_all.shape[0]
    seqs = rows_all // seq
    loc = seq // group
    half = dim // 2
    n_qkv = 3 * dim // TW
    n_all = 4 * dim // TW
    pairs = dim // TW
    core = me % 2
    mate = me + 1 - 2 * core
    recv = (r0, r1, r2, r3)

    def remote(src, dst, ss, rs, peer):
        return pltpu.make_async_remote_copy(src_ref=src, dst_ref=dst, send_sem=ss, recv_sem=rs, device_id=(peer,), device_id_type=MESH)

    def link(d):
        w = 2 + d + d * d
        bit = (me // w) % 2
        return bit, me + w * (1 - 2 * bit)

    def aligned(x, n):
        return pl.multiple_of(x, n)

    def dims(u, p, t):
        return (u + p + t - 1) % 3

    def offs(u, p, size):
        o = [0]
        for t in (1, 2, 3):
            b, _ = link(dims(u, p, t))
            o.append(o[-1] + b * (size >> t))
        return o

    def rs_all(u, t):
        sl = u % NS
        return remote(recv[t].at[sl], recv[t].at[sl], s_send.at[t, sl], s_recv.at[t, sl], mate)

    def rs_start(u, t):
        sl, nb = u % NS, u % NB

        @pl.when(u >= NS)
        def _():
            pl.semaphore_wait(credit.at[t, sl], 1 if t == 0 else 3)
            rs_all(u, t).wait_send()

        if t == 0:
            src = acc.at[nb, pl.ds(aligned((1 - core) * half, half), half)]
            remote(src, r0.at[sl], s_send.at[0, sl], s_recv.at[0, sl], mate).start()
            return
        for p, (base, size) in enumerate(PARTS):
            o = offs(u, p, size)
            n = size >> t
            b, peer = link(dims(u, p, t))
            row = core * half + base + o[t - 1] + (1 - b) * n
            remote(acc.at[nb, pl.ds(aligned(row, 8), n)], recv[t].at[sl, pl.ds(base >> t, n)],
                   s_send.at[t, sl], s_recv.at[t, sl], peer).start()

    def rs_finish(u, t):
        sl, nb = u % NS, u % NB
        rs_all(u, t).wait_recv()
        if t == 0:
            rows = pl.ds(aligned(core * half, half), half)
            acc[nb, rows] = acc[nb, rows] + r0[sl]
            pl.semaphore_signal(credit.at[0, sl], inc=1, device_id=(mate,), device_id_type=MESH)
            return
        for p, (base, size) in enumerate(PARTS):
            n = size >> t
            rows = pl.ds(aligned(core * half + base + offs(u, p, size)[t], 8), n)
            acc[nb, rows] = acc[nb, rows] + recv[t][sl, pl.ds(base >> t, n)]
            pl.semaphore_signal(credit.at[t, sl], inc=1, device_id=(link(dims(u, p, t))[1],), device_id_type=MESH)

    def tile_col(u):
        return jnp.where(u < n_qkv, (u % 3) * pairs + u // 3, u) * TW

    def g_at(u, row, n):
        return g_hbm.at[pl.ds(aligned(row, 8), n), pl.ds(aligned(tile_col(u), TW), TW)]

    def ag_all(u, t):
        r = g_hbm.at[pl.ds(0, half >> t), pl.ds(0, TW)]
        return remote(r, r, g_send.at[t, u % NS], g_recv.at[t, u], mate)

    def ag_start(u, t):
        @pl.when(u >= NS)
        def _():
            ag_all(u, t).wait_send()

        if t == 0:
            r = g_at(u, core * half, half)
            remote(r, r, g_send.at[0, u % NS], g_recv.at[0, u], mate).start()
            return
        for p, (base, size) in enumerate(PARTS):
            n = size >> t
            row = core * half + base + offs(u, p, size)[t]
            dst = g_at(u, row, n)
            src = acc.at[u % NB, pl.ds(aligned(row, 8), n)] if t == 3 else dst
            remote(src, dst, g_send.at[t, u % NS], g_recv.at[t, u], link(dims(u, p, t))[1]).start()

    def local_start(u):
        for p, (base, size) in enumerate(PARTS):
            n = size >> 3
            row = core * half + base + offs(u, p, size)[3]
            pltpu.make_async_copy(acc.at[u % NB, pl.ds(aligned(row, 8), n)], g_at(u, row, n), loc_sem.at[u % NS]).start()

    def local_wait(u):
        n = half >> 3
        pltpu.make_async_copy(acc.at[0, pl.ds(0, n)], g_hbm.at[pl.ds(0, n), pl.ds(0, TW)], loc_sem.at[u % NS]).wait()

    def attn_in(a):
        s, p, sl = a % seqs, a // seqs, a % 2
        rows = pl.ds(aligned(s * seq, seq), seq)
        cols = pl.ds(aligned(p * TW, TW), TW)
        return (pltpu.make_async_copy(qkv.at[:, rows, cols], qkv_v.at[sl], in_sem.at[0, sl]),
                pltpu.make_async_copy(d_attn.at[rows, cols], do_v.at[sl], in_sem.at[1, sl]))

    def attn_out(a):
        s, p, sl = a % seqs, a // seqs, a % 2
        rows = pl.ds(aligned(s * seq, seq), seq)
        cols = pl.ds(aligned(p * TW, TW), TW)
        return (pltpu.make_async_copy(o_v.at[sl], o_hbm.at[rows, cols], out_sem.at[0, sl]),
                pltpu.make_async_copy(o_t_v.at[sl], o_t_hbm.at[cols, rows], out_sem.at[1, sl]),
                pltpu.make_async_copy(dproj_v.at[p % 2, :, rows], dproj_hbm.at[:, rows, cols], out_sem.at[2, sl]))

    n_attn = seqs * pairs

    def attn_step(a):
        @pl.when(a + 1 < n_attn)
        def _():
            for c in attn_in(a + 1):
                c.start()

        for c in attn_in(a):
            c.wait()

        @pl.when(a >= 2)
        def _():
            for c in attn_out(a - 2):
                c.wait()

        s, p, sl = a % seqs, a // seqs, a % 2
        attend(scale, qkv_v.at[sl], do_v.at[sl], tabs, o_v.at[sl], o_t_v.at[sl], dproj_v.at[p % 2, :, pl.ds(aligned(s * seq, seq), seq)])
        for c in attn_out(a):
            c.start()

    def rhs_copy(u):
        j = u - n_qkv
        return pltpu.make_async_copy(do_seq.at[:, pl.ds(aligned(j * TW, TW), TW)], dproj_v.at[0, j % 3], rhs_sem.at[j % 3])

    def dw_tile(u):
        @pl.when(u == n_qkv)
        def _():
            pltpu.make_async_copy(o_t_hbm, lhs, lhs_sem).wait()

        @pl.when(u >= n_qkv)
        def _():
            rhs_copy(u).wait()

        p = jnp.where(u < n_qkv, (u // 3) % 2, 0)

        @pl.loop(0, dim // 512)
        def _(b):
            rows = pl.ds(aligned(b * 512, 512), 512)
            acc[u % NB, rows] = dot_nn(lhs[rows], dproj_v[p, u % 3])

        rs_start(u, 0)

        @pl.when(u == n_qkv - 1)
        def _():
            pltpu.make_async_copy(o_t_hbm, lhs, lhs_sem).start()

        @pl.when(jnp.logical_and(u + 2 >= n_qkv, u + 2 < n_all))
        def _():
            rhs_copy(u + 2).start()

    def seq_rows(c):
        return pl.ds(aligned(c * seq, seq), seq)

    def out_proj(c):
        def body(o_ref, w_ref, h_ref, y_ref):
            y = h_ref[...].astype(F32) + dot_nn(o_ref[...], w_ref[...])
            y_ref[...] = y.astype(BF).reshape(group, loc, y.shape[1])

        tn = 512
        pltpu.emit_pipeline(
            body, grid=(dim // tn,),
            in_specs=[pl.BlockSpec((seq, dim), lambda n: (0, 0)), pl.BlockSpec((dim, tn), lambda n: (0, n)), pl.BlockSpec((seq, tn), lambda n: (0, n))],
            out_specs=[pl.BlockSpec((group, loc, tn), lambda n: (0, 0, n))],
        )(o_hbm.at[seq_rows(c)], w_out, h_seq.at[seq_rows(c)], y_hbm.at[:, c])

    TK = 512
    per = dim // TK

    def d_normed(c, third):
        @pl.when(third == 0)
        def _():
            pltpu.make_async_copy(h_seq.at[seq_rows(c)], h_v, dh_sem.at[0]).start()
            pltpu.make_async_copy(do_seq.at[seq_rows(c)], dout_v, dh_sem.at[1]).start()

        def body(p_ref, w_ref):
            part = dot_nt(p_ref[...], w_ref[...])
            first = jnp.logical_and(third == 0, pl.program_id(0) == 0)

            @pl.when(first)
            def _():
                dn_acc[...] = part

            @pl.when(jnp.logical_not(first))
            def _():
                dn_acc[...] += part

        pltpu.emit_pipeline(
            body, grid=(per,),
            in_specs=[pl.BlockSpec((seq, TK), lambda n: (0, n)), pl.BlockSpec((dim, TK), lambda n: (0, n))],
        )(dproj_hbm.at[third, seq_rows(c)], w_qkv.at[:, pl.ds(aligned(third * dim, dim), dim)])

        @pl.when(third == 2)
        def _():
            pltpu.make_async_copy(h_seq.at[seq_rows(c)], h_v, dh_sem.at[0]).wait()
            pltpu.make_async_copy(do_seq.at[seq_rows(c)], dout_v, dh_sem.at[1]).wait()

            @pl.when(c > 0)
            def _():
                pltpu.make_async_copy(dh_v, dh_hbm.at[:, c], dh_sem.at[2]).wait()

            gain = gain_ref[...].astype(F32)

            @pl.loop(0, group)
            def _(b):
                r = pl.ds(aligned(b * loc, loc), loc)
                h = h_v[r].astype(F32)
                inv = lax.rsqrt(jnp.mean(h * h, axis=-1, keepdims=True) + NORM_EPS)
                dn = dn_acc[r].astype(BF).astype(F32)
                dg = jnp.sum(dn * h * inv, axis=0, keepdims=True)
                ds = dn * gain
                dh = dout_v[r].astype(F32) + inv * ds - h * (inv * inv * inv) * jnp.mean(ds * h, axis=-1, keepdims=True)
                dh_v[b] = dh.astype(BF)
                first = jnp.logical_and(c == 0, b == 0)

                @pl.when(first)
                def _():
                    dg_all[me] = dg

                @pl.when(jnp.logical_not(first))
                def _():
                    dg_all[me] += dg

            pltpu.make_async_copy(dh_v, dh_hbm.at[:, c], dh_sem.at[2]).start()

    barrier = pltpu.get_barrier_semaphore()
    for j in range(1, group):
        pl.semaphore_signal(barrier, inc=1, device_id=(flipped(me, j),), device_id_type=MESH)
    for c in attn_in(0):
        c.start()
    pltpu.make_async_copy(a_t, lhs, lhs_sem).start()
    pltpu.make_async_copy(tab_all, tabs, ld_sem).start()
    pltpu.make_async_copy(tab_all, tabs, ld_sem).wait()
    pl.loop(0, seqs)(attn_step)
    pltpu.make_async_copy(a_t, lhs, lhs_sem).wait()
    pl.semaphore_wait(barrier, group - 1)

    first_out = 3 * (pairs - 1)
    first_dn = first_out + seqs

    def step(i, carry):
        def guarded(lag, fn):
            u = i - lag

            @pl.when(jnp.logical_and(u >= 0, u < n_all))
            def _():
                fn(u)

        def ag0(u):
            ag_all(u, 0).wait_recv()

        def ag1(u):
            ag_all(u, 1).wait_recv()
            ag_start(u, 0)

        def ag2(u):
            ag_all(u, 2).wait_recv()
            ag_start(u, 1)

        def ag3(u):
            ag_all(u, 3).wait_recv()
            local_wait(u)
            ag_start(u, 2)

        def last(u):
            rs_finish(u, 3)
            local_start(u)
            ag_start(u, 3)

        def middle(t):
            def fn(u):
                rs_finish(u, t)
                rs_start(u, t + 1)
            return fn

        for lag, fn in ((1, middle(0)), (2, middle(1)), (3, middle(2)), (4, last), (5, ag3), (6, ag2), (7, ag1), (8, ag0), (0, dw_tile)):
            guarded(lag, fn)

        p, r = i // 3 + 1, i % 3

        @pl.when(p < pairs)
        def _():
            lo = (4 * r + 2) // 3
            hi = (4 * r + 6) // 3

            @pl.loop(lo, hi)
            def _(s):
                attn_step(p * seqs + s)

        @pl.when(i == first_out)
        def _():
            for c in attn_out(n_attn - 2) + attn_out(n_attn - 1):
                c.wait()

        @pl.when(jnp.logical_and(i >= first_out, i < first_dn))
        def _():
            out_proj(i - first_out)

        @pl.when(jnp.logical_and(i >= first_dn, i < first_dn + 3 * seqs))
        def _():
            d_normed((i - first_dn) // 3, (i - first_dn) % 3)

        @pl.when(i == first_dn + 3 * seqs)
        def _():
            for j in range(1, group):
                remote(dg_all.at[me], dg_all.at[me], dg_send, dg_recv, flipped(me, j)).start()

        return carry

    lax.fori_loop(0, n_all + 8, step, 0)

    pltpu.make_async_copy(dh_v, dh_hbm.at[:, 0], dh_sem.at[2]).wait()
    others = remote(dg_all.at[pl.ds(0, group - 1)], dg_all.at[pl.ds(0, group - 1)], dg_send, dg_recv, mate)
    others.wait_recv()
    others.wait_send()
    dgain = dg_all[0]
    for j in range(1, group):
        dgain = dgain + dg_all[j]
    dgain_ref[...] = dgain
    for j in range(NS):
        u = n_all - NS + j
        for t in range(4):
            rs_all(u, t).wait_send()
            pl.semaphore_wait(credit.at[t, u % NS], 1 if t == 0 else 3)
            ag_all(u, t).wait_send()


def main_call(a_t, qkv, d_attn, tab, h_seq, do_seq, w_qkv, w_out, gain):
    dim, rows = a_t.shape
    seq = tab.shape[0]
    seqs = rows // seq
    group = 16
    loc = seq // group
    h = dim // 2
    n_all = 4 * dim // TW
    hbm = pl.BlockSpec(memory_space=pl.ANY)
    vmem = pl.BlockSpec(memory_space=pltpu.VMEM)
    D = pltpu.SemaphoreType.DMA
    S = jax.ShapeDtypeStruct
    V = pltpu.VMEM
    return pl.pallas_call(
        functools.partial(main_kernel, 128 ** -0.5),
        in_specs=[hbm] * 8 + [vmem],
        out_specs=[hbm] * 6 + [vmem],
        out_shape=[S((dim, 4 * dim), F32), S((rows, dim), BF), S((dim, rows), BF), S((3, rows, dim), BF),
                   S((group, seqs, loc, dim), BF), S((group, seqs, loc, dim), BF), S((1, dim), F32)],
        scratch_shapes=[
            V((dim, rows), BF), V((2, 3, rows, TW), BF), V((NB, dim, TW), F32),
            V((NS, h, TW), F32), V((NS, h >> 1, TW), F32), V((NS, h >> 2, TW), F32), V((NS, h >> 3, TW), F32),
            V((2, 3, seq, TW), BF), V((2, seq, TW), BF), V((2, seq, TW), BF), V((2, TW, seq), BF), V((seq, 256), F32),
            V((8, 128), BF), V((seq, dim), F32), V((seq, dim), BF), V((seq, dim), BF), V((group, loc, dim), BF), V((group, 1, dim), F32),
            D, D, D((4, NS)), D((4, NS)), pltpu.SemaphoreType.REGULAR((4, NS)), D((NS,)), D((4, NS)), D((4, n_all)),
            D((2, 2)), D((3, 2)), D((3,)), D((3,)), D, D,
        ],
        compiler_params=pltpu.CompilerParams(collective_id=1, has_side_effects=True, vmem_limit_bytes=67043328),
        cost_estimate=pl.CostEstimate(flops=20 * rows * dim * dim, bytes_accessed=60 * dim * dim, transcendentals=0),
        name="main",
    )(a_t, qkv, d_attn, tab, h_seq, do_seq, w_qkv, w_out, gain)


def solution(mesh):
    group = mesh.shape['sp']
    token_spec = P(None, 'sp', None)
    table_spec = P('sp', None)

    def device_step(hidden, norm_gain, w_qkv, w_out, cos_tab, sin_tab, d_out):
        num_seqs, local_len, dim = hidden.shape
        mine = num_seqs // group
        seq = local_len * group
        rows = mine * seq

        def to_tokens(x):
            x = lax.all_to_all(x, 'sp', split_axis=0, concat_axis=0, tiled=True)
            return x.reshape(num_seqs, local_len, dim)

        gain = norm_gain.reshape(1, dim)
        tab = jnp.concatenate([cos_tab, cos_tab, -sin_tab, sin_tab], axis=1)
        h_seq, do_seq, tab, normed_t, qkv, d_attn = exchange_call(hidden, d_out, tab, gain, w_qkv, w_out)
        dw, _, _, _, y, dh, dgain = main_call(normed_t, qkv, d_attn, tab, h_seq, do_seq, w_qkv, w_out, gain)
        y = to_tokens(y)
        dh = to_tokens(dh)
        return y, dh, dw[:, :3 * dim], dw[:, 3 * dim:], dgain.reshape(dim)

    return jax.shard_map(device_step, mesh=mesh, in_specs=(token_spec, P(None), P(None, None), P(None, None), table_spec, table_spec, token_spec), out_specs=(token_spec, token_spec, P(None, None), P(None, None), P(None)), check_vma=False)
```

```python
import functools
import jax
import jax.numpy as jnp
from jax import lax
from jax.experimental import pallas as pl
from jax.experimental.pallas import tpu as pltpu
from jax.sharding import PartitionSpec as P

NORM_EPS = 1e-6
BF = jnp.bfloat16
F32 = jnp.float32
VMEM_LIMIT = 60 * 1024 * 1024


def dot_nn(a, b):
    return lax.dot_general(a, b, (((1,), (0,)), ((), ())), preferred_element_type=F32)


def dot_nt(a, b):
    return lax.dot_general(a, b, (((1,), (1,)), ((), ())), preferred_element_type=F32)


def rotate(u, cos, sin_signed):
    return u * cos + pltpu.roll(u, 64, 1) * sin_signed


def unrotate(u, cos, sin_signed):
    return u * cos - pltpu.roll(u, 64, 1) * sin_signed


MESH = pl.DeviceIdType.MESH


def flipped(me, j):
    p = me
    for b in range(4):
        w = 1 << b
        if j & w:
            p = p + w * (1 - 2 * ((me // w) % 2))
    return p


ORDER = tuple(int(j, 16) for j in '2481359' + '6ac7bdef')


TW = 256
PARTS = ((0, 384), (384, 320), (704, 320))
NS = 3
NB = 6
BLK = 256


def attend(scale, qkv, do, tabs, o_out, o_t_out, dproj_out):
    seq = qkv.shape[1]
    for h in range(2):
        cols = slice(h * 128, (h + 1) * 128)
        q = qkv[0, :, cols]
        k = qkv[1, :, cols]
        v = qkv[2, :, cols]
        dout = do[:, cols]
        k_t = k.T
        v_t = v.T
        dk = [None] * (seq // BLK)
        dv = [None] * (seq // BLK)
        for j in range(seq // BLK):
            end = (j + 1) * BLK
            rows = slice(j * BLK, end)
            q_j = q[rows]
            do_j = dout[rows]
            s = dot_nt(k[:end], q_j)
            row = lax.broadcasted_iota(jnp.int32, (end, BLK), 0)
            col = lax.broadcasted_iota(jnp.int32, (end, BLK), 1) + j * BLK
            s = jnp.where(row <= col, s * scale, -1e30)
            m = jnp.max(s, axis=0, keepdims=True)
            e = jnp.exp(s - m)
            p = e * (1.0 / jnp.sum(e, axis=0, keepdims=True))
            p_bf = p.astype(BF)
            o_t = dot_nn(v_t[:, :end], p_bf)
            dp = dot_nt(v[:end], do_j).astype(BF).astype(F32)
            delta = jnp.sum(p * dp, axis=0, keepdims=True)
            ds = (p * (dp - delta) * scale).astype(BF)
            dv_j = dot_nn(p_bf, do_j)
            dk_j = dot_nn(ds, q_j)
            dq_t = dot_nn(k_t[:, :end], ds)
            for i in range(j + 1):
                part = slice(i * BLK, (i + 1) * BLK)
                dv[i] = dv_j[part] if dv[i] is None else dv[i] + dv_j[part]
                dk[i] = dk_j[part] if dk[i] is None else dk[i] + dk_j[part]
            o_out[rows, cols] = o_t.T.astype(BF)
            o_t_out[cols, rows] = o_t.astype(BF)
            dq = dq_t.T.astype(BF).astype(F32)
            dproj_out[0, rows, cols] = unrotate(dq, tabs[rows, :128], tabs[rows, 128:]).astype(BF)
        for j in range(seq // BLK):
            rows = slice(j * BLK, (j + 1) * BLK)
            dkj = dk[j].astype(BF).astype(F32)
            dproj_out[1, rows, cols] = unrotate(dkj, tabs[rows, :128], tabs[rows, 128:]).astype(BF)
            dproj_out[2, rows, cols] = dv[j].astype(BF)


def main_kernel(scale, hidden, d_out, cos_ref, sin_ref, w_qkv, w_out, gain_ref,
                g_hbm, h_seq, do_seq, qkv, o_hbm, o_t_hbm, dproj_hbm, y_all, dh_hbm, dh_loc, dh_all, dgain_ref,
                lhs, dproj_v, acc, r0, r1, r2, r3, qkv_v, do_v, o_v, o_t_v, tabs, tab, dn_acc, h_v, dout_v, dh_v, dg_all, wbuf, pbuf, o_c, y_t,
                lhs_sem, ld_sem, s_send, s_recv, credit, loc_sem, g_send, g_recv,
                in_sem, out_sem, rhs_sem, dh_sem, dg_send, dg_recv, w_sem, o_sem, c0_sem,
                h_send, h_recv, d_send, d_recv, t_send, t_recv, own_sem, y_send, y_recv, y_own, x_send, x_recv):
    me = lax.axis_index('sp')
    group = 16
    loc, dim = hidden.shape[1:]
    seqs = hidden.shape[0] // group
    seq = loc * group
    half = dim // 2
    n_qkv = 3 * dim // TW
    n_all = 4 * dim // TW
    pairs = dim // TW
    core = me % 2
    mate = me + 1 - 2 * core
    recv = (r0, r1, r2, r3)
    TN = 512
    per = dim // TN

    def remote(src, dst, ss, rs, peer):
        return pltpu.make_async_remote_copy(src_ref=src, dst_ref=dst, send_sem=ss, recv_sem=rs, device_id=(peer,), device_id_type=MESH)

    def link(d):
        w = 2 + d + d * d
        bit = (me // w) % 2
        return bit, me + w * (1 - 2 * bit)

    def aligned(x, n):
        return pl.multiple_of(x, n)

    def dims(u, p, t):
        return (u + p + t - 1) % 3

    def offs(u, p, size):
        o = [0]
        for t in (1, 2, 3):
            b, _ = link(dims(u, p, t))
            o.append(o[-1] + b * (size >> t))
        return o

    def rs_all(u, t):
        sl = u % NS
        return remote(recv[t].at[sl], recv[t].at[sl], s_send.at[t, sl], s_recv.at[t, sl], mate)

    def rs_start(u, t):
        sl, nb = u % NS, u % NB

        @pl.when(u >= NS)
        def _():
            pl.semaphore_wait(credit.at[t, sl], 1 if t == 0 else 3)

        if t == 0:
            n = half // 4
            for k in range(4):
                src = acc.at[nb, pl.ds(aligned((1 - core) * half + k * n, n), n)]
                remote(src, r0.at[sl, pl.ds(k * n, n)], s_send.at[0, sl], s_recv.at[0, sl], mate).start()
            return
        for p, (base, size) in enumerate(PARTS):
            o = offs(u, p, size)
            n = size >> t
            b, peer = link(dims(u, p, t))
            row = core * half + base + o[t - 1] + (1 - b) * n
            remote(acc.at[nb, pl.ds(aligned(row, 8), n)], recv[t].at[sl, pl.ds(base >> t, n)],
                   s_send.at[t, sl], s_recv.at[t, sl], peer).start()

    def rs_finish(u, t):
        sl, nb = u % NS, u % NB
        rs_all(u, t).wait_recv()
        rs_all(u, t).wait_send()
        if t == 0:
            rows = pl.ds(aligned(core * half, half), half)
            acc[nb, rows] = acc[nb, rows] + r0[sl]
            pl.semaphore_signal(credit.at[0, sl], inc=1, device_id=(mate,), device_id_type=MESH)
            return
        for p, (base, size) in enumerate(PARTS):
            n = size >> t
            rows = pl.ds(aligned(core * half + base + offs(u, p, size)[t], 8), n)
            acc[nb, rows] = acc[nb, rows] + recv[t][sl, pl.ds(base >> t, n)]
            pl.semaphore_signal(credit.at[t, sl], inc=1, device_id=(link(dims(u, p, t))[1],), device_id_type=MESH)

    def tile_col(u):
        return jnp.where(u < n_qkv, (u % 3) * pairs + u // 3, u) * TW

    def g_at(u, row, n):
        return g_hbm.at[pl.ds(aligned(row, 8), n), pl.ds(aligned(tile_col(u), TW), TW)]

    def ag_all(u, t):
        r = g_hbm.at[pl.ds(0, half >> t), pl.ds(0, TW)]
        return remote(r, r, g_send.at[t, u % NS], g_recv.at[t, u], mate)

    def ag_start(u, t):
        if t < 3:
            @pl.when(u >= NS)
            def _():
                ag_all(u, t).wait_send()

        if t == 0:
            r = g_at(u, core * half, half)
            remote(r, r, g_send.at[0, u % NS], g_recv.at[0, u], mate).start()
            return
        for p, (base, size) in enumerate(PARTS):
            n = size >> t
            row = core * half + base + offs(u, p, size)[t]
            dst = g_at(u, row, n)
            src = acc.at[u % NB, pl.ds(aligned(row, 8), n)] if t == 3 else dst
            remote(src, dst, g_send.at[t, u % NS], g_recv.at[t, u], link(dims(u, p, t))[1]).start()

    def local_start(u):
        for p, (base, size) in enumerate(PARTS):
            n = size >> 3
            row = core * half + base + offs(u, p, size)[3]
            pltpu.make_async_copy(acc.at[u % NB, pl.ds(aligned(row, 8), n)], g_at(u, row, n), loc_sem.at[u % NS]).start()

    def local_wait(u):
        n = half >> 3
        pltpu.make_async_copy(acc.at[0, pl.ds(0, n)], g_hbm.at[pl.ds(0, n), pl.ds(0, TW)], loc_sem.at[u % NS]).wait()

    n_attn = seqs * pairs
    n_early = pairs + 2 * (seqs - 1)

    def place(a):
        b, c = a - pairs, a - n_early
        s = jnp.where(a < pairs, 0, 1 + jnp.where(c < 0, b // 2, c % (seqs - 1)))
        p = jnp.where(a < pairs, a, jnp.where(c < 0, b % 2, 2 + c // (seqs - 1)))
        return s, p, seq_rows(s), pl.ds(aligned(p * TW, TW), TW)

    def seq_rows(c):
        return pl.ds(aligned(c * seq, seq), seq)

    def attn_in(a, fn):
        _, _, rows, cols = place(a)
        sl = a % 2
        fn(pltpu.make_async_copy(qkv.at[:, rows, cols], qkv_v.at[sl], in_sem.at[0, sl]))
        fn(pltpu.make_async_copy(w_out.at[cols], o_c.at[sl], in_sem.at[1, sl]))

    def start(copy):
        copy.start()

    def wait(copy):
        copy.wait()

    def dproj_rows(a):
        s, p, _, _ = place(a)
        return dproj_v.at[p % 2, :, seq_rows(jnp.where(jnp.logical_and(s == 0, p >= 2), seqs - 1, s))]

    def attn_out(a):
        _, _, rows, cols = place(a)
        sl = a % 2
        return (pltpu.make_async_copy(o_v.at[sl], o_hbm.at[rows, cols], out_sem.at[0, sl]),
                pltpu.make_async_copy(o_t_v.at[sl], o_t_hbm.at[cols, rows], out_sem.at[1, sl]),
                pltpu.make_async_copy(dproj_rows(a), dproj_hbm.at[:, rows, cols], out_sem.at[2, sl]))

    def attn_out_wait(a):
        for c in attn_out(a):
            c.wait()

    def attn_step(a):
        @pl.when(jnp.logical_and(a != pairs - 1, a + 1 < n_attn))
        def _():
            attn_in(a + 1, start)

        attn_in(a, wait)

        @pl.when(jnp.logical_and(a >= 2, a // 2 != pairs // 2))
        def _():
            attn_out_wait(a)

        s, _, _, _ = place(a)
        sl = a % 2

        @pl.when(s == 0)
        def _():
            do_v[sl] = dot_nt(h_v[...], o_c[sl]).astype(BF)

        @pl.when(jnp.logical_and(s > 0, s < seqs - 1))
        def _():
            total = None
            for n in range(per):
                cols = slice(n * TN, (n + 1) * TN)
                part = dot_nt(wbuf[s - 1, cols], o_c[sl, :, cols])
                total = part if total is None else total + part
            do_v[sl] = total.astype(BF)

        @pl.when(s == seqs - 1)
        def _():
            do_v[sl] = dot_nt(dh_v[...].reshape(seq, dim), o_c[sl]).astype(BF)

        attend(scale, qkv_v.at[sl], do_v.at[sl], tabs, o_v.at[sl], o_t_v.at[sl], dproj_rows(a))
        for c in attn_out(a):
            c.start()

    def first_seq(p):
        rows = seq_rows(0)
        return pltpu.make_async_copy(dproj_hbm.at[:, rows, pl.ds(aligned(p * TW, TW), TW)], dproj_v.at[p % 2, :, rows], c0_sem.at[p % 2])

    def rhs_copy(u):
        j = u - n_qkv
        return pltpu.make_async_copy(do_seq.at[:, pl.ds(aligned(j * TW, TW), TW)], dproj_v.at[0, j % 3], rhs_sem.at[j % 3])

    def dw_tile(u):
        @pl.when(u == n_qkv)
        def _():
            pltpu.make_async_copy(o_t_hbm, lhs, lhs_sem).wait()

        @pl.when(u >= n_qkv)
        def _():
            rhs_copy(u).wait()

        @pl.when(jnp.logical_and(u % 3 == 0, jnp.logical_and(u >= 6, u < n_qkv)))
        def _():
            first_seq(u // 3).wait()

        p = jnp.where(u < n_qkv, (u // 3) % 2, 0)

        @pl.loop(0, dim // 512)
        def _(b):
            rows = pl.ds(aligned(b * 512, 512), 512)
            acc[u % NB, rows] = dot_nn(lhs[rows], dproj_v[p, u % 3])

        rs_start(u, 0)

        @pl.when(u == n_qkv - 1)
        def _():
            pltpu.make_async_copy(o_t_hbm, lhs, lhs_sem).start()

        @pl.when(jnp.logical_and(u + 2 >= n_qkv, u + 2 < n_all))
        def _():
            rhs_copy(u + 2).start()

    n_blocks = 4 * seqs

    def columns(n):
        return pl.ds(aligned(n * TN, TN), TN)

    def block(b):
        is_out = jnp.logical_or(b == 0, jnp.logical_and((b + 1) % 3 == 0, b <= 3 * seqs - 4))
        done = jnp.minimum((b + 1) // 3, seqs - 1)
        return is_out, done, b - 1 - done

    def tile_start(t):
        b, n, sl = t // per, t % per, t % 2
        is_out, c, q = block(b)

        @pl.when(is_out)
        def _():
            pltpu.make_async_copy(w_out.at[:, columns(n)], wbuf.at[sl], w_sem.at[0, sl]).start()
            pltpu.make_async_copy(h_seq.at[seq_rows(c), columns(n)], pbuf.at[sl], w_sem.at[1, sl]).start()

        @pl.when(jnp.logical_not(is_out))
        def _():
            pltpu.make_async_copy(w_qkv.at[:, columns((q % 3) * per + n)], wbuf.at[sl], w_sem.at[0, sl]).start()
            pltpu.make_async_copy(dproj_hbm.at[q % 3, seq_rows(q // 3), columns(n)], pbuf.at[sl], w_sem.at[1, sl]).start()

    def tile_wait(t):
        sl = t % 2
        pltpu.make_async_copy(w_out.at[:, columns(0)], wbuf.at[sl], w_sem.at[0, sl]).wait()
        pltpu.make_async_copy(h_seq.at[seq_rows(0), columns(0)], pbuf.at[sl], w_sem.at[1, sl]).wait()

    def o_load(c):
        n = seq // 2
        return [pltpu.make_async_copy(o_hbm.at[pl.ds(aligned(c * seq + k * n, n), n)], o_c.at[k], o_sem.at[k]) for k in range(2)]

    def y_sent(n):
        r = y_all.at[pl.ds(0, group - 1), :, columns(0)]
        return remote(r, r, y_send.at[n], y_recv.at[0], mate)

    def y_own_copy(c, n):
        return pltpu.make_async_copy(y_t.at[n, me], y_all.at[me * seqs + c, :, columns(n)], y_own.at[n])

    def out_tile(c, n, sl):
        y = pbuf[sl].astype(F32) + dot_nn(o_c[...].reshape(seq, dim), wbuf[sl])

        @pl.when(c > 0)
        def _():
            y_sent(n).wait_send()
            y_own_copy(0, n).wait()

        y_t[n] = y.astype(BF).reshape(group, loc, TN)
        for j in ORDER:
            peer = flipped(me, j)
            remote(y_t.at[n, peer], y_all.at[me * seqs + c, :, columns(n)], y_send.at[n], y_recv.at[c], peer).start()
        y_own_copy(c, n).start()

    def run_block(b):
        is_out, c_out, q = block(b)
        c, third = q // 3, q % 3

        @pl.when(is_out)
        def _():
            for x in o_load(c_out):
                x.wait()

        @pl.when(jnp.logical_and(jnp.logical_not(is_out), third == 2))
        def _():
            pltpu.make_async_copy(h_seq.at[seq_rows(c)], h_v, dh_sem.at[0]).start()
            pltpu.make_async_copy(do_seq.at[seq_rows(c)], dout_v, dh_sem.at[1]).start()

        @pl.loop(0, per)
        def _(n):
            t = b * per + n
            sl = t % 2

            @pl.when(jnp.logical_and(t != per - 1, t + 1 < n_blocks * per))
            def _():
                tile_start(t + 1)

            tile_wait(t)

            @pl.when(is_out)
            def _():
                out_tile(c_out, n, sl)

            @pl.when(jnp.logical_not(is_out))
            def _():
                part = dot_nt(pbuf[sl], wbuf[sl])
                first = jnp.logical_and(third == 0, n == 0)

                @pl.when(first)
                def _():
                    dn_acc[...] = part

                @pl.when(jnp.logical_not(first))
                def _():
                    dn_acc[...] += part

        @pl.when(jnp.logical_and(is_out, jnp.logical_and(c_out > 0, c_out + 1 < seqs)))
        def _():
            for x in o_load(c_out + 1):
                x.start()

        @pl.when(jnp.logical_and(jnp.logical_not(is_out), third == 2))
        def _():
            norm_back(c)

    def norm_back(c):
        pltpu.make_async_copy(h_seq.at[seq_rows(c)], h_v, dh_sem.at[0]).wait()
        pltpu.make_async_copy(do_seq.at[seq_rows(c)], dout_v, dh_sem.at[1]).wait()

        @pl.when(c > 0)
        def _():
            pltpu.make_async_copy(dh_v, dh_hbm.at[:, 0], dh_sem.at[2]).wait()

        gain = gain_ref[...].astype(F32)

        @pl.loop(0, group)
        def _(b):
            r = pl.ds(aligned(b * loc, loc), loc)
            h = h_v[r].astype(F32)
            inv = lax.rsqrt(jnp.mean(h * h, axis=-1, keepdims=True) + NORM_EPS)
            dn = dn_acc[r].astype(BF).astype(F32)
            dg = jnp.sum(dn * h * inv, axis=0, keepdims=True)
            ds = dn * gain
            dh = dout_v[r].astype(F32) + inv * ds - h * (inv * inv * inv) * jnp.mean(ds * h, axis=-1, keepdims=True)
            dh_v[b] = dh.astype(BF)
            first = jnp.logical_and(c == 0, b == 0)

            @pl.when(first)
            def _():
                dg_all[me] = dg

            @pl.when(jnp.logical_not(first))
            def _():
                dg_all[me] += dg

        @pl.when(c < by_xla)
        def _():
            pltpu.make_async_copy(dh_v, dh_hbm.at[:, c], dh_sem.at[2]).start()

        @pl.when(c >= by_xla)
        def _():
            pltpu.make_async_copy(dh_v, dh_loc.at[:, c - by_xla], dh_sem.at[2]).start()

    def dh_send(q):
        k, cols = q // 4, pl.ds(aligned((q % 4) * (dim // 4), dim // 4), dim // 4)
        for j in ORDER:
            peer = flipped(me, j)
            remote(dh_loc.at[peer, k, :, cols], dh_all.at[me, k, :, cols], x_send.at[q], x_recv.at[q], peer).start()
        pltpu.make_async_copy(dh_loc.at[me, k, :, cols], dh_all.at[me, k, :, cols], own_sem.at[q]).start()

    def dh_wait(q):
        r = dh_all.at[pl.ds(0, group - 1), 0, :, pl.ds(0, dim // 4)]
        done = remote(r, r, x_send.at[q], x_recv.at[q], mate)
        done.wait_recv()
        done.wait_send()
        pltpu.make_async_copy(dh_loc.at[0, 0, :, pl.ds(0, dim // 4)], dh_all.at[0, 0, :, pl.ds(0, dim // 4)], own_sem.at[q]).wait()

    def my_rows(c):
        return pl.ds(aligned(c * seq + me * loc, loc), loc)

    def from_all(dst, ss, rs):
        r = dst.at[pl.ds(0, (group - 1) * loc)]
        return remote(r, r, ss, rs, mate)

    def send_all(src, dst, ss, rs, c):
        for j in ORDER:
            peer = flipped(me, j)
            to = dh_v.at[me] if dst is do_seq and c == seqs - 1 else dst.at[my_rows(c)]
            remote(src.at[peer * seqs + c], to, ss.at[c], rs.at[c], peer).start()

    def project(c):
        rows = seq_rows(c)
        from_all(h_seq, h_send.at[c], h_recv.at[c]).wait_recv()
        load = pltpu.make_async_copy(h_seq.at[rows], h_v, ld_sem)
        load.start()
        load.wait()
        gain = gain_ref[...].astype(F32)
        blk = 128

        @pl.loop(0, seq // blk)
        def _(b):
            r = pl.ds(aligned(b * blk, blk), blk)
            h = h_v[r].astype(F32)
            inv = lax.rsqrt(jnp.mean(h * h, axis=-1, keepdims=True) + NORM_EPS)
            n = (h * inv * gain).astype(BF)
            dout_v[r] = n
            lhs[:, pl.ds(aligned(c * seq + b * blk, blk), blk)] = n.T

        @pl.loop(0, 3 * per)
        def _(n):
            t = c * 3 * per + n
            sl = t % 2

            @pl.when(t + 1 < seqs * 3 * per)
            def _():
                qkv_w(t + 1).start()

            qkv_w(t).wait()
            proj = dot_nn(dout_v[...], wbuf[sl])

            @pl.when(t >= 2)
            def _():
                qkv_out(t).wait()

            @pl.when(n < 2 * per)
            def _():
                for h in range(TN // 128):
                    cols = slice(h * 128, (h + 1) * 128)
                    pbuf[sl, :, cols] = rotate(proj[:, cols], tabs[:, :128], tabs[:, 128:]).astype(BF)

            @pl.when(n >= 2 * per)
            def _():
                pbuf[sl] = proj.astype(BF)

            qkv_out(t).start()

    def qkv_w(t):
        return pltpu.make_async_copy(w_qkv.at[:, columns(t % (3 * per))], wbuf.at[t % 2], w_sem.at[0, t % 2])

    def qkv_out(t):
        n = t % (3 * per)
        return pltpu.make_async_copy(pbuf.at[t % 2], qkv.at[n // per, seq_rows(t // (3 * per)), columns(n % per)], w_sem.at[1, t % 2])

    def gradient_in():
        for t in range(2):
            qkv_out(t).wait()
        attn_in(0, start)
        for c in range(seqs - 1):
            from_all(do_seq, d_send.at[c], d_recv.at[c]).wait_recv()
            rows = seq_rows(c)
            if c == 0:
                loads = [pltpu.make_async_copy(do_seq.at[rows], h_v, ld_sem)]
            else:
                loads = [pltpu.make_async_copy(do_seq.at[rows, pl.ds(n * TN, TN)], wbuf.at[c - 1, pl.ds(n * TN, TN)], x_send.at[n]) for n in range(per)]
            for x in loads:
                x.start()
            for x in loads:
                x.wait()
            if c == 0:
                pl.loop(0, pairs)(attn_step)
                attn_out_wait(pairs - 2)
                attn_out_wait(pairs - 1)
                for x in o_load(0):
                    x.start()
                tile_start(0)
                run_block(0)
                attn_in(pairs, start)
            else:
                pl.loop(pairs + 2 * c - 2, pairs + 2 * c)(attn_step)
        from_all(do_seq, d_send.at[seqs - 1], d_recv.at[seqs - 1]).wait_recv()
        last_copy().start()
        attn_step(n_early - 2)

    def last_copy():
        dst = do_seq.at[seq_rows(seqs - 1)]
        return pltpu.make_async_copy(dh_v, dst.reshape(group, loc, dim), ld_sem)

    by_xla = dh_hbm.shape[1]

    def own_in(k):
        src = hidden if k < seqs else d_out
        to = dh_v.at[me] if k == 2 * seqs - 1 else dout_v.at[pl.ds(k * loc, loc)]
        return pltpu.make_async_copy(src.at[me * seqs + k % seqs], to, own_sem.at[k])

    def own_out(k):
        dst = h_seq if k < seqs else do_seq
        return pltpu.make_async_copy(dout_v.at[pl.ds(k * loc, loc)], dst.at[my_rows(k % seqs)], own_sem.at[k])

    for k in range(2 * seqs):
        own_in(k).start()
    cos, sin = cos_ref[...], sin_ref[...]
    tab[...] = jnp.concatenate([cos, cos, -sin, sin], axis=1)
    barrier = pltpu.get_barrier_semaphore()
    for j in range(1, group):
        pl.semaphore_signal(barrier, inc=1, device_id=(flipped(me, j),), device_id_type=MESH)
    pl.semaphore_wait(barrier, group - 1)
    mine = pl.ds(aligned(me * loc, loc), loc)
    for j in ORDER:
        remote(tab, tabs.at[mine], t_send, t_recv, flipped(me, j)).start()
    for c in range(seqs):
        send_all(hidden, h_seq, h_send, h_recv, c)
    for c in range(seqs):
        send_all(d_out, do_seq, d_send, d_recv, c)
    for k in range(2 * seqs):
        own_in(k).wait()
        if k < 2 * seqs - 1:
            own_out(k).start()
    tabs[mine] = tab[...]
    from_all(tabs, t_send, t_recv).wait_recv()
    for k in range(2 * seqs - 1):
        own_out(k).wait()
    qkv_w(0).start()
    pl.loop(0, seqs)(project)
    gradient_in()

    first_out = 3 * (pairs - 1)
    first_dn = first_out + seqs

    def step(i, carry):
        def guarded(lag, fn):
            u = i - lag

            @pl.when(jnp.logical_and(u >= 0, u < n_all))
            def _():
                fn(u)

        def ag0(u):
            ag_all(u, 0).wait_recv()

        def ag1(u):
            ag_all(u, 1).wait_recv()
            ag_start(u, 0)

        def ag2(u):
            ag_all(u, 2).wait_recv()
            ag_start(u, 1)

        def ag3(u):
            ag_all(u, 3).wait_recv()
            ag_all(u, 3).wait_send()
            local_wait(u)
            ag_start(u, 2)

        def last(u):
            rs_finish(u, 3)
            local_start(u)
            ag_start(u, 3)

        def middle(t):
            def fn(u):
                rs_finish(u, t)
                rs_start(u, t + 1)
            return fn

        for lag, fn in enumerate((dw_tile, middle(0), middle(1), middle(2), last, ag3, ag2, ag1, ag0)):
            guarded(lag, fn)

        from_a, to_a = [n_early - 1 + jnp.maximum(k - 2, 0) for k in (i, i + 1)]

        @pl.when(jnp.logical_and(i % 3 == 0, jnp.logical_and(i >= 3, i < first_out)))
        def _():
            first_seq(i // 3 + 1).start()

        @pl.when(i < first_out)
        def _():
            pl.loop(from_a, to_a)(attn_step)

        @pl.when(i == first_out)
        def _():
            attn_out_wait(n_attn - 2)
            attn_out_wait(n_attn - 1)
            for x in o_load(1):
                x.start()
            tile_start(per)

        def blocks(i):
            k = i - first_out
            return jnp.where(k <= seqs, jnp.maximum(3 * k - 1, 1), jnp.minimum(k + 2 * seqs - 1, n_blocks))

        @pl.when(i >= first_out)
        def _():
            pl.loop(blocks(i), blocks(i + 1))(run_block)

        @pl.when(i == 3)
        def _():
            last_copy().wait()

        first_dh = first_dn + seqs + 1

        @pl.when(i == first_dh)
        def _():
            pltpu.make_async_copy(dh_v, dh_hbm.at[:, 0], dh_sem.at[2]).wait()
            for j in range(1, group):
                remote(dg_all.at[me], dg_all.at[me], dg_send, dg_recv, flipped(me, j)).start()

        @pl.when(jnp.logical_and(i >= first_dh, i < first_dh + 4 * (seqs - by_xla)))
        def _():
            dh_send(i - first_dh)

        return carry

    lax.fori_loop(0, n_all + 8, step, 0)

    for c in range(seqs):
        r = y_all.at[pl.ds(0, group - 1)]
        remote(r, r, y_send.at[0], y_recv.at[c], mate).wait_recv()
        from_all(h_seq, h_send.at[c], h_recv.at[c]).wait_send()
        from_all(do_seq, d_send.at[c], d_recv.at[c]).wait_send()
    for n in range(per):
        y_sent(n).wait_send()
        y_own_copy(0, n).wait()
    from_all(tabs, t_send, t_recv).wait_send()
    for q in range(4 * (seqs - by_xla)):
        dh_wait(q)
    others = remote(dg_all.at[pl.ds(0, group - 1)], dg_all.at[pl.ds(0, group - 1)], dg_send, dg_recv, mate)
    others.wait_recv()
    others.wait_send()
    dgain = dg_all[0]
    for j in range(1, group):
        dgain = dgain + dg_all[j]
    dgain_ref[...] = dgain
    for j in range(NS):
        u = n_all - NS + j
        for t in range(4):
            pl.semaphore_wait(credit.at[t, u % NS], 1 if t == 0 else 3)
            if t < 3:
                ag_all(u, t).wait_send()


BY_XLA = 2


def main_call(hidden, d_out, cos_tab, sin_tab, w_qkv, w_out, gain):
    n, loc, dim = hidden.shape
    group = 16
    rows = n * loc
    seqs = n // group
    seq = loc * group
    h = dim // 2
    n_all = 4 * dim // TW
    hbm = pl.BlockSpec(memory_space=pl.ANY)
    vmem = pl.BlockSpec(memory_space=pltpu.VMEM)
    D = pltpu.SemaphoreType.DMA
    S = jax.ShapeDtypeStruct
    V = pltpu.VMEM
    act = S((rows, dim), BF)
    return pl.pallas_call(
        functools.partial(main_kernel, 128 ** -0.5),
        in_specs=[hbm] * 2 + [vmem] * 2 + [hbm] * 2 + [vmem],
        out_specs=[hbm] * 11 + [vmem],
        out_shape=[S((dim, 4 * dim), F32), act, act, S((3, rows, dim), BF),
                   act, S((dim, rows), BF), S((3, rows, dim), BF), S((n, loc, dim), BF),
                   S((group, BY_XLA, loc, dim), BF), S((group, seqs - BY_XLA, loc, dim), BF), S((group, seqs - BY_XLA, loc, dim), BF), S((1, dim), F32)],
        scratch_shapes=[
            V((dim, rows), BF), V((2, 3, rows, TW), BF), V((NB, dim, TW), F32),
            V((NS, h, TW), F32), V((NS, h >> 1, TW), F32), V((NS, h >> 2, TW), F32), V((NS, h >> 3, TW), F32),
            V((2, 3, seq, TW), BF), V((2, seq, TW), BF), V((2, seq, TW), BF), V((2, TW, seq), BF), V((seq, 256), F32), V((loc, 256), F32),
            V((seq, dim), F32), V((seq, dim), BF), V((seq, dim), BF), V((group, loc, dim), BF), V((group, 1, dim), F32),
            V((2, dim, 512), BF), V((2, seq, 512), BF), V((2, seq // 2, dim), BF), V((dim // 512, group, loc, 512), BF),
            D, D, D((4, NS)), D((4, NS)), pltpu.SemaphoreType.REGULAR((4, NS)), D((NS,)), D((4, NS)), D((4, n_all)),
            D((2, 2)), D((3, 2)), D((3,)), D((3,)), D, D, D((2, 2)), D((2,)), D((2,)),
            D((seqs,)), D((seqs,)), D((seqs,)), D((seqs,)), D, D, D((2 * seqs,)), D((dim // 512,)), D((seqs,)), D((dim // 512,)), D((4 * (seqs - BY_XLA),)), D((4 * (seqs - BY_XLA),)),
        ],
        compiler_params=pltpu.CompilerParams(collective_id=0, has_side_effects=True, vmem_limit_bytes=67043328),
        cost_estimate=pl.CostEstimate(flops=28 * rows * dim * dim, bytes_accessed=90 * dim * dim, transcendentals=0),
        name="main",
    )(hidden, d_out, cos_tab, sin_tab, w_qkv, w_out, gain)


def place_kernel(y_in, b_in, y_out, dh_out):
    y_out[...] = y_in[...]
    dh_out[...] = b_in[...]


def place_call(y, b):
    n, loc, dim = y.shape
    group, k = b.shape[:2]
    seqs = n // group
    return pl.pallas_call(
        place_kernel,
        grid=(4,),
        in_specs=[pl.BlockSpec((n // 4, loc, dim), lambda j: (j, 0, 0)), pl.BlockSpec((group // 4, k, loc, dim), lambda j: (j, 0, 0, 0))],
        out_specs=[pl.BlockSpec((n // 4, loc, dim), lambda j: (j, 0, 0)), pl.BlockSpec((group // 4, k, loc, dim), lambda j: (j, seqs // k - 1, 0, 0))],
        out_shape=[jax.ShapeDtypeStruct((n, loc, dim), BF), jax.ShapeDtypeStruct((group, seqs, loc, dim), BF)],
        cost_estimate=pl.CostEstimate(flops=8 * n * loc * dim, bytes_accessed=6 * n * loc * dim, transcendentals=0),
        name="place",
    )(y, b)


def fill_kernel(a_in, dh_in, dh_out):
    dh_out[...] = a_in[...]


def fill_call(a, dh):
    group, k, loc, dim = a.shape
    return pl.pallas_call(
        fill_kernel,
        grid=(4,),
        in_specs=[pl.BlockSpec((group // 4, k, loc, dim), lambda j: (j, 0, 0, 0)), pl.BlockSpec(memory_space=pl.ANY)],
        out_specs=pl.BlockSpec((group // 4, k, loc, dim), lambda j: (j, 0, 0, 0)),
        out_shape=jax.ShapeDtypeStruct(dh.shape, BF),
        input_output_aliases={1: 0},
        name="fill",
    )(a, dh)


def solution(mesh):
    group = mesh.shape['sp']
    token_spec = P(None, 'sp', None)
    table_spec = P('sp', None)

    def device_step(hidden, norm_gain, w_qkv, w_out, cos_tab, sin_tab, d_out):
        num_seqs, local_len, dim = hidden.shape
        gain = norm_gain.reshape(1, dim)
        dw, _, _, _, _, _, _, y, dh_a, _, dh_b, dgain = main_call(hidden, d_out, cos_tab, sin_tab, w_qkv, w_out, gain)
        dh_a = lax.all_to_all(dh_a, 'sp', split_axis=0, concat_axis=0, tiled=True)
        y, dh = place_call(y, dh_b)
        dh = fill_call(dh_a, dh).reshape(num_seqs, local_len, dim)
        return y, dh, dw[:, :3 * dim], dw[:, 3 * dim:], dgain.reshape(dim)

    return jax.shard_map(device_step, mesh=mesh, in_specs=(token_spec, P(), P(), P(), table_spec, table_spec, token_spec), out_specs=(token_spec, token_spec, P(), P(), P()), check_vma=False)
```

```python
import functools
import jax
import jax.numpy as jnp
from jax import lax
from jax.experimental import pallas as pl
from jax.experimental.pallas import tpu as pltpu
from jax.sharding import PartitionSpec as P

NORM_EPS = 1e-6
BF = jnp.bfloat16
F32 = jnp.float32
VMEM_LIMIT = 60 * 1024 * 1024


def dot_nn(a, b):
    return lax.dot_general(a, b, (((1,), (0,)), ((), ())), preferred_element_type=F32)


def dot_nt(a, b):
    return lax.dot_general(a, b, (((1,), (1,)), ((), ())), preferred_element_type=F32)


def rotate(u, cos, sin_signed):
    return u * cos + pltpu.roll(u, 64, 1) * sin_signed


def unrotate(u, cos, sin_signed):
    return u * cos - pltpu.roll(u, 64, 1) * sin_signed


MESH = pl.DeviceIdType.MESH


def flipped(me, j):
    p = me
    for b in range(4):
        w = 1 << b
        if j & w:
            p = p + w * (1 - 2 * ((me // w) % 2))
    return p


ORDER = tuple(int(j, 16) for j in '2481359' + '6ac7bdef')


TW = 256
PARTS = ((0, 384), (384, 320), (704, 320))
NS = 3
NB = 6
BLK = 256


def attend(scale, qkv, do, tabs, o_out, o_t_out, dproj_out):
    seq = qkv.shape[1]
    for h in range(2):
        cols = slice(h * 128, (h + 1) * 128)
        q = qkv[0, :, cols]
        k = qkv[1, :, cols]
        v = qkv[2, :, cols]
        dout = do[:, cols]
        k_t = k.T
        v_t = v.T
        dk = [None] * (seq // BLK)
        dv = [None] * (seq // BLK)
        for j in range(seq // BLK):
            end = (j + 1) * BLK
            rows = slice(j * BLK, end)
            q_j = q[rows]
            do_j = dout[rows]
            s = dot_nt(k[:end], q_j)
            row = lax.broadcasted_iota(jnp.int32, (end, BLK), 0)
            col = lax.broadcasted_iota(jnp.int32, (end, BLK), 1) + j * BLK
            s = jnp.where(row <= col, s * scale, -1e30)
            m = jnp.max(s, axis=0, keepdims=True)
            e = jnp.exp(s - m)
            p = e * (1.0 / jnp.sum(e, axis=0, keepdims=True))
            p_bf = p.astype(BF)
            o_t = dot_nn(v_t[:, :end], p_bf)
            dp = dot_nt(v[:end], do_j).astype(BF).astype(F32)
            delta = jnp.sum(p * dp, axis=0, keepdims=True)
            ds = (p * (dp - delta) * scale).astype(BF)
            dv_j = dot_nn(p_bf, do_j)
            dk_j = dot_nn(ds, q_j)
            dq_t = dot_nn(k_t[:, :end], ds)
            for i in range(j + 1):
                part = slice(i * BLK, (i + 1) * BLK)
                dv[i] = dv_j[part] if dv[i] is None else dv[i] + dv_j[part]
                dk[i] = dk_j[part] if dk[i] is None else dk[i] + dk_j[part]
            o_out[rows, cols] = o_t.T.astype(BF)
            o_t_out[cols, rows] = o_t.astype(BF)
            dq = dq_t.T.astype(BF).astype(F32)
            dproj_out[0, rows, cols] = unrotate(dq, tabs[rows, :128], tabs[rows, 128:]).astype(BF)
        for j in range(seq // BLK):
            rows = slice(j * BLK, (j + 1) * BLK)
            dkj = dk[j].astype(BF).astype(F32)
            dproj_out[1, rows, cols] = unrotate(dkj, tabs[rows, :128], tabs[rows, 128:]).astype(BF)
            dproj_out[2, rows, cols] = dv[j].astype(BF)


def main_kernel(scale, hidden, d_out, cos_ref, sin_ref, w_qkv, w_out, gain_ref,
                g_hbm, h_seq, do_seq, qkv, o_hbm, o_t_hbm, dproj_hbm, y_all, dh_hbm, dh_loc, dh_all, dgain_ref,
                lhs, dproj_v, acc, r0, r1, r2, r3, qkv_v, do_v, o_v, o_t_v, tabs, tab, dn_acc, h_v, dout_v, dh_v, dg_all, wbuf, pbuf, o_c, y_t,
                lhs_sem, ld_sem, s_send, s_recv, credit, loc_sem, g_send, g_recv,
                in_sem, out_sem, rhs_sem, dh_sem, dg_send, dg_recv, w_sem, o_sem, c0_sem,
                h_send, h_recv, d_send, d_recv, t_send, t_recv, own_sem, y_send, y_recv, y_own, x_send, x_recv):
    me = lax.axis_index('sp')
    group = 16
    loc, dim = hidden.shape[1:]
    seqs = hidden.shape[0] // group
    seq = loc * group
    half = dim // 2
    n_qkv = 3 * dim // TW
    n_all = 4 * dim // TW
    pairs = dim // TW
    core = me % 2
    mate = me + 1 - 2 * core
    recv = (r0, r1, r2, r3)
    TN = 512
    per = dim // TN

    def remote(src, dst, ss, rs, peer):
        return pltpu.make_async_remote_copy(src_ref=src, dst_ref=dst, send_sem=ss, recv_sem=rs, device_id=(peer,), device_id_type=MESH)

    def link(d):
        w = 2 + d + d * d
        bit = (me // w) % 2
        return bit, me + w * (1 - 2 * bit)

    def aligned(x, n):
        return pl.multiple_of(x, n)

    def dims(u, p, t):
        return (u + p + t - 1) % 3

    def offs(u, p, size):
        o = [0]
        for t in (1, 2, 3):
            b, _ = link(dims(u, p, t))
            o.append(o[-1] + b * (size >> t))
        return o

    def rs_all(u, t):
        sl = u % NS
        return remote(recv[t].at[sl], recv[t].at[sl], s_send.at[t, sl], s_recv.at[t, sl], mate)

    def rs_start(u, t):
        sl, nb = u % NS, u % NB

        @pl.when(u >= NS)
        def _():
            pl.semaphore_wait(credit.at[t, sl], 1 if t == 0 else 3)

        if t == 0:
            n = half // 4
            for k in range(4):
                src = acc.at[nb, pl.ds(aligned((1 - core) * half + k * n, n), n)]
                remote(src, r0.at[sl, pl.ds(k * n, n)], s_send.at[0, sl], s_recv.at[0, sl], mate).start()
            return
        for p, (base, size) in enumerate(PARTS):
            o = offs(u, p, size)
            n = size >> t
            b, peer = link(dims(u, p, t))
            row = core * half + base + o[t - 1] + (1 - b) * n
            remote(acc.at[nb, pl.ds(aligned(row, 8), n)], recv[t].at[sl, pl.ds(base >> t, n)],
                   s_send.at[t, sl], s_recv.at[t, sl], peer).start()

    def rs_finish(u, t):
        sl, nb = u % NS, u % NB
        rs_all(u, t).wait_recv()
        rs_all(u, t).wait_send()
        if t == 0:
            rows = pl.ds(aligned(core * half, half), half)
            acc[nb, rows] = acc[nb, rows] + r0[sl]
            pl.semaphore_signal(credit.at[0, sl], inc=1, device_id=(mate,), device_id_type=MESH)
            return
        for p, (base, size) in enumerate(PARTS):
            n = size >> t
            rows = pl.ds(aligned(core * half + base + offs(u, p, size)[t], 8), n)
            acc[nb, rows] = acc[nb, rows] + recv[t][sl, pl.ds(base >> t, n)]
            pl.semaphore_signal(credit.at[t, sl], inc=1, device_id=(link(dims(u, p, t))[1],), device_id_type=MESH)

    def tile_col(u):
        return jnp.where(u < n_qkv, (u % 3) * pairs + u // 3, u) * TW

    def g_at(u, row, n):
        return g_hbm.at[pl.ds(aligned(row, 8), n), pl.ds(aligned(tile_col(u), TW), TW)]

    def ag_all(u, t):
        r = g_hbm.at[pl.ds(0, half >> t), pl.ds(0, TW)]
        return remote(r, r, g_send.at[t, u % NS], g_recv.at[t, u], mate)

    def ag_start(u, t):
        if t < 3:
            @pl.when(u >= NS)
            def _():
                ag_all(u, t).wait_send()

        if t == 0:
            r = g_at(u, core * half, half)
            remote(r, r, g_send.at[0, u % NS], g_recv.at[0, u], mate).start()
            return
        for p, (base, size) in enumerate(PARTS):
            n = size >> t
            row = core * half + base + offs(u, p, size)[t]
            dst = g_at(u, row, n)
            src = acc.at[u % NB, pl.ds(aligned(row, 8), n)] if t == 3 else dst
            remote(src, dst, g_send.at[t, u % NS], g_recv.at[t, u], link(dims(u, p, t))[1]).start()

    def local_start(u):
        for p, (base, size) in enumerate(PARTS):
            n = size >> 3
            row = core * half + base + offs(u, p, size)[3]
            pltpu.make_async_copy(acc.at[u % NB, pl.ds(aligned(row, 8), n)], g_at(u, row, n), loc_sem.at[u % NS]).start()

    def local_wait(u):
        n = half >> 3
        pltpu.make_async_copy(acc.at[0, pl.ds(0, n)], g_hbm.at[pl.ds(0, n), pl.ds(0, TW)], loc_sem.at[u % NS]).wait()

    n_attn = seqs * pairs
    n_early = pairs + 2 * (seqs - 1)

    def place(a):
        b, c = a - pairs, a - n_early
        s = jnp.where(a < pairs, 0, 1 + jnp.where(c < 0, b // 2, c % (seqs - 1)))
        p = jnp.where(a < pairs, a, jnp.where(c < 0, b % 2, 2 + c // (seqs - 1)))
        return s, p, seq_rows(s), pl.ds(aligned(p * TW, TW), TW)

    def seq_rows(c):
        return pl.ds(aligned(c * seq, seq), seq)

    def attn_in(a, fn):
        _, _, rows, cols = place(a)
        sl = a % 2
        fn(pltpu.make_async_copy(qkv.at[:, rows, cols], qkv_v.at[sl], in_sem.at[0, sl]))
        fn(pltpu.make_async_copy(w_out.at[cols], o_c.at[sl], in_sem.at[1, sl]))

    def start(copy):
        copy.start()

    def wait(copy):
        copy.wait()

    def dproj_rows(a):
        s, p, _, _ = place(a)
        return dproj_v.at[p % 2, :, seq_rows(jnp.where(jnp.logical_and(s == 0, p >= 2), seqs - 1, s))]

    def attn_out(a):
        _, _, rows, cols = place(a)
        sl = a % 2
        return (pltpu.make_async_copy(o_v.at[sl], o_hbm.at[rows, cols], out_sem.at[0, sl]),
                pltpu.make_async_copy(o_t_v.at[sl], o_t_hbm.at[cols, rows], out_sem.at[1, sl]),
                pltpu.make_async_copy(dproj_rows(a), dproj_hbm.at[:, rows, cols], out_sem.at[2, sl]))

    def attn_out_wait(a):
        for c in attn_out(a):
            c.wait()

    def attn_step(a):
        @pl.when(jnp.logical_and(a != pairs - 1, a + 1 < n_attn))
        def _():
            attn_in(a + 1, start)

        attn_in(a, wait)

        @pl.when(jnp.logical_and(a >= 2, a // 2 != pairs // 2))
        def _():
            attn_out_wait(a)

        s, _, _, _ = place(a)
        sl = a % 2

        @pl.when(s == 0)
        def _():
            do_v[sl] = dot_nt(h_v[...], o_c[sl]).astype(BF)

        @pl.when(jnp.logical_and(s > 0, s < seqs - 1))
        def _():
            total = None
            for n in range(per):
                cols = slice(n * TN, (n + 1) * TN)
                part = dot_nt(wbuf[s - 1, cols], o_c[sl, :, cols])
                total = part if total is None else total + part
            do_v[sl] = total.astype(BF)

        @pl.when(s == seqs - 1)
        def _():
            do_v[sl] = dot_nt(dh_v[...].reshape(seq, dim), o_c[sl]).astype(BF)

        attend(scale, qkv_v.at[sl], do_v.at[sl], tabs, o_v.at[sl], o_t_v.at[sl], dproj_rows(a))
        for c in attn_out(a):
            c.start()

    def first_seq(p):
        rows = seq_rows(0)
        return pltpu.make_async_copy(dproj_hbm.at[:, rows, pl.ds(aligned(p * TW, TW), TW)], dproj_v.at[p % 2, :, rows], c0_sem.at[p % 2])

    def rhs_copy(u):
        j = u - n_qkv
        return pltpu.make_async_copy(do_seq.at[:, pl.ds(aligned(j * TW, TW), TW)], dproj_v.at[0, j % 3], rhs_sem.at[j % 3])

    def dw_tile(u):
        @pl.when(u == n_qkv)
        def _():
            pltpu.make_async_copy(o_t_hbm, lhs, lhs_sem).wait()

        @pl.when(u >= n_qkv)
        def _():
            rhs_copy(u).wait()

        @pl.when(jnp.logical_and(u % 3 == 0, jnp.logical_and(u >= 6, u < n_qkv)))
        def _():
            first_seq(u // 3).wait()

        p = jnp.where(u < n_qkv, (u // 3) % 2, 0)

        def half_tile(mine):
            @pl.loop(0, half // TN)
            def _(b):
                rows = pl.ds(aligned(mine * half + b * TN, TN), TN)
                acc[u % NB, rows] = dot_nn(lhs[rows], dproj_v[p, u % 3])

        half_tile(1 - core)
        rs_start(u, 0)
        half_tile(core)

        @pl.when(u == n_qkv - 1)
        def _():
            pltpu.make_async_copy(o_t_hbm, lhs, lhs_sem).start()

        @pl.when(jnp.logical_and(u + 2 >= n_qkv, u + 2 < n_all))
        def _():
            rhs_copy(u + 2).start()

    n_blocks = 4 * seqs

    def columns(n):
        return pl.ds(aligned(n * TN, TN), TN)

    def block(b):
        is_out = jnp.logical_or(b == 0, jnp.logical_and((b + 1) % 3 == 0, b <= 3 * seqs - 4))
        done = jnp.minimum((b + 1) // 3, seqs - 1)
        return is_out, done, b - 1 - done

    def tile_start(t):
        b, n, sl = t // per, t % per, t % 2
        is_out, c, q = block(b)

        @pl.when(is_out)
        def _():
            pltpu.make_async_copy(w_out.at[:, columns(n)], wbuf.at[sl], w_sem.at[0, sl]).start()
            pltpu.make_async_copy(h_seq.at[seq_rows(c), columns(n)], pbuf.at[sl], w_sem.at[1, sl]).start()

        @pl.when(jnp.logical_not(is_out))
        def _():
            pltpu.make_async_copy(w_qkv.at[:, columns((q % 3) * per + n)], wbuf.at[sl], w_sem.at[0, sl]).start()
            pltpu.make_async_copy(dproj_hbm.at[q % 3, seq_rows(q // 3), columns(n)], pbuf.at[sl], w_sem.at[1, sl]).start()

    def tile_wait(t):
        sl = t % 2
        pltpu.make_async_copy(w_out.at[:, columns(0)], wbuf.at[sl], w_sem.at[0, sl]).wait()
        pltpu.make_async_copy(h_seq.at[seq_rows(0), columns(0)], pbuf.at[sl], w_sem.at[1, sl]).wait()

    def o_load(c):
        n = seq // 2
        return [pltpu.make_async_copy(o_hbm.at[pl.ds(aligned(c * seq + k * n, n), n)], o_c.at[k], o_sem.at[k]) for k in range(2)]

    def y_sent(n):
        r = y_all.at[pl.ds(0, group - 1), :, columns(0)]
        return remote(r, r, y_send.at[n], y_recv.at[0], mate)

    def y_own_copy(c, n):
        return pltpu.make_async_copy(y_t.at[n, me], y_all.at[me * seqs + c, :, columns(n)], y_own.at[n])

    def out_tile(c, n, sl):
        y = pbuf[sl].astype(F32) + dot_nn(o_c[...].reshape(seq, dim), wbuf[sl])

        @pl.when(c > 0)
        def _():
            y_sent(n).wait_send()
            y_own_copy(0, n).wait()

        y_t[n] = y.astype(BF).reshape(group, loc, TN)
        for j in ORDER:
            peer = flipped(me, j)
            remote(y_t.at[n, peer], y_all.at[me * seqs + c, :, columns(n)], y_send.at[n], y_recv.at[c], peer).start()
        y_own_copy(c, n).start()

    def run_block(b):
        is_out, c_out, q = block(b)
        c, third = q // 3, q % 3

        @pl.when(is_out)
        def _():
            for x in o_load(c_out):
                x.wait()

        @pl.when(jnp.logical_and(jnp.logical_not(is_out), third == 2))
        def _():
            pltpu.make_async_copy(h_seq.at[seq_rows(c)], h_v, dh_sem.at[0]).start()
            pltpu.make_async_copy(do_seq.at[seq_rows(c)], dout_v, dh_sem.at[1]).start()

        @pl.loop(0, per)
        def _(n):
            t = b * per + n
            sl = t % 2

            @pl.when(jnp.logical_and(t != per - 1, t + 1 < n_blocks * per))
            def _():
                tile_start(t + 1)

            tile_wait(t)

            @pl.when(is_out)
            def _():
                out_tile(c_out, n, sl)

            @pl.when(jnp.logical_not(is_out))
            def _():
                part = dot_nt(pbuf[sl], wbuf[sl])
                first = jnp.logical_and(third == 0, n == 0)

                @pl.when(first)
                def _():
                    dn_acc[...] = part

                @pl.when(jnp.logical_not(first))
                def _():
                    dn_acc[...] += part

        @pl.when(jnp.logical_and(is_out, jnp.logical_and(c_out > 0, c_out + 1 < seqs)))
        def _():
            for x in o_load(c_out + 1):
                x.start()

        @pl.when(jnp.logical_and(jnp.logical_not(is_out), third == 2))
        def _():
            norm_back(c)

    def norm_back(c):
        pltpu.make_async_copy(h_seq.at[seq_rows(c)], h_v, dh_sem.at[0]).wait()
        pltpu.make_async_copy(do_seq.at[seq_rows(c)], dout_v, dh_sem.at[1]).wait()

        @pl.when(c > 0)
        def _():
            pltpu.make_async_copy(dh_v, dh_hbm.at[:, 0], dh_sem.at[2]).wait()

        gain = gain_ref[...].astype(F32).reshape(1, dim)

        @pl.loop(0, group)
        def _(b):
            r = pl.ds(aligned(b * loc, loc), loc)
            h = h_v[r].astype(F32)
            inv = lax.rsqrt(jnp.mean(h * h, axis=-1, keepdims=True) + NORM_EPS)
            dn = dn_acc[r].astype(BF).astype(F32)
            dg = jnp.sum(dn * h * inv, axis=0, keepdims=True)
            ds = dn * gain
            dh = dout_v[r].astype(F32) + inv * ds - h * (inv * inv * inv) * jnp.mean(ds * h, axis=-1, keepdims=True)
            dh_v[b] = dh.astype(BF)
            first = jnp.logical_and(c == 0, b == 0)

            @pl.when(first)
            def _():
                dg_all[me] = dg

            @pl.when(jnp.logical_not(first))
            def _():
                dg_all[me] += dg

        @pl.when(c < by_xla)
        def _():
            pltpu.make_async_copy(dh_v, dh_hbm.at[:, c], dh_sem.at[2]).start()

        @pl.when(c >= by_xla)
        def _():
            pltpu.make_async_copy(dh_v, dh_loc.at[:, c - by_xla], dh_sem.at[2]).start()

    def dh_send(q):
        k, cols = q // 4, pl.ds(aligned((q % 4) * (dim // 4), dim // 4), dim // 4)
        for j in ORDER:
            peer = flipped(me, j)
            remote(dh_loc.at[peer, k, :, cols], dh_all.at[me, k, :, cols], x_send.at[q], x_recv.at[q], peer).start()
        pltpu.make_async_copy(dh_loc.at[me, k, :, cols], dh_all.at[me, k, :, cols], own_sem.at[q]).start()

    def dh_wait(q):
        r = dh_all.at[pl.ds(0, group - 1), 0, :, pl.ds(0, dim // 4)]
        done = remote(r, r, x_send.at[q], x_recv.at[q], mate)
        done.wait_recv()
        done.wait_send()
        pltpu.make_async_copy(dh_loc.at[0, 0, :, pl.ds(0, dim // 4)], dh_all.at[0, 0, :, pl.ds(0, dim // 4)], own_sem.at[q]).wait()

    def my_rows(c):
        return pl.ds(aligned(c * seq + me * loc, loc), loc)

    def from_all(dst, ss, rs):
        r = dst.at[pl.ds(0, (group - 1) * loc)]
        return remote(r, r, ss, rs, mate)

    def send_all(src, dst, ss, rs, c):
        for j in ORDER:
            peer = flipped(me, j)
            to = dh_v.at[me] if dst is do_seq and c == seqs - 1 else dst.at[my_rows(c)]
            remote(src.at[peer * seqs + c], to, ss.at[c], rs.at[c], peer).start()

    def project(c):
        rows = seq_rows(c)
        from_all(h_seq, h_send.at[c], h_recv.at[c]).wait_recv()
        load = pltpu.make_async_copy(h_seq.at[rows], h_v, ld_sem)
        load.start()
        load.wait()
        gain = gain_ref[...].astype(F32).reshape(1, dim)
        blk = 128

        @pl.loop(0, seq // blk)
        def _(b):
            r = pl.ds(aligned(b * blk, blk), blk)
            h = h_v[r].astype(F32)
            inv = lax.rsqrt(jnp.mean(h * h, axis=-1, keepdims=True) + NORM_EPS)
            n = (h * inv * gain).astype(BF)
            dout_v[r] = n
            lhs[:, pl.ds(aligned(c * seq + b * blk, blk), blk)] = n.T

        @pl.loop(0, 3 * per)
        def _(n):
            t = c * 3 * per + n
            sl = t % 2

            @pl.when(t + 1 < seqs * 3 * per)
            def _():
                qkv_w(t + 1).start()

            qkv_w(t).wait()
            proj = dot_nn(dout_v[...], wbuf[sl])

            @pl.when(t >= 2)
            def _():
                qkv_out(t).wait()

            @pl.when(n < 2 * per)
            def _():
                for h in range(TN // 128):
                    cols = slice(h * 128, (h + 1) * 128)
                    pbuf[sl, :, cols] = rotate(proj[:, cols], tabs[:, :128], tabs[:, 128:]).astype(BF)

            @pl.when(n >= 2 * per)
            def _():
                pbuf[sl] = proj.astype(BF)

            qkv_out(t).start()

    def qkv_w(t):
        return pltpu.make_async_copy(w_qkv.at[:, columns(t % (3 * per))], wbuf.at[t % 2], w_sem.at[0, t % 2])

    def qkv_out(t):
        n = t % (3 * per)
        return pltpu.make_async_copy(pbuf.at[t % 2], qkv.at[n // per, seq_rows(t // (3 * per)), columns(n % per)], w_sem.at[1, t % 2])

    def gradient_in():
        for t in range(2):
            qkv_out(t).wait()
        attn_in(0, start)
        for c in range(seqs - 1):
            from_all(do_seq, d_send.at[c], d_recv.at[c]).wait_recv()
            rows = seq_rows(c)
            if c == 0:
                loads = [pltpu.make_async_copy(do_seq.at[rows], h_v, ld_sem)]
            else:
                loads = [pltpu.make_async_copy(do_seq.at[rows, pl.ds(n * TN, TN)], wbuf.at[c - 1, pl.ds(n * TN, TN)], x_send.at[n]) for n in range(per)]
            for x in loads:
                x.start()
            for x in loads:
                x.wait()
            if c == 0:
                pl.loop(0, pairs)(attn_step)
                attn_out_wait(pairs - 2)
                attn_out_wait(pairs - 1)
                for x in o_load(0):
                    x.start()
                tile_start(0)
                run_block(0)
                attn_in(pairs, start)
            else:
                pl.loop(pairs + 2 * c - 2, pairs + 2 * c)(attn_step)
        from_all(do_seq, d_send.at[seqs - 1], d_recv.at[seqs - 1]).wait_recv()
        last_copy().start()
        attn_step(n_early - 2)

    def last_copy():
        dst = do_seq.at[seq_rows(seqs - 1)]
        return pltpu.make_async_copy(dh_v, dst.reshape(group, loc, dim), ld_sem)

    by_xla = dh_hbm.shape[1]

    def own_in(k):
        src = hidden if k < seqs else d_out
        to = dh_v.at[me] if k == 2 * seqs - 1 else dout_v.at[pl.ds(k * loc, loc)]
        return pltpu.make_async_copy(src.at[me * seqs + k % seqs], to, own_sem.at[k])

    def own_out(k):
        dst = h_seq if k < seqs else do_seq
        return pltpu.make_async_copy(dout_v.at[pl.ds(k * loc, loc)], dst.at[my_rows(k % seqs)], own_sem.at[k])

    for k in range(2 * seqs):
        own_in(k).start()
    cos, sin = cos_ref[...], sin_ref[...]
    tab[...] = jnp.concatenate([cos, cos, -sin, sin], axis=1)
    barrier = pltpu.get_barrier_semaphore()
    for j in range(1, group):
        pl.semaphore_signal(barrier, inc=1, device_id=(flipped(me, j),), device_id_type=MESH)
    pl.semaphore_wait(barrier, group - 1)
    mine = pl.ds(aligned(me * loc, loc), loc)
    for j in ORDER:
        remote(tab, tabs.at[mine], t_send, t_recv, flipped(me, j)).start()
    for c in range(seqs):
        send_all(hidden, h_seq, h_send, h_recv, c)
    for c in range(seqs):
        send_all(d_out, do_seq, d_send, d_recv, c)
    for k in range(2 * seqs):
        own_in(k).wait()
        if k < 2 * seqs - 1:
            own_out(k).start()
    tabs[mine] = tab[...]
    from_all(tabs, t_send, t_recv).wait_recv()
    for k in range(2 * seqs - 1):
        own_out(k).wait()
    qkv_w(0).start()
    pl.loop(0, seqs)(project)
    gradient_in()

    first_out = 3 * (pairs - 1)
    first_dn = first_out + seqs

    def step(i, carry):
        def guarded(lag, fn):
            u = i - lag

            @pl.when(jnp.logical_and(u >= 0, u < n_all))
            def _():
                fn(u)

        def ag0(u):
            ag_all(u, 0).wait_recv()

        def ag1(u):
            ag_all(u, 1).wait_recv()
            ag_start(u, 0)

        def ag2(u):
            ag_all(u, 2).wait_recv()
            ag_start(u, 1)

        def ag3(u):
            ag_all(u, 3).wait_recv()
            ag_all(u, 3).wait_send()
            local_wait(u)
            ag_start(u, 2)

        def last(u):
            rs_finish(u, 3)
            local_start(u)
            ag_start(u, 3)

        def middle(t):
            def fn(u):
                rs_finish(u, t)
                rs_start(u, t + 1)
            return fn

        guarded(0, dw_tile)

        from_a, to_a = [n_early - 1 + jnp.where(k > 2, k - 1, 0) for k in (i, i + 1)]

        @pl.when(jnp.logical_and(i % 3 == 0, jnp.logical_and(i >= 3, i < first_out)))
        def _():
            first_seq(i // 3 + 1).start()

        @pl.when(i < first_out)
        def _():
            pl.loop(from_a, jnp.minimum(to_a, n_attn))(attn_step)

        for lag, fn in enumerate((middle(0), middle(1), middle(2), last, ag3, ag2, ag1, ag0)):
            guarded(lag + 1, fn)

        @pl.when(i == first_out)
        def _():
            attn_out_wait(n_attn - 2)
            attn_out_wait(n_attn - 1)
            for x in o_load(1):
                x.start()
            tile_start(per)

        def blocks(i):
            k = i - first_out
            return jnp.where(k <= seqs, jnp.maximum(3 * k - 1, 1), jnp.minimum(k + 2 * seqs, n_blocks))

        @pl.when(i >= first_out)
        def _():
            pl.loop(blocks(i), blocks(i + 1))(run_block)

        @pl.when(i == 3)
        def _():
            last_copy().wait()

        first_dh = first_dn + seqs

        @pl.when(i == first_dh)
        def _():
            pltpu.make_async_copy(dh_v, dh_hbm.at[:, 0], dh_sem.at[2]).wait()
            for j in range(1, group):
                remote(dg_all.at[me], dg_all.at[me], dg_send, dg_recv, flipped(me, j)).start()

        @pl.when(jnp.logical_and(i >= first_dh, i < first_dh + 4 * (seqs - by_xla)))
        def _():
            dh_send(i - first_dh)

        return carry

    lax.fori_loop(0, n_all + 8, step, 0)

    for c in range(seqs):
        r = y_all.at[pl.ds(0, group - 1)]
        remote(r, r, y_send.at[0], y_recv.at[c], mate).wait_recv()
        from_all(h_seq, h_send.at[c], h_recv.at[c]).wait_send()
        from_all(do_seq, d_send.at[c], d_recv.at[c]).wait_send()
    for n in range(per):
        y_sent(n).wait_send()
        y_own_copy(0, n).wait()
    from_all(tabs, t_send, t_recv).wait_send()
    for q in range(4 * (seqs - by_xla)):
        dh_wait(q)
    others = remote(dg_all.at[pl.ds(0, group - 1)], dg_all.at[pl.ds(0, group - 1)], dg_send, dg_recv, mate)
    others.wait_recv()
    others.wait_send()
    dgain = dg_all[0]
    for j in range(1, group):
        dgain = dgain + dg_all[j]
    dgain_ref[...] = dgain.reshape(dim)
    for j in range(NS):
        u = n_all - NS + j
        for t in range(4):
            pl.semaphore_wait(credit.at[t, u % NS], 1 if t == 0 else 3)
            if t < 3:
                ag_all(u, t).wait_send()


BY_XLA = 2


def main_call(hidden, d_out, cos_tab, sin_tab, w_qkv, w_out, gain):
    n, loc, dim = hidden.shape
    group = 16
    rows = n * loc
    seqs = n // group
    seq = loc * group
    h = dim // 2
    n_all = 4 * dim // TW
    hbm = pl.BlockSpec(memory_space=pl.ANY)
    vmem = pl.BlockSpec(memory_space=pltpu.VMEM)
    D = pltpu.SemaphoreType.DMA
    S = jax.ShapeDtypeStruct
    V = pltpu.VMEM
    act = S((rows, dim), BF)
    return pl.pallas_call(
        functools.partial(main_kernel, 128 ** -0.5),
        in_specs=[hbm] * 2 + [vmem] * 2 + [hbm] * 2 + [vmem],
        out_specs=[hbm] * 11 + [vmem],
        out_shape=[S((dim, 4 * dim), F32), act, act, S((3, rows, dim), BF),
                   act, S((dim, rows), BF), S((3, rows, dim), BF), S((n, loc, dim), BF),
                   S((group, BY_XLA, loc, dim), BF), S((group, seqs - BY_XLA, loc, dim), BF), S((group, seqs - BY_XLA, loc, dim), BF), S((dim,), F32)],
        scratch_shapes=[
            V((dim, rows), BF), V((2, 3, rows, TW), BF), V((NB, dim, TW), F32),
            V((NS, h, TW), F32), V((NS, h >> 1, TW), F32), V((NS, h >> 2, TW), F32), V((NS, h >> 3, TW), F32),
            V((2, 3, seq, TW), BF), V((2, seq, TW), BF), V((2, seq, TW), BF), V((2, TW, seq), BF), V((seq, 256), F32), V((loc, 256), F32),
            V((seq, dim), F32), V((seq, dim), BF), V((seq, dim), BF), V((group, loc, dim), BF), V((group, 1, dim), F32),
            V((2, dim, 512), BF), V((2, seq, 512), BF), V((2, seq // 2, dim), BF), V((dim // 512, group, loc, 512), BF),
            D, D, D((4, NS)), D((4, NS)), pltpu.SemaphoreType.REGULAR((4, NS)), D((NS,)), D((4, NS)), D((4, n_all)),
            D((2, 2)), D((3, 2)), D((3,)), D((3,)), D, D, D((2, 2)), D((2,)), D((2,)),
            D((seqs,)), D((seqs,)), D((seqs,)), D((seqs,)), D, D, D((2 * seqs,)), D((dim // 512,)), D((seqs,)), D((dim // 512,)), D((4 * (seqs - BY_XLA),)), D((4 * (seqs - BY_XLA),)),
        ],
        compiler_params=pltpu.CompilerParams(collective_id=0, has_side_effects=True, vmem_limit_bytes=67043328),
        cost_estimate=pl.CostEstimate(flops=28 * rows * dim * dim, bytes_accessed=90 * dim * dim, transcendentals=0),
        name="main",
    )(hidden, d_out, cos_tab, sin_tab, w_qkv, w_out, gain)


def place_kernel(y_in, b_in, y_out, dh_out):
    y_out[...] = y_in[...]
    dh_out[...] = b_in[...]


def place_call(y, b):
    n, loc, dim = y.shape
    group, k = b.shape[:2]
    seqs = n // group
    return pl.pallas_call(
        place_kernel,
        grid=(4,),
        in_specs=[pl.BlockSpec((n // 4, loc, dim), lambda j: (j, 0, 0)), pl.BlockSpec((group // 4, k, loc, dim), lambda j: (j, 0, 0, 0))],
        out_specs=[pl.BlockSpec((n // 4, loc, dim), lambda j: (j, 0, 0)), pl.BlockSpec((group // 4, k, loc, dim), lambda j: (j, seqs // k - 1, 0, 0))],
        out_shape=[jax.ShapeDtypeStruct((n, loc, dim), BF), jax.ShapeDtypeStruct((group, seqs, loc, dim), BF)],
        cost_estimate=pl.CostEstimate(flops=8 * n * loc * dim, bytes_accessed=6 * n * loc * dim, transcendentals=0),
        name="place",
    )(y, b)


def fill_kernel(a_in, dh_in, dh_out):
    dh_out[...] = a_in[...]


def fill_call(a, dh):
    group, k, loc, dim = a.shape
    return pl.pallas_call(
        fill_kernel,
        grid=(4,),
        in_specs=[pl.BlockSpec((group // 4, k, loc, dim), lambda j: (j, 0, 0, 0)), pl.BlockSpec(memory_space=pl.ANY)],
        out_specs=pl.BlockSpec((group // 4, k, loc, dim), lambda j: (j, 0, 0, 0)),
        out_shape=jax.ShapeDtypeStruct(dh.shape, BF),
        input_output_aliases={1: 0},
        name="fill",
    )(a, dh)


def solution(mesh):
    group = mesh.shape['sp']
    token_spec = P(None, 'sp', None)
    table_spec = P('sp', None)

    def device_step(hidden, norm_gain, w_qkv, w_out, cos_tab, sin_tab, d_out):
        num_seqs, local_len, dim = hidden.shape
        dw, _, _, _, _, _, _, y, dh_a, _, dh_b, dgain = main_call(hidden, d_out, cos_tab, sin_tab, w_qkv, w_out, norm_gain)
        dh_a = lax.all_to_all(dh_a, 'sp', split_axis=0, concat_axis=0, tiled=True)
        y, dh = place_call(y, dh_b)
        dh = fill_call(dh_a, dh).reshape(num_seqs, local_len, dim)
        return y, dh, dw[:, :3 * dim], dw[:, 3 * dim:], dgain

    return jax.shard_map(device_step, mesh=mesh, in_specs=(token_spec, P(), P(), P(), table_spec, table_spec, token_spec), out_specs=(token_spec, token_spec, P(), P(), P()), check_vma=False)
```

```python
import functools
import jax
import jax.numpy as jnp
from jax import lax
from jax.experimental import pallas as pl
from jax.experimental.pallas import tpu as pltpu
from jax.sharding import PartitionSpec as P

NORM_EPS = 1e-6
HEAD = 128
BF = jnp.bfloat16
F32 = jnp.float32
VMEM_LIMIT = 60 * 1024 * 1024


def dot_nn(a, b):
    return lax.dot_general(a, b, (((1,), (0,)), ((), ())), preferred_element_type=F32)


def dot_nt(a, b):
    return lax.dot_general(a, b, (((1,), (1,)), ((), ())), preferred_element_type=F32)


def rotate(u, cos, sin_signed):
    return u * cos + pltpu.roll(u, 64, 1) * sin_signed


def unrotate(u, cos, sin_signed):
    return u * cos - pltpu.roll(u, 64, 1) * sin_signed


MESH = pl.DeviceIdType.MESH


def flipped(me, j):
    p = me
    for b in range(4):
        w = 1 << b
        if j & w:
            p = p + w * (1 - 2 * ((me // w) % 2))
    return p


ORDER = tuple(int(j, 16) for j in '2481359' + '6ac7bdef')


TW = 256
PARTS = ((0, 384), (384, 320), (704, 320))
NS = 3
NB = 6
BLK = 256


def attend(scale, qkv, do, tabs, o_out, o_t_out, dproj_out):
    seq = qkv.shape[1]
    for h in range(2):
        cols = slice(h * 128, (h + 1) * 128)
        q = qkv[0, :, cols]
        k = qkv[1, :, cols]
        v = qkv[2, :, cols]
        dout = do[:, cols]
        k_t = k.T
        v_t = v.T
        dk = [None] * (seq // BLK)
        dv = [None] * (seq // BLK)
        for j in range(seq // BLK):
            end = (j + 1) * BLK
            rows = slice(j * BLK, end)
            q_j = q[rows]
            do_j = dout[rows]
            s = dot_nt(k[:end], q_j)
            row = lax.broadcasted_iota(jnp.int32, (end, BLK), 0)
            col = lax.broadcasted_iota(jnp.int32, (end, BLK), 1) + j * BLK
            s = jnp.where(row <= col, s * scale, -1e30)
            m = jnp.max(s, axis=0, keepdims=True)
            e = jnp.exp(s - m)
            p = e * (1.0 / jnp.sum(e, axis=0, keepdims=True))
            p_bf = p.astype(BF)
            o_t = dot_nn(v_t[:, :end], p_bf)
            dp = dot_nt(v[:end], do_j).astype(BF).astype(F32)
            delta = jnp.sum(p * dp, axis=0, keepdims=True)
            ds = (p * (dp - delta) * scale).astype(BF)
            dv_j = dot_nn(p_bf, do_j)
            dk_j = dot_nn(ds, q_j)
            dq_t = dot_nn(k_t[:, :end], ds)
            for i in range(j + 1):
                part = slice(i * BLK, (i + 1) * BLK)
                dv[i] = dv_j[part] if dv[i] is None else dv[i] + dv_j[part]
                dk[i] = dk_j[part] if dk[i] is None else dk[i] + dk_j[part]
            o_out[rows, cols] = o_t.T.astype(BF)
            o_t_out[cols, rows] = o_t.astype(BF)
            dq = dq_t.T.astype(BF).astype(F32)
            dproj_out[0, rows, cols] = unrotate(dq, tabs[rows, :HEAD], tabs[rows, HEAD:]).astype(BF)
        for j in range(seq // BLK):
            rows = slice(j * BLK, (j + 1) * BLK)
            dkj = dk[j].astype(BF).astype(F32)
            dproj_out[1, rows, cols] = unrotate(dkj, tabs[rows, :HEAD], tabs[rows, HEAD:]).astype(BF)
            dproj_out[2, rows, cols] = dv[j].astype(BF)


def main_kernel(scale, hidden, d_out, cos_ref, sin_ref, w_qkv, w_out, gain_ref,
                g_hbm, h_seq, do_seq, qkv, o_hbm, o_t_hbm, dproj_hbm, y_all, dh_hbm, dh_loc, dh_all, dgain_ref,
                lhs, dproj_v, acc, r0, r1, r2, r3, qkv_v, do_v, o_v, o_t_v, tabs, tab, tab_all, dn_acc, h_v, dout_v, dh_v, dg_all, wbuf, pbuf, o_c, y_t,
                lhs_sem, ld_sem, s_send, s_recv, credit, loc_sem, g_send, g_recv,
                in_sem, out_sem, rhs_sem, dh_sem, dg_send, dg_recv, w_sem, o_sem, c0_sem,
                h_send, h_recv, d_send, d_recv, t_send, t_recv, own_sem, y_send, y_recv, y_own, x_send, x_recv):
    me = lax.axis_index('sp')
    group = 16
    loc, dim = hidden.shape[1:]
    seqs = hidden.shape[0] // group
    seq = loc * group
    half = dim // 2
    n_qkv = 3 * dim // TW
    n_all = 4 * dim // TW
    pairs = dim // TW
    core = me % 2
    mate = me + 1 - 2 * core
    recv = (r0, r1, r2, r3)
    TN = 512
    per = dim // TN

    def remote(src, dst, ss, rs, peer):
        return pltpu.make_async_remote_copy(src_ref=src, dst_ref=dst, send_sem=ss, recv_sem=rs, device_id=(peer,), device_id_type=MESH)

    def link(d):
        w = 2 + d + d * d
        bit = (me // w) % 2
        return bit, me + w * (1 - 2 * bit)

    def aligned(x, n):
        return pl.multiple_of(x, n)

    def dims(u, p, t):
        return (u + p + t - 1) % 3

    def offs(u, p, size):
        o = [0]
        for t in (1, 2, 3):
            b, _ = link(dims(u, p, t))
            o.append(o[-1] + b * (size >> t))
        return o

    def rs_all(u, t):
        sl = u % NS
        return remote(recv[t].at[sl], recv[t].at[sl], s_send.at[t, sl], s_recv.at[t, sl], mate)

    def rs_start(u, t):
        sl, nb = u % NS, u % NB

        @pl.when(u >= NS)
        def _():
            pl.semaphore_wait(credit.at[t, sl], 1 if t == 0 else 3)

        if t == 0:
            n = half // 4
            for k in range(4):
                src = acc.at[nb, pl.ds(aligned((1 - core) * half + k * n, n), n)]
                remote(src, r0.at[sl, pl.ds(k * n, n)], s_send.at[0, sl], s_recv.at[0, sl], mate).start()
            return
        for p, (base, size) in enumerate(PARTS):
            o = offs(u, p, size)
            n = size >> t
            b, peer = link(dims(u, p, t))
            row = core * half + base + o[t - 1] + (1 - b) * n
            remote(acc.at[nb, pl.ds(aligned(row, 8), n)], recv[t].at[sl, pl.ds(base >> t, n)],
                   s_send.at[t, sl], s_recv.at[t, sl], peer).start()

    def rs_finish(u, t):
        sl, nb = u % NS, u % NB
        rs_all(u, t).wait_recv()
        rs_all(u, t).wait_send()
        if t == 0:
            rows = pl.ds(aligned(core * half, half), half)
            acc[nb, rows] = acc[nb, rows] + r0[sl]
            pl.semaphore_signal(credit.at[0, sl], inc=1, device_id=(mate,), device_id_type=MESH)
            return
        for p, (base, size) in enumerate(PARTS):
            n = size >> t
            rows = pl.ds(aligned(core * half + base + offs(u, p, size)[t], 8), n)
            acc[nb, rows] = acc[nb, rows] + recv[t][sl, pl.ds(base >> t, n)]
            pl.semaphore_signal(credit.at[t, sl], inc=1, device_id=(link(dims(u, p, t))[1],), device_id_type=MESH)

    def tile_col(u):
        return jnp.where(u < n_qkv, (u % 3) * pairs + u // 3, u) * TW

    def g_at(u, row, n):
        return g_hbm.at[pl.ds(aligned(row, 8), n), pl.ds(aligned(tile_col(u), TW), TW)]

    def ag_all(u, t):
        r = g_hbm.at[pl.ds(0, half >> t), pl.ds(0, TW)]
        return remote(r, r, g_send.at[t, u % NS], g_recv.at[t, u], mate)

    def ag_start(u, t):
        if t < 3:
            @pl.when(u >= NS)
            def _():
                ag_all(u, t).wait_send()

        if t == 0:
            r = g_at(u, core * half, half)
            remote(r, r, g_send.at[0, u % NS], g_recv.at[0, u], mate).start()
            return
        for p, (base, size) in enumerate(PARTS):
            n = size >> t
            row = core * half + base + offs(u, p, size)[t]
            dst = g_at(u, row, n)
            src = acc.at[u % NB, pl.ds(aligned(row, 8), n)] if t == 3 else dst
            remote(src, dst, g_send.at[t, u % NS], g_recv.at[t, u], link(dims(u, p, t))[1]).start()

    def local_start(u):
        for p, (base, size) in enumerate(PARTS):
            n = size >> 3
            row = core * half + base + offs(u, p, size)[3]
            pltpu.make_async_copy(acc.at[u % NB, pl.ds(aligned(row, 8), n)], g_at(u, row, n), loc_sem.at[u % NS]).start()

    def local_wait(u):
        n = half >> 3
        pltpu.make_async_copy(acc.at[0, pl.ds(0, n)], g_hbm.at[pl.ds(0, n), pl.ds(0, TW)], loc_sem.at[u % NS]).wait()

    n_attn = seqs * pairs
    n_early = pairs + 2 * (seqs - 1)

    def place(a):
        b, c = a - pairs, a - n_early
        s = jnp.where(a < pairs, 0, 1 + jnp.where(c < 0, b // 2, c % (seqs - 1)))
        p = jnp.where(a < pairs, a, jnp.where(c < 0, b % 2, 2 + c // (seqs - 1)))
        return s, p, seq_rows(s), pl.ds(aligned(p * TW, TW), TW)

    def seq_rows(c):
        return pl.ds(aligned(c * seq, seq), seq)

    def attn_in(a, fn):
        _, _, rows, cols = place(a)
        sl = a % 2
        fn(pltpu.make_async_copy(qkv.at[:, rows, cols], qkv_v.at[sl], in_sem.at[0, sl]))
        fn(pltpu.make_async_copy(w_out.at[cols], o_c.at[sl], in_sem.at[1, sl]))

    def start(copy):
        copy.start()

    def wait(copy):
        copy.wait()

    def dproj_rows(a):
        s, p, _, _ = place(a)
        return dproj_v.at[p % 2, :, seq_rows(jnp.where(jnp.logical_and(s == 0, p >= 2), seqs - 1, s))]

    def attn_out(a):
        _, _, rows, cols = place(a)
        sl = a % 2
        return (pltpu.make_async_copy(o_v.at[sl], o_hbm.at[rows, cols], out_sem.at[0, sl]),
                pltpu.make_async_copy(o_t_v.at[sl], o_t_hbm.at[cols, rows], out_sem.at[1, sl]),
                pltpu.make_async_copy(dproj_rows(a), dproj_hbm.at[:, rows, cols], out_sem.at[2, sl]))

    def attn_out_wait(a):
        for c in attn_out(a):
            c.wait()

    def attn_step(a):
        @pl.when(jnp.logical_and(a != pairs - 1, a + 1 < n_attn))
        def _():
            attn_in(a + 1, start)

        attn_in(a, wait)

        @pl.when(jnp.logical_and(a >= 2, a // 2 != pairs // 2))
        def _():
            attn_out_wait(a)

        s, _, _, _ = place(a)
        sl = a % 2

        @pl.when(s == 0)
        def _():
            do_v[sl] = dot_nt(h_v[...], o_c[sl]).astype(BF)

        @pl.when(jnp.logical_and(s > 0, s < seqs - 1))
        def _():
            total = None
            for n in range(per):
                cols = slice(n * TN, (n + 1) * TN)
                part = dot_nt(wbuf[s - 1, cols], o_c[sl, :, cols])
                total = part if total is None else total + part
            do_v[sl] = total.astype(BF)

        @pl.when(s == seqs - 1)
        def _():
            do_v[sl] = dot_nt(dh_v[...].reshape(seq, dim), o_c[sl]).astype(BF)

        attend(scale, qkv_v.at[sl], do_v.at[sl], tabs, o_v.at[sl], o_t_v.at[sl], dproj_rows(a))
        for c in attn_out(a):
            c.start()

    def first_seq(p):
        rows = seq_rows(0)
        return pltpu.make_async_copy(dproj_hbm.at[:, rows, pl.ds(aligned(p * TW, TW), TW)], dproj_v.at[p % 2, :, rows], c0_sem.at[p % 2])

    def rhs_copy(u):
        j = u - n_qkv
        return pltpu.make_async_copy(do_seq.at[:, pl.ds(aligned(j * TW, TW), TW)], dproj_v.at[0, j % 3], rhs_sem.at[j % 3])

    def dw_tile(u):
        @pl.when(u == n_qkv)
        def _():
            pltpu.make_async_copy(o_t_hbm, lhs, lhs_sem).wait()

        @pl.when(u >= n_qkv)
        def _():
            rhs_copy(u).wait()

        @pl.when(jnp.logical_and(u % 3 == 0, jnp.logical_and(u >= 6, u < n_qkv)))
        def _():
            first_seq(u // 3).wait()

        p = jnp.where(u < n_qkv, (u // 3) % 2, 0)

        def half_tile(mine):
            @pl.loop(0, half // TN)
            def _(b):
                rows = pl.ds(aligned(mine * half + b * TN, TN), TN)
                acc[u % NB, rows] = dot_nn(lhs[rows], dproj_v[p, u % 3])

        half_tile(1 - core)
        rs_start(u, 0)
        half_tile(core)

        @pl.when(u == n_qkv - 1)
        def _():
            pltpu.make_async_copy(o_t_hbm, lhs, lhs_sem).start()

        @pl.when(jnp.logical_and(u + 2 >= n_qkv, u + 2 < n_all))
        def _():
            rhs_copy(u + 2).start()

    n_blocks = 4 * seqs

    def columns(n):
        return pl.ds(aligned(n * TN, TN), TN)

    def block(b):
        is_out = jnp.logical_or(b == 0, jnp.logical_and((b + 1) % 3 == 0, b <= 3 * seqs - 4))
        done = jnp.minimum((b + 1) // 3, seqs - 1)
        return is_out, done, b - 1 - done

    def tile_start(t):
        b, n, sl = t // per, t % per, t % 2
        is_out, c, q = block(b)

        @pl.when(is_out)
        def _():
            pltpu.make_async_copy(w_out.at[:, columns(n)], wbuf.at[sl], w_sem.at[0, sl]).start()
            pltpu.make_async_copy(h_seq.at[seq_rows(c), columns(n)], pbuf.at[sl], w_sem.at[1, sl]).start()

        @pl.when(jnp.logical_not(is_out))
        def _():
            pltpu.make_async_copy(w_qkv.at[:, columns((q % 3) * per + n)], wbuf.at[sl], w_sem.at[0, sl]).start()
            pltpu.make_async_copy(dproj_hbm.at[q % 3, seq_rows(q // 3), columns(n)], pbuf.at[sl], w_sem.at[1, sl]).start()

    def tile_wait(t):
        sl = t % 2
        pltpu.make_async_copy(w_out.at[:, columns(0)], wbuf.at[sl], w_sem.at[0, sl]).wait()
        pltpu.make_async_copy(h_seq.at[seq_rows(0), columns(0)], pbuf.at[sl], w_sem.at[1, sl]).wait()

    def o_load(c):
        n = seq // 2
        return [pltpu.make_async_copy(o_hbm.at[pl.ds(aligned(c * seq + k * n, n), n)], o_c.at[k], o_sem.at[k]) for k in range(2)]

    def y_sent(n):
        r = y_all.at[pl.ds(0, group - 1), :, columns(0)]
        return remote(r, r, y_send.at[n], y_recv.at[0], mate)

    def y_own_copy(c, n):
        return pltpu.make_async_copy(y_t.at[n, me], y_all.at[me * seqs + c, :, columns(n)], y_own.at[n])

    def out_tile(c, n, sl):
        y = pbuf[sl].astype(F32) + dot_nn(o_c[...].reshape(seq, dim), wbuf[sl])

        @pl.when(c > 0)
        def _():
            y_sent(n).wait_send()
            y_own_copy(0, n).wait()

        y_t[n] = y.astype(BF).reshape(group, loc, TN)
        for j in ORDER:
            peer = flipped(me, j)
            remote(y_t.at[n, peer], y_all.at[me * seqs + c, :, columns(n)], y_send.at[n], y_recv.at[c], peer).start()
        y_own_copy(c, n).start()

    def run_block(b):
        is_out, c_out, q = block(b)
        c, third = q // 3, q % 3

        @pl.when(is_out)
        def _():
            for x in o_load(c_out):
                x.wait()

        @pl.when(jnp.logical_and(jnp.logical_not(is_out), third == 2))
        def _():
            pltpu.make_async_copy(h_seq.at[seq_rows(c)], h_v, dh_sem.at[0]).start()
            pltpu.make_async_copy(do_seq.at[seq_rows(c)], dout_v, dh_sem.at[1]).start()

        @pl.loop(0, per)
        def _(n):
            t = b * per + n
            sl = t % 2

            @pl.when(jnp.logical_and(t != per - 1, t + 1 < n_blocks * per))
            def _():
                tile_start(t + 1)

            tile_wait(t)

            @pl.when(is_out)
            def _():
                out_tile(c_out, n, sl)

            @pl.when(jnp.logical_not(is_out))
            def _():
                part = dot_nt(pbuf[sl], wbuf[sl])
                first = jnp.logical_and(third == 0, n == 0)

                @pl.when(first)
                def _():
                    dn_acc[...] = part

                @pl.when(jnp.logical_not(first))
                def _():
                    dn_acc[...] += part

        @pl.when(jnp.logical_and(is_out, jnp.logical_and(c_out > 0, c_out + 1 < seqs)))
        def _():
            for x in o_load(c_out + 1):
                x.start()

        @pl.when(jnp.logical_and(jnp.logical_not(is_out), third == 2))
        def _():
            norm_back(c)

    def norm_back(c):
        pltpu.make_async_copy(h_seq.at[seq_rows(c)], h_v, dh_sem.at[0]).wait()
        pltpu.make_async_copy(do_seq.at[seq_rows(c)], dout_v, dh_sem.at[1]).wait()

        @pl.when(c > 0)
        def _():
            pltpu.make_async_copy(dh_v, dh_hbm.at[:, 0], dh_sem.at[2]).wait()

        gain = gain_ref[...].astype(F32).reshape(1, dim)

        @pl.loop(0, group)
        def _(b):
            r = pl.ds(aligned(b * loc, loc), loc)
            h = h_v[r].astype(F32)
            inv = lax.rsqrt(jnp.mean(h * h, axis=-1, keepdims=True) + NORM_EPS)
            dn = dn_acc[r].astype(BF).astype(F32)
            dg = jnp.sum(dn * h * inv, axis=0, keepdims=True)
            ds = dn * gain
            dh = dout_v[r].astype(F32) + inv * ds - h * (inv * inv * inv) * jnp.mean(ds * h, axis=-1, keepdims=True)
            dh_v[b] = dh.astype(BF)
            first = jnp.logical_and(c == 0, b == 0)

            @pl.when(first)
            def _():
                dg_all[me] = dg

            @pl.when(jnp.logical_not(first))
            def _():
                dg_all[me] += dg

        @pl.when(c < by_xla)
        def _():
            pltpu.make_async_copy(dh_v, dh_hbm.at[:, c], dh_sem.at[2]).start()

        @pl.when(c >= by_xla)
        def _():
            pltpu.make_async_copy(dh_v, dh_loc.at[:, c - by_xla], dh_sem.at[2]).start()

    def dh_send(q):
        k, cols = q // 4, pl.ds(aligned((q % 4) * (dim // 4), dim // 4), dim // 4)
        for j in ORDER:
            peer = flipped(me, j)
            remote(dh_loc.at[peer, k, :, cols], dh_all.at[me, k, :, cols], x_send.at[q], x_recv.at[q], peer).start()
        pltpu.make_async_copy(dh_loc.at[me, k, :, cols], dh_all.at[me, k, :, cols], own_sem.at[q]).start()

    def dh_wait(q):
        r = dh_all.at[pl.ds(0, group - 1), 0, :, pl.ds(0, dim // 4)]
        done = remote(r, r, x_send.at[q], x_recv.at[q], mate)
        done.wait_recv()
        done.wait_send()
        pltpu.make_async_copy(dh_loc.at[0, 0, :, pl.ds(0, dim // 4)], dh_all.at[0, 0, :, pl.ds(0, dim // 4)], own_sem.at[q]).wait()

    def my_rows(c):
        return pl.ds(aligned(c * seq + me * loc, loc), loc)

    def from_all(dst, ss, rs):
        r = dst.at[pl.ds(0, (group - 1) * loc)]
        return remote(r, r, ss, rs, mate)

    def send_all(src, dst, ss, rs, c):
        for j in ORDER:
            peer = flipped(me, j)
            to = dh_v.at[me] if dst is do_seq and c == seqs - 1 else dst.at[my_rows(c)]
            remote(src.at[peer * seqs + c], to, ss.at[c], rs.at[c], peer).start()

    def project(c):
        rows = seq_rows(c)
        from_all(h_seq, h_send.at[c], h_recv.at[c]).wait_recv()
        load = pltpu.make_async_copy(h_seq.at[rows], h_v, ld_sem)
        load.start()
        load.wait()
        gain = gain_ref[...].astype(F32).reshape(1, dim)
        blk = 128

        @pl.loop(0, seq // blk)
        def _(b):
            r = pl.ds(aligned(b * blk, blk), blk)
            h = h_v[r].astype(F32)
            inv = lax.rsqrt(jnp.mean(h * h, axis=-1, keepdims=True) + NORM_EPS)
            n = (h * inv * gain).astype(BF)
            dout_v[r] = n
            lhs[:, pl.ds(aligned(c * seq + b * blk, blk), blk)] = n.T

        @pl.loop(0, 3 * per)
        def _(n):
            t = c * 3 * per + n
            sl = t % 2

            @pl.when(t + 1 < seqs * 3 * per)
            def _():
                qkv_w(t + 1).start()

            qkv_w(t).wait()
            proj = dot_nn(dout_v[...], wbuf[sl])

            @pl.when(t >= 2)
            def _():
                qkv_out(t).wait()

            @pl.when(n < 2 * per)
            def _():
                for h in range(TN // 128):
                    cols = slice(h * 128, (h + 1) * 128)
                    pbuf[sl, :, cols] = rotate(proj[:, cols], tabs[:, :HEAD], tabs[:, HEAD:]).astype(BF)

            @pl.when(n >= 2 * per)
            def _():
                pbuf[sl] = proj.astype(BF)

            qkv_out(t).start()

    def qkv_w(t):
        return pltpu.make_async_copy(w_qkv.at[:, columns(t % (3 * per))], wbuf.at[t % 2], w_sem.at[0, t % 2])

    def qkv_out(t):
        n = t % (3 * per)
        return pltpu.make_async_copy(pbuf.at[t % 2], qkv.at[n // per, seq_rows(t // (3 * per)), columns(n % per)], w_sem.at[1, t % 2])

    def gradient_in():
        for t in range(2):
            qkv_out(t).wait()
        attn_in(0, start)
        for c in range(seqs - 1):
            from_all(do_seq, d_send.at[c], d_recv.at[c]).wait_recv()
            rows = seq_rows(c)
            if c == 0:
                loads = [pltpu.make_async_copy(do_seq.at[rows], h_v, ld_sem)]
            else:
                loads = [pltpu.make_async_copy(do_seq.at[rows, pl.ds(n * TN, TN)], wbuf.at[c - 1, pl.ds(n * TN, TN)], x_send.at[n]) for n in range(per)]
            for x in loads:
                x.start()
            for x in loads:
                x.wait()
            if c == 0:
                pl.loop(0, pairs)(attn_step)
                attn_out_wait(pairs - 2)
                attn_out_wait(pairs - 1)
                for x in o_load(0):
                    x.start()
                tile_start(0)
                run_block(0)
                attn_in(pairs, start)
            else:
                pl.loop(pairs + 2 * c - 2, pairs + 2 * c)(attn_step)
        from_all(do_seq, d_send.at[seqs - 1], d_recv.at[seqs - 1]).wait_recv()
        last_copy().start()
        attn_step(n_early - 2)

    def last_copy():
        dst = do_seq.at[seq_rows(seqs - 1)]
        return pltpu.make_async_copy(dh_v, dst.reshape(group, loc, dim), ld_sem)

    by_xla = dh_hbm.shape[1]

    def own_in(k):
        src = hidden if k < seqs else d_out
        to = dh_v.at[me] if k == 2 * seqs - 1 else dout_v.at[pl.ds(k * loc, loc)]
        return pltpu.make_async_copy(src.at[me * seqs + k % seqs], to, own_sem.at[k])

    def own_out(k):
        dst = h_seq if k < seqs else do_seq
        return pltpu.make_async_copy(dout_v.at[pl.ds(k * loc, loc)], dst.at[my_rows(k % seqs)], own_sem.at[k])

    barrier = pltpu.get_barrier_semaphore()
    for j in reversed(ORDER):
        pl.semaphore_signal(barrier, inc=1, device_id=(flipped(me, j),), device_id_type=MESH)
    for k in range(2 * seqs):
        own_in(k).start()
    qkv_w(0).start()
    mine = pl.ds(aligned(me * loc, loc), loc)
    tab[...] = jnp.concatenate([cos_ref[...], sin_ref[...]], axis=1)
    tab_all[mine] = tab[...]
    pl.semaphore_wait(barrier, group - 1)
    for j in ORDER:
        remote(tab, tab_all.at[mine], t_send, t_recv, flipped(me, j)).start()
    for c in range(seqs):
        send_all(hidden, h_seq, h_send, h_recv, c)
    for c in range(seqs):
        send_all(d_out, do_seq, d_send, d_recv, c)
    for k in range(2 * seqs):
        own_in(k).wait()
        if k < 2 * seqs - 1:
            own_out(k).start()
    from_all(tab_all, t_send, t_recv).wait_recv()
    table = tab_all[...]
    swapped = pltpu.roll(table, 64, 1)
    left = lax.broadcasted_iota(jnp.int32, table.shape, 1) < 64
    tabs[:, :HEAD] = jnp.where(left, table, swapped)
    tabs[:, HEAD:] = jnp.where(left, -swapped, table)
    for k in range(2 * seqs - 1):
        own_out(k).wait()
    pl.loop(0, seqs)(project)
    gradient_in()

    first_out = 3 * (pairs - 1)
    first_dn = first_out + seqs

    def step(i, carry):
        def guarded(lag, fn):
            u = i - lag

            @pl.when(jnp.logical_and(u >= 0, u < n_all))
            def _():
                fn(u)

        def ag0(u):
            ag_all(u, 0).wait_recv()

        def ag1(u):
            ag_all(u, 1).wait_recv()
            ag_start(u, 0)

        def ag2(u):
            ag_all(u, 2).wait_recv()
            ag_start(u, 1)

        def ag3(u):
            ag_all(u, 3).wait_recv()
            ag_all(u, 3).wait_send()
            local_wait(u)
            ag_start(u, 2)

        def last(u):
            rs_finish(u, 3)
            local_start(u)
            ag_start(u, 3)

        def middle(t):
            def fn(u):
                rs_finish(u, t)
                rs_start(u, t + 1)
            return fn

        guarded(0, dw_tile)

        from_a, to_a = [n_early - 1 + jnp.where(k > 2, k - 1, 0) for k in (i, i + 1)]

        @pl.when(jnp.logical_and(i % 3 == 0, jnp.logical_and(i >= 3, i < first_out)))
        def _():
            first_seq(i // 3 + 1).start()

        @pl.when(i < first_out)
        def _():
            pl.loop(from_a, jnp.minimum(to_a, n_attn))(attn_step)

        for lag, fn in enumerate((middle(0), middle(1), middle(2), last, ag3, ag2, ag1, ag0)):
            guarded(lag + 1, fn)

        @pl.when(i == first_out)
        def _():
            attn_out_wait(n_attn - 2)
            attn_out_wait(n_attn - 1)
            for x in o_load(1):
                x.start()
            tile_start(per)

        def blocks(i):
            k = i - first_out
            return jnp.where(k <= seqs, jnp.maximum(3 * k - 1, 1), jnp.minimum(k + 2 * seqs, n_blocks))

        @pl.when(i >= first_out)
        def _():
            pl.loop(blocks(i), blocks(i + 1))(run_block)

        @pl.when(i == 3)
        def _():
            last_copy().wait()

        first_dh = first_dn + seqs

        @pl.when(i == first_dh)
        def _():
            pltpu.make_async_copy(dh_v, dh_hbm.at[:, 0], dh_sem.at[2]).wait()
            for j in range(1, group):
                remote(dg_all.at[me], dg_all.at[me], dg_send, dg_recv, flipped(me, j)).start()

        @pl.when(jnp.logical_and(i >= first_dh, i < first_dh + 4 * (seqs - by_xla)))
        def _():
            dh_send(i - first_dh)

        return carry

    lax.fori_loop(0, n_all + 8, step, 0)

    for c in range(seqs):
        r = y_all.at[pl.ds(0, group - 1)]
        remote(r, r, y_send.at[0], y_recv.at[c], mate).wait_recv()
        from_all(h_seq, h_send.at[c], h_recv.at[c]).wait_send()
        from_all(do_seq, d_send.at[c], d_recv.at[c]).wait_send()
    for n in range(per):
        y_sent(n).wait_send()
        y_own_copy(0, n).wait()
    from_all(tab_all, t_send, t_recv).wait_send()
    for q in range(4 * (seqs - by_xla)):
        dh_wait(q)
    others = remote(dg_all.at[pl.ds(0, group - 1)], dg_all.at[pl.ds(0, group - 1)], dg_send, dg_recv, mate)
    others.wait_recv()
    others.wait_send()
    dgain = dg_all[0]
    for j in range(1, group):
        dgain = dgain + dg_all[j]
    dgain_ref[...] = dgain.reshape(dim)
    for j in range(NS):
        u = n_all - NS + j
        for t in range(4):
            pl.semaphore_wait(credit.at[t, u % NS], 1 if t == 0 else 3)
            if t < 3:
                ag_all(u, t).wait_send()


BY_XLA = 2


def main_call(hidden, d_out, cos_tab, sin_tab, w_qkv, w_out, gain):
    n, loc, dim = hidden.shape
    group = 16
    rows = n * loc
    seqs = n // group
    seq = loc * group
    h = dim // 2
    n_all = 4 * dim // TW
    hbm = pl.BlockSpec(memory_space=pl.ANY)
    vmem = pl.BlockSpec(memory_space=pltpu.VMEM)
    D = pltpu.SemaphoreType.DMA
    S = jax.ShapeDtypeStruct
    V = pltpu.VMEM
    act = S((rows, dim), BF)
    return pl.pallas_call(
        functools.partial(main_kernel, 128 ** -0.5),
        in_specs=[hbm] * 2 + [vmem] * 2 + [hbm] * 2 + [vmem],
        out_specs=[hbm] * 11 + [vmem],
        out_shape=[S((dim, 4 * dim), F32), act, act, S((3, rows, dim), BF),
                   act, S((dim, rows), BF), S((3, rows, dim), BF), S((n, loc, dim), BF),
                   S((group, BY_XLA, loc, dim), BF), S((group, seqs - BY_XLA, loc, dim), BF), S((group, seqs - BY_XLA, loc, dim), BF), S((dim,), F32)],
        scratch_shapes=[
            V((dim, rows), BF), V((2, 3, rows, TW), BF), V((NB, dim, TW), F32),
            V((NS, h, TW), F32), V((NS, h >> 1, TW), F32), V((NS, h >> 2, TW), F32), V((NS, h >> 3, TW), F32),
            V((2, 3, seq, TW), BF), V((2, seq, TW), BF), V((2, seq, TW), BF), V((2, TW, seq), BF), V((seq, 256), F32), V((loc, 128), F32), V((seq, 128), F32),
            V((seq, dim), F32), V((seq, dim), BF), V((seq, dim), BF), V((group, loc, dim), BF), V((group, 1, dim), F32),
            V((2, dim, 512), BF), V((2, seq, 512), BF), V((2, seq // 2, dim), BF), V((dim // 512, group, loc, 512), BF),
            D, D, D((4, NS)), D((4, NS)), pltpu.SemaphoreType.REGULAR((4, NS)), D((NS,)), D((4, NS)), D((4, n_all)),
            D((2, 2)), D((3, 2)), D((3,)), D((3,)), D, D, D((2, 2)), D((2,)), D((2,)),
            D((seqs,)), D((seqs,)), D((seqs,)), D((seqs,)), D, D, D((2 * seqs,)), D((dim // 512,)), D((seqs,)), D((dim // 512,)), D((4 * (seqs - BY_XLA),)), D((4 * (seqs - BY_XLA),)),
        ],
        compiler_params=pltpu.CompilerParams(collective_id=0, has_side_effects=True, vmem_limit_bytes=67043328),
        cost_estimate=pl.CostEstimate(flops=28 * rows * dim * dim, bytes_accessed=90 * dim * dim, transcendentals=0),
        name="main",
    )(hidden, d_out, cos_tab, sin_tab, w_qkv, w_out, gain)


def place_kernel(y_in, b_in, y_out, dh_out):
    y_out[...] = y_in[...]
    dh_out[...] = b_in[...]


def place_call(y, b):
    n, loc, dim = y.shape
    group, k = b.shape[:2]
    seqs = n // group
    return pl.pallas_call(
        place_kernel,
        grid=(2,),
        in_specs=[pl.BlockSpec((n // 2, loc, dim), lambda j: (j, 0, 0)), pl.BlockSpec((group // 2, k, loc, dim), lambda j: (j, 0, 0, 0))],
        out_specs=[pl.BlockSpec((n // 2, loc, dim), lambda j: (j, 0, 0)), pl.BlockSpec((group // 2, k, loc, dim), lambda j: (j, seqs // k - 1, 0, 0))],
        out_shape=[jax.ShapeDtypeStruct((n, loc, dim), BF), jax.ShapeDtypeStruct((group, seqs, loc, dim), BF)],
        cost_estimate=pl.CostEstimate(flops=8 * n * loc * dim, bytes_accessed=6 * n * loc * dim, transcendentals=0),
        name="place",
    )(y, b)


def fill_kernel(a_in, dh_in, dh_out):
    dh_out[...] = a_in[...]


def fill_call(a, dh):
    group, k, loc, dim = a.shape
    return pl.pallas_call(
        fill_kernel,
        grid=(2,),
        in_specs=[pl.BlockSpec((group // 2, k, loc, dim), lambda j: (j, 0, 0, 0)), pl.BlockSpec(memory_space=pl.ANY)],
        out_specs=pl.BlockSpec((group // 2, k, loc, dim), lambda j: (j, 0, 0, 0)),
        out_shape=jax.ShapeDtypeStruct(dh.shape, BF),
        input_output_aliases={1: 0},
        name="fill",
    )(a, dh)


def solution(mesh):
    group = mesh.shape['sp']
    token_spec = P(None, 'sp', None)
    table_spec = P('sp', None)

    def device_step(hidden, norm_gain, w_qkv, w_out, cos_tab, sin_tab, d_out):
        num_seqs, local_len, dim = hidden.shape
        dw, _, _, _, _, _, _, y, dh_a, _, dh_b, dgain = main_call(hidden, d_out, cos_tab, sin_tab, w_qkv, w_out, norm_gain)
        dh_a = lax.all_to_all(dh_a, 'sp', split_axis=0, concat_axis=0, tiled=True)
        y, dh = place_call(y, dh_b)
        dh = fill_call(dh_a, dh).reshape(num_seqs, local_len, dim)
        return y, dh, dw[:, :3 * dim], dw[:, 3 * dim:], dgain

    return jax.shard_map(device_step, mesh=mesh, in_specs=(token_spec, P(), P(), P(), table_spec, table_spec, token_spec), out_specs=(token_spec, token_spec, P(), P(), P()), check_vma=False)
```

```python
import functools
import jax
import jax.numpy as jnp
from jax import lax
from jax.experimental import pallas as pl
from jax.experimental.pallas import tpu as pltpu
from jax.sharding import PartitionSpec as P

NORM_EPS = 1e-6
HEAD = 128
BF = jnp.bfloat16
F32 = jnp.float32
VMEM_LIMIT = 60 * 1024 * 1024


def dot_nn(a, b):
    return lax.dot_general(a, b, (((1,), (0,)), ((), ())), preferred_element_type=F32)


def dot_nt(a, b):
    return lax.dot_general(a, b, (((1,), (1,)), ((), ())), preferred_element_type=F32)


def rotate(u, cos, sin_signed):
    return u * cos + pltpu.roll(u, 64, 1) * sin_signed


def unrotate(u, cos, sin_signed):
    return u * cos - pltpu.roll(u, 64, 1) * sin_signed


MESH = pl.DeviceIdType.MESH


def flipped(me, j):
    p = me
    for b in range(4):
        w = 1 << b
        if j & w:
            p = p + w * (1 - 2 * ((me // w) % 2))
    return p


ORDER = tuple(int(j, 16) for j in '2481359' + '6ac7bdef')


TW = 256
PARTS = ((0, 384), (384, 320), (704, 320))
NS = 3
NB = 6
BLK = 256


def attend(scale, qkv, do, tabs, o_out, o_t_out, dproj_out):
    seq = qkv.shape[1]
    for h in range(2):
        cols = slice(h * 128, (h + 1) * 128)
        q = qkv[0, :, cols]
        k = qkv[1, :, cols]
        v = qkv[2, :, cols]
        dout = do[:, cols]
        k_t = k.T
        v_t = v.T
        dk = [None] * (seq // BLK)
        dv = [None] * (seq // BLK)
        for j in range(seq // BLK):
            end = (j + 1) * BLK
            rows = slice(j * BLK, end)
            q_j = q[rows]
            do_j = dout[rows]
            s = dot_nt(k[:end], q_j)
            row = lax.broadcasted_iota(jnp.int32, (end, BLK), 0)
            col = lax.broadcasted_iota(jnp.int32, (end, BLK), 1) + j * BLK
            s = jnp.where(row <= col, s * scale, -1e30)
            m = jnp.max(s, axis=0, keepdims=True)
            e = jnp.exp(s - m)
            p = e * (1.0 / jnp.sum(e, axis=0, keepdims=True))
            p_bf = p.astype(BF)
            o_t = dot_nn(v_t[:, :end], p_bf)
            dp = dot_nt(v[:end], do_j).astype(BF).astype(F32)
            delta = jnp.sum(p * dp, axis=0, keepdims=True)
            ds = (p * (dp - delta) * scale).astype(BF)
            dv_j = dot_nn(p_bf, do_j)
            dk_j = dot_nn(ds, q_j)
            dq_t = dot_nn(k_t[:, :end], ds)
            for i in range(j + 1):
                part = slice(i * BLK, (i + 1) * BLK)
                dv[i] = dv_j[part] if dv[i] is None else dv[i] + dv_j[part]
                dk[i] = dk_j[part] if dk[i] is None else dk[i] + dk_j[part]
            o_out[rows, cols] = o_t.T.astype(BF)
            o_t_out[cols, rows] = o_t.astype(BF)
            dq = dq_t.T.astype(BF).astype(F32)
            dproj_out[0, rows, cols] = unrotate(dq, tabs[rows, :HEAD], tabs[rows, HEAD:]).astype(BF)
        for j in range(seq // BLK):
            rows = slice(j * BLK, (j + 1) * BLK)
            dkj = dk[j].astype(BF).astype(F32)
            dproj_out[1, rows, cols] = unrotate(dkj, tabs[rows, :HEAD], tabs[rows, HEAD:]).astype(BF)
            dproj_out[2, rows, cols] = dv[j].astype(BF)


def main_kernel(scale, hidden, d_out, cos_ref, sin_ref, w_qkv, w_out, gain_ref,
                g_hbm, h_seq, do_seq, qkv, o_hbm, o_t_hbm, dproj_hbm, y_all, dh_hbm, dh_loc, dh_all, dgain_ref,
                lhs, dproj_v, acc, r0, r1, r2, r3, qkv_v, do_v, o_v, o_t_v, tabs, tab, tab_all, dn_acc, h_v, dout_v, dh_v, dg_all, wbuf, pbuf, o_c, y_t,
                lhs_sem, ld_sem, s_send, s_recv, credit, loc_sem, g_send, g_recv,
                in_sem, out_sem, rhs_sem, dh_sem, dg_send, dg_recv, w_sem, o_sem, c0_sem,
                h_send, h_recv, d_send, d_recv, t_send, t_recv, own_sem, y_send, y_recv, y_own, x_send, x_recv):
    me = lax.axis_index('sp')
    group = 16
    loc, dim = hidden.shape[1:]
    seqs = hidden.shape[0] // group
    seq = loc * group
    half = dim // 2
    n_qkv = 3 * dim // TW
    n_all = 4 * dim // TW
    pairs = dim // TW
    core = me % 2
    mate = me + 1 - 2 * core
    recv = (r0, r1, r2, r3)
    TN = 512
    per = dim // TN

    def remote(src, dst, ss, rs, peer):
        return pltpu.make_async_remote_copy(src_ref=src, dst_ref=dst, send_sem=ss, recv_sem=rs, device_id=(peer,), device_id_type=MESH)

    def link(d):
        w = 2 + d + d * d
        bit = (me // w) % 2
        return bit, me + w * (1 - 2 * bit)

    def aligned(x, n):
        return pl.multiple_of(x, n)

    def dims(u, p, t):
        return (u + p + t - 1) % 3

    def offs(u, p, size):
        o = [0]
        for t in (1, 2, 3):
            b, _ = link(dims(u, p, t))
            o.append(o[-1] + b * (size >> t))
        return o

    def rs_all(u, t):
        sl = u % NS
        return remote(recv[t].at[sl], recv[t].at[sl], s_send.at[t, sl], s_recv.at[t, sl], mate)

    def rs_start(u, t):
        sl, nb = u % NS, u % NB

        @pl.when(u >= NS)
        def _():
            pl.semaphore_wait(credit.at[t, sl], 1 if t == 0 else 3)

        if t == 0:
            n = half // 4
            for k in range(4):
                src = acc.at[nb, pl.ds(aligned((1 - core) * half + k * n, n), n)]
                remote(src, r0.at[sl, pl.ds(k * n, n)], s_send.at[0, sl], s_recv.at[0, sl], mate).start()
            return
        for p, (base, size) in enumerate(PARTS):
            o = offs(u, p, size)
            n = size >> t
            b, peer = link(dims(u, p, t))
            row = core * half + base + o[t - 1] + (1 - b) * n
            remote(acc.at[nb, pl.ds(aligned(row, 8), n)], recv[t].at[sl, pl.ds(base >> t, n)],
                   s_send.at[t, sl], s_recv.at[t, sl], peer).start()

    def rs_finish(u, t):
        sl, nb = u % NS, u % NB
        rs_all(u, t).wait_recv()
        rs_all(u, t).wait_send()
        if t == 0:
            rows = pl.ds(aligned(core * half, half), half)
            acc[nb, rows] = acc[nb, rows] + r0[sl]
            pl.semaphore_signal(credit.at[0, sl], inc=1, device_id=(mate,), device_id_type=MESH)
            return
        for p, (base, size) in enumerate(PARTS):
            n = size >> t
            rows = pl.ds(aligned(core * half + base + offs(u, p, size)[t], 8), n)
            acc[nb, rows] = acc[nb, rows] + recv[t][sl, pl.ds(base >> t, n)]
            pl.semaphore_signal(credit.at[t, sl], inc=1, device_id=(link(dims(u, p, t))[1],), device_id_type=MESH)

    def tile_col(u):
        return jnp.where(u < n_qkv, (u % 3) * pairs + u // 3, u) * TW

    def g_at(u, row, n):
        return g_hbm.at[pl.ds(aligned(row, 8), n), pl.ds(aligned(tile_col(u), TW), TW)]

    def ag_all(u, t):
        r = g_hbm.at[pl.ds(0, half >> t), pl.ds(0, TW)]
        return remote(r, r, g_send.at[t, u % NS], g_recv.at[t, u], mate)

    def ag_mate(u, late):
        for p, (base, size) in enumerate(PARTS):
            n = size >> 1
            b, _ = link(dims(u, p, 1))
            r = g_at(u, core * half + base + (1 - b if late else b) * n, n)
            remote(r, r, g_send.at[0, u % NS], g_recv.at[0, u], mate).start()

    def ag_start(u, t):
        if t < 3:
            @pl.when(u >= NS)
            def _():
                ag_all(u, t).wait_send()

        for p, (base, size) in enumerate(PARTS):
            n = size >> t
            row = core * half + base + offs(u, p, size)[t]
            dst = g_at(u, row, n)
            src = acc.at[u % NB, pl.ds(aligned(row, 8), n)] if t == 3 else dst
            remote(src, dst, g_send.at[t, u % NS], g_recv.at[t, u], link(dims(u, p, t))[1]).start()

    def local_start(u):
        for p, (base, size) in enumerate(PARTS):
            n = size >> 3
            row = core * half + base + offs(u, p, size)[3]
            pltpu.make_async_copy(acc.at[u % NB, pl.ds(aligned(row, 8), n)], g_at(u, row, n), loc_sem.at[u % NS]).start()

    def local_wait(u):
        n = half >> 3
        pltpu.make_async_copy(acc.at[0, pl.ds(0, n)], g_hbm.at[pl.ds(0, n), pl.ds(0, TW)], loc_sem.at[u % NS]).wait()

    n_attn = seqs * pairs
    n_early = pairs + 2 * (seqs - 1)

    def place(a):
        b, c = a - pairs, a - n_early
        s = jnp.where(a < pairs, 0, 1 + jnp.where(c < 0, b // 2, c % (seqs - 1)))
        p = jnp.where(a < pairs, a, jnp.where(c < 0, b % 2, 2 + c // (seqs - 1)))
        return s, p, seq_rows(s), pl.ds(aligned(p * TW, TW), TW)

    def seq_rows(c):
        return pl.ds(aligned(c * seq, seq), seq)

    def attn_in(a, fn):
        _, _, rows, cols = place(a)
        sl = a % 2
        fn(pltpu.make_async_copy(qkv.at[:, rows, cols], qkv_v.at[sl], in_sem.at[0, sl]))
        fn(pltpu.make_async_copy(w_out.at[cols], o_c.at[sl], in_sem.at[1, sl]))

    def start(copy):
        copy.start()

    def wait(copy):
        copy.wait()

    def dproj_rows(a):
        s, p, _, _ = place(a)
        return dproj_v.at[p % 2, :, seq_rows(jnp.where(jnp.logical_and(s == 0, p >= 2), seqs - 1, s))]

    def attn_out(a):
        _, _, rows, cols = place(a)
        sl = a % 2
        return (pltpu.make_async_copy(o_v.at[sl], o_hbm.at[rows, cols], out_sem.at[0, sl]),
                pltpu.make_async_copy(o_t_v.at[sl], o_t_hbm.at[cols, rows], out_sem.at[1, sl]),
                pltpu.make_async_copy(dproj_rows(a), dproj_hbm.at[:, rows, cols], out_sem.at[2, sl]))

    def attn_out_wait(a):
        for c in attn_out(a):
            c.wait()

    def attn_step(a):
        @pl.when(jnp.logical_and(a != pairs - 1, a + 1 < n_attn))
        def _():
            attn_in(a + 1, start)

        attn_in(a, wait)

        @pl.when(jnp.logical_and(a >= 2, a // 2 != pairs // 2))
        def _():
            attn_out_wait(a)

        s, _, _, _ = place(a)
        sl = a % 2

        @pl.when(s == 0)
        def _():
            do_v[sl] = dot_nt(h_v[...], o_c[sl]).astype(BF)

        @pl.when(jnp.logical_and(s > 0, s < seqs - 1))
        def _():
            total = None
            for n in range(per):
                cols = slice(n * TN, (n + 1) * TN)
                part = dot_nt(wbuf[s - 1, cols], o_c[sl, :, cols])
                total = part if total is None else total + part
            do_v[sl] = total.astype(BF)

        @pl.when(s == seqs - 1)
        def _():
            do_v[sl] = dot_nt(dh_v[...].reshape(seq, dim), o_c[sl]).astype(BF)

        attend(scale, qkv_v.at[sl], do_v.at[sl], tabs, o_v.at[sl], o_t_v.at[sl], dproj_rows(a))
        for c in attn_out(a):
            c.start()

    def first_seq(p):
        rows = seq_rows(0)
        return pltpu.make_async_copy(dproj_hbm.at[:, rows, pl.ds(aligned(p * TW, TW), TW)], dproj_v.at[p % 2, :, rows], c0_sem.at[p % 2])

    def rhs_copy(u):
        j = u - n_qkv
        return pltpu.make_async_copy(do_seq.at[:, pl.ds(aligned(j * TW, TW), TW)], dproj_v.at[0, j % 3], rhs_sem.at[j % 3])

    def dw_tile(u):
        @pl.when(u == n_qkv)
        def _():
            pltpu.make_async_copy(o_t_hbm, lhs, lhs_sem).wait()

        @pl.when(u >= n_qkv)
        def _():
            rhs_copy(u).wait()

        @pl.when(jnp.logical_and(u % 3 == 0, jnp.logical_and(u >= 6, u < n_qkv)))
        def _():
            first_seq(u // 3).wait()

        p = jnp.where(u < n_qkv, (u // 3) % 2, 0)

        def half_tile(mine):
            @pl.loop(0, half // TN)
            def _(b):
                rows = pl.ds(aligned(mine * half + b * TN, TN), TN)
                acc[u % NB, rows] = dot_nn(lhs[rows], dproj_v[p, u % 3])

        half_tile(1 - core)
        rs_start(u, 0)
        half_tile(core)

        @pl.when(u == n_qkv - 1)
        def _():
            pltpu.make_async_copy(o_t_hbm, lhs, lhs_sem).start()

        @pl.when(jnp.logical_and(u + 2 >= n_qkv, u + 2 < n_all))
        def _():
            rhs_copy(u + 2).start()

    n_blocks = 4 * seqs

    def columns(n):
        return pl.ds(aligned(n * TN, TN), TN)

    def block(b):
        is_out = jnp.logical_or(b == 0, jnp.logical_and((b + 1) % 3 == 0, b <= 3 * seqs - 4))
        done = jnp.minimum((b + 1) // 3, seqs - 1)
        return is_out, done, b - 1 - done

    def tile_start(t):
        b, n, sl = t // per, t % per, t % 2
        is_out, c, q = block(b)

        @pl.when(is_out)
        def _():
            pltpu.make_async_copy(w_out.at[:, columns(n)], wbuf.at[sl], w_sem.at[0, sl]).start()
            pltpu.make_async_copy(h_seq.at[seq_rows(c), columns(n)], pbuf.at[sl], w_sem.at[1, sl]).start()

        @pl.when(jnp.logical_not(is_out))
        def _():
            pltpu.make_async_copy(w_qkv.at[:, columns((q % 3) * per + n)], wbuf.at[sl], w_sem.at[0, sl]).start()
            pltpu.make_async_copy(dproj_hbm.at[q % 3, seq_rows(q // 3), columns(n)], pbuf.at[sl], w_sem.at[1, sl]).start()

    def tile_wait(t):
        sl = t % 2
        pltpu.make_async_copy(w_out.at[:, columns(0)], wbuf.at[sl], w_sem.at[0, sl]).wait()
        pltpu.make_async_copy(h_seq.at[seq_rows(0), columns(0)], pbuf.at[sl], w_sem.at[1, sl]).wait()

    def o_load(c):
        n = seq // 2
        return [pltpu.make_async_copy(o_hbm.at[pl.ds(aligned(c * seq + k * n, n), n)], o_c.at[k], o_sem.at[k]) for k in range(2)]

    def y_sent(n):
        r = y_all.at[pl.ds(0, group - 1), :, columns(0)]
        return remote(r, r, y_send.at[n], y_recv.at[0], mate)

    def y_own_copy(c, n):
        return pltpu.make_async_copy(y_t.at[n, me], y_all.at[me * seqs + c, :, columns(n)], y_own.at[n])

    def out_tile(c, n, sl):
        y = pbuf[sl].astype(F32) + dot_nn(o_c[...].reshape(seq, dim), wbuf[sl])

        @pl.when(c > 0)
        def _():
            y_sent(n).wait_send()
            y_own_copy(0, n).wait()

        y_t[n] = y.astype(BF).reshape(group, loc, TN)
        for j in ORDER:
            peer = flipped(me, j)
            remote(y_t.at[n, peer], y_all.at[me * seqs + c, :, columns(n)], y_send.at[n], y_recv.at[c], peer).start()
        y_own_copy(c, n).start()

    def run_block(b):
        is_out, c_out, q = block(b)
        c, third = q // 3, q % 3

        @pl.when(is_out)
        def _():
            for x in o_load(c_out):
                x.wait()

        @pl.when(jnp.logical_and(jnp.logical_not(is_out), third == 2))
        def _():
            pltpu.make_async_copy(h_seq.at[seq_rows(c)], h_v, dh_sem.at[0]).start()
            pltpu.make_async_copy(do_seq.at[seq_rows(c)], dout_v, dh_sem.at[1]).start()

        @pl.loop(0, per)
        def _(n):
            t = b * per + n
            sl = t % 2

            @pl.when(jnp.logical_and(t != per - 1, t + 1 < n_blocks * per))
            def _():
                tile_start(t + 1)

            tile_wait(t)

            @pl.when(is_out)
            def _():
                out_tile(c_out, n, sl)

            @pl.when(jnp.logical_not(is_out))
            def _():
                part = dot_nt(pbuf[sl], wbuf[sl])
                first = jnp.logical_and(third == 0, n == 0)

                @pl.when(first)
                def _():
                    dn_acc[...] = part

                @pl.when(jnp.logical_not(first))
                def _():
                    dn_acc[...] += part

        @pl.when(jnp.logical_and(is_out, jnp.logical_and(c_out > 0, c_out + 1 < seqs)))
        def _():
            for x in o_load(c_out + 1):
                x.start()

        @pl.when(jnp.logical_and(jnp.logical_not(is_out), third == 2))
        def _():
            norm_back(c)

    def norm_back(c):
        pltpu.make_async_copy(h_seq.at[seq_rows(c)], h_v, dh_sem.at[0]).wait()
        pltpu.make_async_copy(do_seq.at[seq_rows(c)], dout_v, dh_sem.at[1]).wait()

        @pl.when(c > 0)
        def _():
            pltpu.make_async_copy(dh_v, dh_hbm.at[:, 0], dh_sem.at[2]).wait()

        gain = gain_ref[...].astype(F32).reshape(1, dim)

        @pl.loop(0, group)
        def _(b):
            r = pl.ds(aligned(b * loc, loc), loc)
            h = h_v[r].astype(F32)
            inv = lax.rsqrt(jnp.mean(h * h, axis=-1, keepdims=True) + NORM_EPS)
            dn = dn_acc[r].astype(BF).astype(F32)
            dg = jnp.sum(dn * h * inv, axis=0, keepdims=True)
            ds = dn * gain
            dh = dout_v[r].astype(F32) + inv * ds - h * (inv * inv * inv) * jnp.mean(ds * h, axis=-1, keepdims=True)
            dh_v[b] = dh.astype(BF)
            first = jnp.logical_and(c == 0, b == 0)

            @pl.when(first)
            def _():
                dg_all[me] = dg

            @pl.when(jnp.logical_not(first))
            def _():
                dg_all[me] += dg

        @pl.when(c < by_xla)
        def _():
            pltpu.make_async_copy(dh_v, dh_hbm.at[:, c], dh_sem.at[2]).start()

        @pl.when(c >= by_xla)
        def _():
            pltpu.make_async_copy(dh_v, dh_loc.at[:, c - by_xla], dh_sem.at[2]).start()

    def dh_send(q):
        k, cols = q // 4, pl.ds(aligned((q % 4) * (dim // 4), dim // 4), dim // 4)
        for j in ORDER:
            peer = flipped(me, j)
            remote(dh_loc.at[peer, k, :, cols], dh_all.at[me, k, :, cols], x_send.at[q], x_recv.at[q], peer).start()
        pltpu.make_async_copy(dh_loc.at[me, k, :, cols], dh_all.at[me, k, :, cols], own_sem.at[q]).start()

    def dh_wait(q):
        r = dh_all.at[pl.ds(0, group - 1), 0, :, pl.ds(0, dim // 4)]
        done = remote(r, r, x_send.at[q], x_recv.at[q], mate)
        done.wait_recv()
        done.wait_send()
        pltpu.make_async_copy(dh_loc.at[0, 0, :, pl.ds(0, dim // 4)], dh_all.at[0, 0, :, pl.ds(0, dim // 4)], own_sem.at[q]).wait()

    def my_rows(c):
        return pl.ds(aligned(c * seq + me * loc, loc), loc)

    def from_all(dst, ss, rs):
        r = dst.at[pl.ds(0, (group - 1) * loc)]
        return remote(r, r, ss, rs, mate)

    def send_all(src, dst, ss, rs, c):
        for j in ORDER:
            peer = flipped(me, j)
            to = dh_v.at[me] if dst is do_seq and c == seqs - 1 else dst.at[my_rows(c)]
            remote(src.at[peer * seqs + c], to, ss.at[c], rs.at[c], peer).start()

    def project(c):
        rows = seq_rows(c)
        from_all(h_seq, h_send.at[c], h_recv.at[c]).wait_recv()
        load = pltpu.make_async_copy(h_seq.at[rows], h_v, ld_sem)
        load.start()
        load.wait()
        gain = gain_ref[...].astype(F32).reshape(1, dim)
        blk = 128

        @pl.loop(0, seq // blk)
        def _(b):
            r = pl.ds(aligned(b * blk, blk), blk)
            h = h_v[r].astype(F32)
            inv = lax.rsqrt(jnp.mean(h * h, axis=-1, keepdims=True) + NORM_EPS)
            n = (h * inv * gain).astype(BF)
            dout_v[r] = n
            lhs[:, pl.ds(aligned(c * seq + b * blk, blk), blk)] = n.T

        @pl.loop(0, 3 * per)
        def _(n):
            t = c * 3 * per + n
            sl = t % 2

            @pl.when(t + 1 < seqs * 3 * per)
            def _():
                qkv_w(t + 1).start()

            qkv_w(t).wait()
            proj = dot_nn(dout_v[...], wbuf[sl])

            @pl.when(t >= 2)
            def _():
                qkv_out(t).wait()

            @pl.when(n < 2 * per)
            def _():
                for h in range(TN // 128):
                    cols = slice(h * 128, (h + 1) * 128)
                    pbuf[sl, :, cols] = rotate(proj[:, cols], tabs[:, :HEAD], tabs[:, HEAD:]).astype(BF)

            @pl.when(n >= 2 * per)
            def _():
                pbuf[sl] = proj.astype(BF)

            qkv_out(t).start()

    def qkv_w(t):
        return pltpu.make_async_copy(w_qkv.at[:, columns(t % (3 * per))], wbuf.at[t % 2], w_sem.at[0, t % 2])

    def qkv_out(t):
        n = t % (3 * per)
        return pltpu.make_async_copy(pbuf.at[t % 2], qkv.at[n // per, seq_rows(t // (3 * per)), columns(n % per)], w_sem.at[1, t % 2])

    def gradient_in():
        for t in range(2):
            qkv_out(t).wait()
        attn_in(0, start)
        for c in range(seqs - 1):
            from_all(do_seq, d_send.at[c], d_recv.at[c]).wait_recv()
            rows = seq_rows(c)
            if c == 0:
                loads = [pltpu.make_async_copy(do_seq.at[rows], h_v, ld_sem)]
            else:
                loads = [pltpu.make_async_copy(do_seq.at[rows, pl.ds(n * TN, TN)], wbuf.at[c - 1, pl.ds(n * TN, TN)], x_send.at[n]) for n in range(per)]
            for x in loads:
                x.start()
            for x in loads:
                x.wait()
            if c == 0:
                pl.loop(0, pairs)(attn_step)
                attn_out_wait(pairs - 2)
                attn_out_wait(pairs - 1)
                for x in o_load(0):
                    x.start()
                tile_start(0)
                run_block(0)
                attn_in(pairs, start)
            else:
                pl.loop(pairs + 2 * c - 2, pairs + 2 * c)(attn_step)
        from_all(do_seq, d_send.at[seqs - 1], d_recv.at[seqs - 1]).wait_recv()
        last_copy().start()
        attn_step(n_early - 2)

    def last_copy():
        dst = do_seq.at[seq_rows(seqs - 1)]
        return pltpu.make_async_copy(dh_v, dst.reshape(group, loc, dim), ld_sem)

    by_xla = dh_hbm.shape[1]

    def own_in(k):
        src = hidden if k < seqs else d_out
        to = dh_v.at[me] if k == 2 * seqs - 1 else dout_v.at[pl.ds(k * loc, loc)]
        return pltpu.make_async_copy(src.at[me * seqs + k % seqs], to, own_sem.at[k])

    def own_out(k):
        dst = h_seq if k < seqs else do_seq
        return pltpu.make_async_copy(dout_v.at[pl.ds(k * loc, loc)], dst.at[my_rows(k % seqs)], own_sem.at[k])

    barrier = pltpu.get_barrier_semaphore()
    for j in reversed(ORDER):
        pl.semaphore_signal(barrier, inc=1, device_id=(flipped(me, j),), device_id_type=MESH)
    for k in range(2 * seqs):
        own_in(k).start()
    qkv_w(0).start()
    mine = pl.ds(aligned(me * loc, loc), loc)
    tab[...] = jnp.concatenate([cos_ref[...], sin_ref[...]], axis=1)
    tab_all[mine] = tab[...]
    pl.semaphore_wait(barrier, group - 1)
    for j in ORDER:
        remote(tab, tab_all.at[mine], t_send, t_recv, flipped(me, j)).start()
    for c in range(seqs):
        send_all(hidden, h_seq, h_send, h_recv, c)
    for c in range(seqs):
        send_all(d_out, do_seq, d_send, d_recv, c)
    for k in range(2 * seqs):
        own_in(k).wait()
        if k < 2 * seqs - 1:
            own_out(k).start()
    from_all(tab_all, t_send, t_recv).wait_recv()
    table = tab_all[...]
    swapped = pltpu.roll(table, 64, 1)
    left = lax.broadcasted_iota(jnp.int32, table.shape, 1) < 64
    tabs[:, :HEAD] = jnp.where(left, table, swapped)
    tabs[:, HEAD:] = jnp.where(left, -swapped, table)
    for k in range(2 * seqs - 1):
        own_out(k).wait()
    pl.loop(0, seqs)(project)
    gradient_in()

    first_out = 3 * (pairs - 1)
    first_dn = first_out + seqs

    def step(i, carry):
        def guarded(lag, fn):
            u = i - lag

            @pl.when(jnp.logical_and(u >= 0, u < n_all))
            def _():
                fn(u)

        def ag0(u):
            ag_all(u, 0).wait_recv()

        def ag1(u):
            ag_all(u, 1).wait_recv()
            ag_mate(u, True)

        def ag2(u):
            ag_all(u, 2).wait_recv()
            ag_start(u, 1)

            @pl.when(u >= NS)
            def _():
                ag_all(u, 0).wait_send()

            ag_mate(u, False)

        def ag3(u):
            ag_all(u, 3).wait_recv()
            ag_all(u, 3).wait_send()
            local_wait(u)
            ag_start(u, 2)

        def last(u):
            rs_finish(u, 3)
            local_start(u)
            ag_start(u, 3)

        def middle(t):
            def fn(u):
                rs_finish(u, t)
                rs_start(u, t + 1)
            return fn

        guarded(0, dw_tile)

        from_a, to_a = [n_early - 1 + jnp.where(k > 2, k - 1, 0) for k in (i, i + 1)]

        @pl.when(jnp.logical_and(i % 3 == 0, jnp.logical_and(i >= 3, i < first_out)))
        def _():
            first_seq(i // 3 + 1).start()

        @pl.when(i < first_out)
        def _():
            pl.loop(from_a, jnp.minimum(to_a, n_attn))(attn_step)

        for lag, fn in enumerate((middle(0), middle(1), middle(2), last, ag3, ag2, ag1, ag0)):
            guarded(lag + 1, fn)

        @pl.when(i == first_out)
        def _():
            attn_out_wait(n_attn - 2)
            attn_out_wait(n_attn - 1)
            for x in o_load(1):
                x.start()
            tile_start(per)

        def blocks(i):
            k = i - first_out
            return jnp.where(k <= seqs, jnp.maximum(3 * k - 1, 1), jnp.minimum(k + 2 * seqs, n_blocks))

        @pl.when(i >= first_out)
        def _():
            pl.loop(blocks(i), blocks(i + 1))(run_block)

        @pl.when(i == 3)
        def _():
            last_copy().wait()

        first_dh = first_dn + seqs

        @pl.when(i == first_dh)
        def _():
            pltpu.make_async_copy(dh_v, dh_hbm.at[:, 0], dh_sem.at[2]).wait()
            for j in range(1, group):
                remote(dg_all.at[me], dg_all.at[me], dg_send, dg_recv, flipped(me, j)).start()

        @pl.when(jnp.logical_and(i >= first_dh, i < first_dh + 4 * (seqs - by_xla)))
        def _():
            dh_send(i - first_dh)

        return carry

    lax.fori_loop(0, n_all + 8, step, 0)

    for c in range(seqs):
        r = y_all.at[pl.ds(0, group - 1)]
        remote(r, r, y_send.at[0], y_recv.at[c], mate).wait_recv()
        from_all(h_seq, h_send.at[c], h_recv.at[c]).wait_send()
        from_all(do_seq, d_send.at[c], d_recv.at[c]).wait_send()
    for n in range(per):
        y_sent(n).wait_send()
        y_own_copy(0, n).wait()
    from_all(tab_all, t_send, t_recv).wait_send()
    for q in range(4 * (seqs - by_xla)):
        dh_wait(q)
    r = dg_all.at[pl.ds(0, group - 1)]
    others = remote(r, r, dg_send, dg_recv, mate)
    others.wait_recv()
    others.wait_send()
    dgain = dg_all[0]
    for j in range(1, group):
        dgain = dgain + dg_all[j]
    dgain_ref[...] = dgain.reshape(dim)
    for j in range(NS):
        u = n_all - NS + j
        for t in range(4):
            pl.semaphore_wait(credit.at[t, u % NS], 1 if t == 0 else 3)
            if t < 3:
                ag_all(u, t).wait_send()


BY_XLA = 2


def main_call(hidden, d_out, cos_tab, sin_tab, w_qkv, w_out, gain):
    n, loc, dim = hidden.shape
    group = 16
    rows = n * loc
    seqs = n // group
    seq = loc * group
    h = dim // 2
    n_all = 4 * dim // TW
    hbm = pl.BlockSpec(memory_space=pl.ANY)
    vmem = pl.BlockSpec(memory_space=pltpu.VMEM)
    D = pltpu.SemaphoreType.DMA
    S = jax.ShapeDtypeStruct
    V = pltpu.VMEM
    act = S((rows, dim), BF)
    return pl.pallas_call(
        functools.partial(main_kernel, 128 ** -0.5),
        in_specs=[hbm] * 2 + [vmem] * 2 + [hbm] * 2 + [vmem],
        out_specs=[hbm] * 11 + [vmem],
        out_shape=[S((dim, 4 * dim), F32), act, act, S((3, rows, dim), BF),
                   act, S((dim, rows), BF), S((3, rows, dim), BF), S((n, loc, dim), BF),
                   S((group, BY_XLA, loc, dim), BF), S((group, seqs - BY_XLA, loc, dim), BF), S((group, seqs - BY_XLA, loc, dim), BF), S((dim,), F32)],
        scratch_shapes=[
            V((dim, rows), BF), V((2, 3, rows, TW), BF), V((NB, dim, TW), F32),
            V((NS, h, TW), F32), V((NS, h >> 1, TW), F32), V((NS, h >> 2, TW), F32), V((NS, h >> 3, TW), F32),
            V((2, 3, seq, TW), BF), V((2, seq, TW), BF), V((2, seq, TW), BF), V((2, TW, seq), BF), V((seq, 256), F32), V((loc, 128), F32), V((seq, 128), F32),
            V((seq, dim), F32), V((seq, dim), BF), V((seq, dim), BF), V((group, loc, dim), BF), V((group, 1, dim), F32),
            V((2, dim, 512), BF), V((2, seq, 512), BF), V((2, seq // 2, dim), BF), V((dim // 512, group, loc, 512), BF),
            D, D, D((4, NS)), D((4, NS)), pltpu.SemaphoreType.REGULAR((4, NS)), D((NS,)), D((4, NS)), D((4, n_all)),
            D((2, 2)), D((3, 2)), D((3,)), D((3,)), D, D, D((2, 2)), D((2,)), D((2,)),
            D((seqs,)), D((seqs,)), D((seqs,)), D((seqs,)), D, D, D((2 * seqs,)), D((dim // 512,)), D((seqs,)), D((dim // 512,)), D((4 * (seqs - BY_XLA),)), D((4 * (seqs - BY_XLA),)),
        ],
        compiler_params=pltpu.CompilerParams(collective_id=0, has_side_effects=True, vmem_limit_bytes=67043328),
        cost_estimate=pl.CostEstimate(flops=28 * rows * dim * dim, bytes_accessed=90 * dim * dim, transcendentals=0),
        name="main",
    )(hidden, d_out, cos_tab, sin_tab, w_qkv, w_out, gain)


def place_kernel(y_in, b_in, y_out, dh_out):
    y_out[...] = y_in[...]
    dh_out[...] = b_in[...]


def place_call(y, b):
    n, loc, dim = y.shape
    group, k = b.shape[:2]
    seqs = n // group
    return pl.pallas_call(
        place_kernel,
        grid=(2,),
        in_specs=[pl.BlockSpec((n // 2, loc, dim), lambda j: (j, 0, 0)), pl.BlockSpec((group // 2, k, loc, dim), lambda j: (j, 0, 0, 0))],
        out_specs=[pl.BlockSpec((n // 2, loc, dim), lambda j: (j, 0, 0)), pl.BlockSpec((group // 2, k, loc, dim), lambda j: (j, seqs // k - 1, 0, 0))],
        out_shape=[jax.ShapeDtypeStruct((n, loc, dim), BF), jax.ShapeDtypeStruct((group, seqs, loc, dim), BF)],
        cost_estimate=pl.CostEstimate(flops=8 * n * loc * dim, bytes_accessed=6 * n * loc * dim, transcendentals=0),
        name="place",
    )(y, b)


def fill_kernel(a_in, dh_in, dh_out):
    dh_out[...] = a_in[...]


def fill_call(a, dh):
    group, k, loc, dim = a.shape
    return pl.pallas_call(
        fill_kernel,
        grid=(2,),
        in_specs=[pl.BlockSpec((group // 2, k, loc, dim), lambda j: (j, 0, 0, 0)), pl.BlockSpec(memory_space=pl.ANY)],
        out_specs=pl.BlockSpec((group // 2, k, loc, dim), lambda j: (j, 0, 0, 0)),
        out_shape=jax.ShapeDtypeStruct(dh.shape, BF),
        input_output_aliases={1: 0},
        name="fill",
    )(a, dh)


def solution(mesh):
    group = mesh.shape['sp']
    token_spec = P(None, 'sp', None)
    table_spec = P('sp', None)

    def device_step(hidden, norm_gain, w_qkv, w_out, cos_tab, sin_tab, d_out):
        num_seqs, local_len, dim = hidden.shape
        dw, _, _, _, _, _, _, y, dh_a, _, dh_b, dgain = main_call(hidden, d_out, cos_tab, sin_tab, w_qkv, w_out, norm_gain)
        dh_a = lax.all_to_all(dh_a, 'sp', split_axis=0, concat_axis=0, tiled=True)
        y, dh = place_call(y, dh_b)
        dh = fill_call(dh_a, dh).reshape(num_seqs, local_len, dim)
        return y, dh, dw[:, :3 * dim], dw[:, 3 * dim:], dgain

    return jax.shard_map(device_step, mesh=mesh, in_specs=(token_spec, P(), P(), P(), table_spec, table_spec, token_spec), out_specs=(token_spec, token_spec, P(), P(), P()), check_vma=False)
```

```python
import functools
import jax
import jax.numpy as jnp
from jax import lax
from jax.experimental import pallas as pl
from jax.experimental.pallas import tpu as pltpu
from jax.sharding import PartitionSpec as P

NORM_EPS = 1e-6
HEAD = 128
BF = jnp.bfloat16
F32 = jnp.float32
VMEM_LIMIT = 60 * 1024 * 1024


def dot_nn(a, b):
    return lax.dot_general(a, b, (((1,), (0,)), ((), ())), preferred_element_type=F32)


def dot_nt(a, b):
    return lax.dot_general(a, b, (((1,), (1,)), ((), ())), preferred_element_type=F32)


def rotate(u, cos, sin_signed):
    return u * cos + pltpu.roll(u, 64, 1) * sin_signed


def unrotate(u, cos, sin_signed):
    return u * cos - pltpu.roll(u, 64, 1) * sin_signed


MESH = pl.DeviceIdType.MESH


def flipped(me, j):
    p = me
    for b in range(4):
        w = 1 << b
        if j & w:
            p = p + w * (1 - 2 * ((me // w) % 2))
    return p


ORDER = tuple(int(j, 16) for j in '2481359' + '6ac7bdef')


TW = 256
PARTS = ((0, 384), (384, 320), (704, 320))
NS = 3
NB = 6
BLK = 256


def attend(scale, qkv, do, tabs, o_out, o_t_out, dproj_out):
    seq = qkv.shape[1]
    for h in range(2):
        cols = slice(h * 128, (h + 1) * 128)
        q = qkv[0, :, cols]
        k = qkv[1, :, cols]
        v = qkv[2, :, cols]
        dout = do[:, cols]
        k_t = k.T
        v_t = v.T
        dk = [None] * (seq // BLK)
        dv = [None] * (seq // BLK)
        for j in range(seq // BLK):
            end = (j + 1) * BLK
            rows = slice(j * BLK, end)
            q_j = q[rows]
            do_j = dout[rows]
            s = dot_nt(k[:end], q_j)
            row = lax.broadcasted_iota(jnp.int32, (end, BLK), 0)
            col = lax.broadcasted_iota(jnp.int32, (end, BLK), 1) + j * BLK
            s = jnp.where(row <= col, s * scale, -1e30)
            m = jnp.max(s, axis=0, keepdims=True)
            e = jnp.exp(s - m)
            p = e * (1.0 / jnp.sum(e, axis=0, keepdims=True))
            p_bf = p.astype(BF)
            o_t = dot_nn(v_t[:, :end], p_bf)
            dp = dot_nt(v[:end], do_j).astype(BF).astype(F32)
            delta = jnp.sum(p * dp, axis=0, keepdims=True)
            ds = (p * (dp - delta) * scale).astype(BF)
            dv_j = dot_nn(p_bf, do_j)
            dk_j = dot_nn(ds, q_j)
            dq_t = dot_nn(k_t[:, :end], ds)
            for i in range(j + 1):
                part = slice(i * BLK, (i + 1) * BLK)
                dv[i] = dv_j[part] if dv[i] is None else dv[i] + dv_j[part]
                dk[i] = dk_j[part] if dk[i] is None else dk[i] + dk_j[part]
            o_out[rows, cols] = o_t.T.astype(BF)
            o_t_out[cols, rows] = o_t.astype(BF)
            dq = dq_t.T.astype(BF).astype(F32)
            dproj_out[0, rows, cols] = unrotate(dq, tabs[rows, :HEAD], tabs[rows, HEAD:]).astype(BF)
        for j in range(seq // BLK):
            rows = slice(j * BLK, (j + 1) * BLK)
            dkj = dk[j].astype(BF).astype(F32)
            dproj_out[1, rows, cols] = unrotate(dkj, tabs[rows, :HEAD], tabs[rows, HEAD:]).astype(BF)
            dproj_out[2, rows, cols] = dv[j].astype(BF)


def main_kernel(scale, hidden, d_out, cos_ref, sin_ref, w_qkv, w_out, gain_ref,
                g_hbm, h_seq, do_seq, qkv, o_hbm, o_t_hbm, dproj_hbm, y_all, dh_hbm, dh_loc, dh_all, dgain_ref,
                lhs, dproj_v, acc, r0, r1, r2, r3, qkv_v, do_v, o_v, o_t_v, tabs, tab, tab_all, dn_acc, h_v, dout_v, dh_v, dg_all, wbuf, pbuf, o_c, y_t,
                lhs_sem, ld_sem, s_send, s_recv, credit, loc_sem, g_send, g_recv,
                in_sem, out_sem, rhs_sem, dh_sem, dg_send, dg_recv, w_sem, o_sem, c0_sem,
                h_send, h_recv, d_send, d_recv, t_send, t_recv, own_sem, y_send, y_recv, y_own, x_send, x_recv):
    me = lax.axis_index('sp')
    group = 16
    loc, dim = hidden.shape[1:]
    seqs = hidden.shape[0] // group
    seq = loc * group
    half = dim // 2
    n_qkv = 3 * dim // TW
    n_all = 4 * dim // TW
    pairs = dim // TW
    core = me % 2
    mate = me + 1 - 2 * core
    recv = (r0, r1, r2, r3)
    TN = 512
    per = dim // TN

    def remote(src, dst, ss, rs, peer):
        return pltpu.make_async_remote_copy(src_ref=src, dst_ref=dst, send_sem=ss, recv_sem=rs, device_id=(peer,), device_id_type=MESH)

    def link(d):
        w = 2 + d + d * d
        bit = (me // w) % 2
        return bit, me + w * (1 - 2 * bit)

    def aligned(x, n):
        return pl.multiple_of(x, n)

    def dims(u, p, t):
        return (u + p + t - 1) % 3

    def offs(u, p, size):
        o = [0]
        for t in (1, 2, 3):
            b, _ = link(dims(u, p, t))
            o.append(o[-1] + b * (size >> t))
        return o

    def rs_all(u, t):
        sl = u % NS
        return remote(recv[t].at[sl], recv[t].at[sl], s_send.at[t, sl], s_recv.at[t, sl], mate)

    def rs_start(u, t):
        sl, nb = u % NS, u % NB

        @pl.when(u >= NS)
        def _():
            pl.semaphore_wait(credit.at[t, sl], 1 if t == 0 else 3)

        if t == 0:
            n = half // 4
            for k in range(4):
                src = acc.at[nb, pl.ds(aligned((1 - core) * half + k * n, n), n)]
                remote(src, r0.at[sl, pl.ds(k * n, n)], s_send.at[0, sl], s_recv.at[0, sl], mate).start()
            return
        for p, (base, size) in enumerate(PARTS):
            o = offs(u, p, size)
            n = size >> t
            b, peer = link(dims(u, p, t))
            row = core * half + base + o[t - 1] + (1 - b) * n
            remote(acc.at[nb, pl.ds(aligned(row, 8), n)], recv[t].at[sl, pl.ds(base >> t, n)],
                   s_send.at[t, sl], s_recv.at[t, sl], peer).start()

    def rs_finish(u, t):
        sl, nb = u % NS, u % NB
        rs_all(u, t).wait_recv()
        rs_all(u, t).wait_send()
        if t == 0:
            rows = pl.ds(aligned(core * half, half), half)
            acc[nb, rows] = acc[nb, rows] + r0[sl]
            pl.semaphore_signal(credit.at[0, sl], inc=1, device_id=(mate,), device_id_type=MESH)
            return
        for p, (base, size) in enumerate(PARTS):
            n = size >> t
            rows = pl.ds(aligned(core * half + base + offs(u, p, size)[t], 8), n)
            acc[nb, rows] = acc[nb, rows] + recv[t][sl, pl.ds(base >> t, n)]
            pl.semaphore_signal(credit.at[t, sl], inc=1, device_id=(link(dims(u, p, t))[1],), device_id_type=MESH)

    def tile_col(u):
        return jnp.where(u < n_qkv, (u % 3) * pairs + u // 3, u) * TW

    def g_at(u, row, n):
        return g_hbm.at[pl.ds(aligned(row, 8), n), pl.ds(aligned(tile_col(u), TW), TW)]

    def ag_all(u, t):
        r = g_hbm.at[pl.ds(0, half >> t), pl.ds(0, TW)]
        return remote(r, r, g_send.at[t, u % NS], g_recv.at[t, u], mate)

    def ag_mate(u, late):
        for p, (base, size) in enumerate(PARTS):
            n = size >> 1
            b, _ = link(dims(u, p, 1))
            r = g_at(u, core * half + base + (1 - b if late else b) * n, n)
            remote(r, r, g_send.at[0, u % NS], g_recv.at[0, u], mate).start()

    def ag_start(u, t):
        if t < 3:
            @pl.when(u >= NS)
            def _():
                ag_all(u, t).wait_send()

        for p, (base, size) in enumerate(PARTS):
            n = size >> t
            row = core * half + base + offs(u, p, size)[t]
            dst = g_at(u, row, n)
            src = acc.at[u % NB, pl.ds(aligned(row, 8), n)] if t == 3 else dst
            remote(src, dst, g_send.at[t, u % NS], g_recv.at[t, u], link(dims(u, p, t))[1]).start()

    def local_start(u):
        for p, (base, size) in enumerate(PARTS):
            n = size >> 3
            row = core * half + base + offs(u, p, size)[3]
            pltpu.make_async_copy(acc.at[u % NB, pl.ds(aligned(row, 8), n)], g_at(u, row, n), loc_sem.at[u % NS]).start()

    def local_wait(u):
        n = half >> 3
        pltpu.make_async_copy(acc.at[0, pl.ds(0, n)], g_hbm.at[pl.ds(0, n), pl.ds(0, TW)], loc_sem.at[u % NS]).wait()

    n_attn = seqs * pairs
    n_early = pairs + 2 * (seqs - 1)

    def place(a):
        b, c = a - pairs, a - n_early
        s = jnp.where(a < pairs, 0, 1 + jnp.where(c < 0, b // 2, c % (seqs - 1)))
        p = jnp.where(a < pairs, a, jnp.where(c < 0, b % 2, 2 + c // (seqs - 1)))
        return s, p, seq_rows(s), pl.ds(aligned(p * TW, TW), TW)

    def seq_rows(c):
        return pl.ds(aligned(c * seq, seq), seq)

    def attn_in(a, fn):
        _, _, rows, cols = place(a)
        sl = a % 2
        fn(pltpu.make_async_copy(qkv.at[:, rows, cols], qkv_v.at[sl], in_sem.at[0, sl]))
        fn(pltpu.make_async_copy(w_out.at[cols], o_c.at[sl], in_sem.at[1, sl]))

    def start(copy):
        copy.start()

    def wait(copy):
        copy.wait()

    def dproj_rows(a):
        s, p, _, _ = place(a)
        return dproj_v.at[p % 2, :, seq_rows(jnp.where(jnp.logical_and(s == 0, p >= 2), seqs - 1, s))]

    def attn_out(a):
        _, _, rows, cols = place(a)
        sl = a % 2
        return (pltpu.make_async_copy(o_v.at[sl], o_hbm.at[rows, cols], out_sem.at[0, sl]),
                pltpu.make_async_copy(o_t_v.at[sl], o_t_hbm.at[cols, rows], out_sem.at[1, sl]),
                pltpu.make_async_copy(dproj_rows(a), dproj_hbm.at[:, rows, cols], out_sem.at[2, sl]))

    def attn_out_wait(a):
        for c in attn_out(a):
            c.wait()

    def attn_step(a):
        @pl.when(jnp.logical_and(a != pairs - 1, a + 1 < n_attn))
        def _():
            attn_in(a + 1, start)

        attn_in(a, wait)

        @pl.when(jnp.logical_and(a >= 2, a // 2 != pairs // 2))
        def _():
            attn_out_wait(a)

        s, _, _, _ = place(a)
        sl = a % 2

        @pl.when(s == 0)
        def _():
            do_v[sl] = dot_nt(h_v[...], o_c[sl]).astype(BF)

        @pl.when(jnp.logical_and(s > 0, s < seqs - 1))
        def _():
            total = None
            for n in range(per):
                cols = slice(n * TN, (n + 1) * TN)
                part = dot_nt(wbuf[s - 1, cols], o_c[sl, :, cols])
                total = part if total is None else total + part
            do_v[sl] = total.astype(BF)

        @pl.when(s == seqs - 1)
        def _():
            do_v[sl] = dot_nt(dh_v[...].reshape(seq, dim), o_c[sl]).astype(BF)

        attend(scale, qkv_v.at[sl], do_v.at[sl], tabs, o_v.at[sl], o_t_v.at[sl], dproj_rows(a))
        for c in attn_out(a):
            c.start()

    def first_seq(p):
        rows = seq_rows(0)
        return pltpu.make_async_copy(dproj_hbm.at[:, rows, pl.ds(aligned(p * TW, TW), TW)], dproj_v.at[p % 2, :, rows], c0_sem.at[p % 2])

    def rhs_copy(u):
        j = u - n_qkv
        return pltpu.make_async_copy(do_seq.at[:, pl.ds(aligned(j * TW, TW), TW)], dproj_v.at[0, j % 3], rhs_sem.at[j % 3])

    def dw_tile(u):
        @pl.when(u == n_qkv)
        def _():
            pltpu.make_async_copy(o_t_hbm, lhs, lhs_sem).wait()

        @pl.when(u >= n_qkv)
        def _():
            rhs_copy(u).wait()

        @pl.when(jnp.logical_and(u % 3 == 0, jnp.logical_and(u >= 6, u < n_qkv)))
        def _():
            first_seq(u // 3).wait()

        p = jnp.where(u < n_qkv, (u // 3) % 2, 0)

        def half_tile(mine):
            @pl.loop(0, half // TN)
            def _(b):
                rows = pl.ds(aligned(mine * half + b * TN, TN), TN)
                acc[u % NB, rows] = dot_nn(lhs[rows], dproj_v[p, u % 3])

        half_tile(1 - core)
        rs_start(u, 0)
        half_tile(core)

        @pl.when(u == n_qkv - 1)
        def _():
            pltpu.make_async_copy(o_t_hbm, lhs, lhs_sem).start()

        @pl.when(jnp.logical_and(u + 2 >= n_qkv, u + 2 < n_all))
        def _():
            rhs_copy(u + 2).start()

    n_blocks = 4 * seqs

    def columns(n):
        return pl.ds(aligned(n * TN, TN), TN)

    def block(b):
        is_out = jnp.logical_or(b == 0, jnp.logical_and((b + 1) % 3 == 0, b <= 3 * seqs - 4))
        done = jnp.minimum((b + 1) // 3, seqs - 1)
        return is_out, done, b - 1 - done

    def tile_start(t):
        b, n, sl = t // per, t % per, t % 2
        is_out, c, q = block(b)

        @pl.when(is_out)
        def _():
            pltpu.make_async_copy(w_out.at[:, columns(n)], wbuf.at[sl], w_sem.at[0, sl]).start()
            pltpu.make_async_copy(h_seq.at[seq_rows(c), columns(n)], pbuf.at[sl], w_sem.at[1, sl]).start()

        @pl.when(jnp.logical_not(is_out))
        def _():
            pltpu.make_async_copy(w_qkv.at[:, columns((q % 3) * per + n)], wbuf.at[sl], w_sem.at[0, sl]).start()
            pltpu.make_async_copy(dproj_hbm.at[q % 3, seq_rows(q // 3), columns(n)], pbuf.at[sl], w_sem.at[1, sl]).start()

    def tile_wait(t):
        sl = t % 2
        pltpu.make_async_copy(w_out.at[:, columns(0)], wbuf.at[sl], w_sem.at[0, sl]).wait()
        pltpu.make_async_copy(h_seq.at[seq_rows(0), columns(0)], pbuf.at[sl], w_sem.at[1, sl]).wait()

    def o_load(c):
        n = seq // 2
        return [pltpu.make_async_copy(o_hbm.at[pl.ds(aligned(c * seq + k * n, n), n)], o_c.at[k], o_sem.at[k]) for k in range(2)]

    def y_sent(n):
        r = y_all.at[pl.ds(0, group - 1), :, columns(0)]
        return remote(r, r, y_send.at[n], y_recv.at[0], mate)

    def y_own_copy(c, n):
        return pltpu.make_async_copy(y_t.at[n, me], y_all.at[me * seqs + c, :, columns(n)], y_own.at[n])

    def out_tile(c, n, sl):
        y = pbuf[sl].astype(F32) + dot_nn(o_c[...].reshape(seq, dim), wbuf[sl])

        @pl.when(c > 0)
        def _():
            y_sent(n).wait_send()
            y_own_copy(0, n).wait()

        y_t[n] = y.astype(BF).reshape(group, loc, TN)
        for j in ORDER:
            peer = flipped(me, j)
            remote(y_t.at[n, peer], y_all.at[me * seqs + c, :, columns(n)], y_send.at[n], y_recv.at[c], peer).start()
        y_own_copy(c, n).start()

    def run_block(b):
        is_out, c_out, q = block(b)
        c, third = q // 3, q % 3

        @pl.when(is_out)
        def _():
            for x in o_load(c_out):
                x.wait()

        @pl.when(jnp.logical_and(jnp.logical_not(is_out), third == 2))
        def _():
            pltpu.make_async_copy(h_seq.at[seq_rows(c)], h_v, dh_sem.at[0]).start()
            pltpu.make_async_copy(do_seq.at[seq_rows(c)], dout_v, dh_sem.at[1]).start()

        @pl.loop(0, per)
        def _(n):
            t = b * per + n
            sl = t % 2

            @pl.when(jnp.logical_and(t != per - 1, t + 1 < n_blocks * per))
            def _():
                tile_start(t + 1)

            tile_wait(t)

            @pl.when(is_out)
            def _():
                out_tile(c_out, n, sl)

            @pl.when(jnp.logical_not(is_out))
            def _():
                part = dot_nt(pbuf[sl], wbuf[sl])
                first = jnp.logical_and(third == 0, n == 0)

                @pl.when(first)
                def _():
                    dn_acc[...] = part

                @pl.when(jnp.logical_not(first))
                def _():
                    dn_acc[...] += part

        @pl.when(jnp.logical_and(is_out, jnp.logical_and(c_out > 0, c_out + 1 < seqs)))
        def _():
            for x in o_load(c_out + 1):
                x.start()

        @pl.when(jnp.logical_and(jnp.logical_not(is_out), third == 2))
        def _():
            norm_back(c)

    def norm_back(c):
        pltpu.make_async_copy(h_seq.at[seq_rows(c)], h_v, dh_sem.at[0]).wait()
        pltpu.make_async_copy(do_seq.at[seq_rows(c)], dout_v, dh_sem.at[1]).wait()

        @pl.when(c > 0)
        def _():
            pltpu.make_async_copy(dh_v, dh_hbm.at[:, 0], dh_sem.at[2]).wait()

        gain = gain_ref[...].astype(F32).reshape(1, dim)

        @pl.loop(0, group)
        def _(b):
            r = pl.ds(aligned(b * loc, loc), loc)
            h = h_v[r].astype(F32)
            inv = lax.rsqrt(jnp.mean(h * h, axis=-1, keepdims=True) + NORM_EPS)
            dn = dn_acc[r].astype(BF).astype(F32)
            dg = jnp.sum(dn * h * inv, axis=0, keepdims=True)
            ds = dn * gain
            dh = dout_v[r].astype(F32) + inv * ds - h * (inv * inv * inv) * jnp.mean(ds * h, axis=-1, keepdims=True)
            dh_v[b] = dh.astype(BF)
            first = jnp.logical_and(c == 0, b == 0)

            @pl.when(first)
            def _():
                dg_all[me] = dg

            @pl.when(jnp.logical_not(first))
            def _():
                dg_all[me] += dg

        @pl.when(c < by_xla)
        def _():
            pltpu.make_async_copy(dh_v, dh_hbm.at[:, c], dh_sem.at[2]).start()

        @pl.when(c >= by_xla)
        def _():
            pltpu.make_async_copy(dh_v, dh_loc.at[:, c - by_xla], dh_sem.at[2]).start()

    def dh_send(q):
        k, cols = q // 4, pl.ds(aligned((q % 4) * (dim // 4), dim // 4), dim // 4)
        for j in ORDER:
            peer = flipped(me, j)
            remote(dh_loc.at[peer, k, :, cols], dh_all.at[me, k, :, cols], x_send.at[q], x_recv.at[q], peer).start()
        pltpu.make_async_copy(dh_loc.at[me, k, :, cols], dh_all.at[me, k, :, cols], own_sem.at[q]).start()

    def dh_wait(q):
        r = dh_all.at[pl.ds(0, group - 1), 0, :, pl.ds(0, dim // 4)]
        done = remote(r, r, x_send.at[q], x_recv.at[q], mate)
        done.wait_recv()
        done.wait_send()
        pltpu.make_async_copy(dh_loc.at[0, 0, :, pl.ds(0, dim // 4)], dh_all.at[0, 0, :, pl.ds(0, dim // 4)], own_sem.at[q]).wait()

    def my_rows(c):
        return pl.ds(aligned(c * seq + me * loc, loc), loc)

    def from_all(dst, ss, rs):
        r = dst.at[pl.ds(0, (group - 1) * loc)]
        return remote(r, r, ss, rs, mate)

    def send_all(src, dst, ss, rs, c):
        for j in ORDER:
            peer = flipped(me, j)
            to = dh_v.at[me] if dst is do_seq and c == seqs - 1 else dst.at[my_rows(c)]
            remote(src.at[peer * seqs + c], to, ss.at[c], rs.at[c], peer).start()

    def project(c):
        rows = seq_rows(c)
        from_all(h_seq, h_send.at[c], h_recv.at[c]).wait_recv()
        load = pltpu.make_async_copy(h_seq.at[rows], h_v, ld_sem)
        load.start()
        load.wait()
        gain = gain_ref[...].astype(F32).reshape(1, dim)
        blk = 128

        @pl.loop(0, seq // blk)
        def _(b):
            r = pl.ds(aligned(b * blk, blk), blk)
            h = h_v[r].astype(F32)
            inv = lax.rsqrt(jnp.mean(h * h, axis=-1, keepdims=True) + NORM_EPS)
            n = (h * inv * gain).astype(BF)
            dout_v[r] = n
            lhs[:, pl.ds(aligned(c * seq + b * blk, blk), blk)] = n.T

        @pl.loop(0, 3 * per)
        def _(n):
            t = c * 3 * per + n
            sl = t % 2

            @pl.when(t + 1 < seqs * 3 * per)
            def _():
                qkv_w(t + 1).start()

            qkv_w(t).wait()
            proj = dot_nn(dout_v[...], wbuf[sl])

            @pl.when(t >= 2)
            def _():
                qkv_out(t).wait()

            @pl.when(n < 2 * per)
            def _():
                for h in range(TN // 128):
                    cols = slice(h * 128, (h + 1) * 128)
                    pbuf[sl, :, cols] = rotate(proj[:, cols], tabs[:, :HEAD], tabs[:, HEAD:]).astype(BF)

            @pl.when(n >= 2 * per)
            def _():
                pbuf[sl] = proj.astype(BF)

            qkv_out(t).start()

    def qkv_w(t):
        return pltpu.make_async_copy(w_qkv.at[:, columns(t % (3 * per))], wbuf.at[t % 2], w_sem.at[0, t % 2])

    def qkv_out(t):
        n = t % (3 * per)
        return pltpu.make_async_copy(pbuf.at[t % 2], qkv.at[n // per, seq_rows(t // (3 * per)), columns(n % per)], w_sem.at[1, t % 2])

    def gradient_in():
        for t in range(2):
            qkv_out(t).wait()
        attn_in(0, start)
        for c in range(seqs - 1):
            from_all(do_seq, d_send.at[c], d_recv.at[c]).wait_recv()
            rows = seq_rows(c)
            if c == 0:
                loads = [pltpu.make_async_copy(do_seq.at[rows], h_v, ld_sem)]
            else:
                loads = [pltpu.make_async_copy(do_seq.at[rows, pl.ds(n * TN, TN)], wbuf.at[c - 1, pl.ds(n * TN, TN)], x_send.at[n]) for n in range(per)]
            for x in loads:
                x.start()
            for x in loads:
                x.wait()
            if c == 0:
                pl.loop(0, pairs)(attn_step)
                attn_out_wait(pairs - 2)
                attn_out_wait(pairs - 1)
                for x in o_load(0):
                    x.start()
                tile_start(0)
                run_block(0)
                attn_in(pairs, start)
            else:
                pl.loop(pairs + 2 * c - 2, pairs + 2 * c)(attn_step)
        from_all(do_seq, d_send.at[seqs - 1], d_recv.at[seqs - 1]).wait_recv()
        last_copy().start()
        attn_step(n_early - 2)

    def last_copy():
        dst = do_seq.at[seq_rows(seqs - 1)]
        return pltpu.make_async_copy(dh_v, dst.reshape(group, loc, dim), ld_sem)

    by_xla = dh_hbm.shape[1]

    def own_in(k):
        src = hidden if k < seqs else d_out
        to = dh_v.at[me] if k == 2 * seqs - 1 else dout_v.at[pl.ds(k * loc, loc)]
        return pltpu.make_async_copy(src.at[me * seqs + k % seqs], to, own_sem.at[k])

    def own_out(k):
        dst = h_seq if k < seqs else do_seq
        return pltpu.make_async_copy(dout_v.at[pl.ds(k * loc, loc)], dst.at[my_rows(k % seqs)], own_sem.at[k])

    barrier = pltpu.get_barrier_semaphore()
    for j in reversed(ORDER):
        pl.semaphore_signal(barrier, inc=1, device_id=(flipped(me, j),), device_id_type=MESH)
    for k in range(2 * seqs):
        own_in(k).start()
    qkv_w(0).start()
    mine = pl.ds(aligned(me * loc, loc), loc)
    tab[...] = jnp.concatenate([cos_ref[...], sin_ref[...]], axis=1)
    tab_all[mine] = tab[...]
    pl.semaphore_wait(barrier, group - 1)
    for j in ORDER:
        remote(tab, tab_all.at[mine], t_send, t_recv, flipped(me, j)).start()
    for c in range(seqs):
        send_all(hidden, h_seq, h_send, h_recv, c)
    for c in range(seqs):
        send_all(d_out, do_seq, d_send, d_recv, c)
    for k in range(2 * seqs):
        own_in(k).wait()
        if k < 2 * seqs - 1:
            own_out(k).start()
    from_all(tab_all, t_send, t_recv).wait_recv()
    table = tab_all[...]
    swapped = pltpu.roll(table, 64, 1)
    left = lax.broadcasted_iota(jnp.int32, table.shape, 1) < 64
    tabs[:, :HEAD] = jnp.where(left, table, swapped)
    tabs[:, HEAD:] = jnp.where(left, -swapped, table)
    for k in range(2 * seqs - 1):
        own_out(k).wait()
    pl.loop(0, seqs)(project)
    gradient_in()

    first_out = 3 * (pairs - 1)
    first_dn = first_out + seqs

    def settle():
        for c in range(seqs):
            r = y_all.at[pl.ds(0, group - 1)]
            remote(r, r, y_send.at[0], y_recv.at[c], mate).wait_recv()
            from_all(h_seq, h_send.at[c], h_recv.at[c]).wait_send()
            from_all(do_seq, d_send.at[c], d_recv.at[c]).wait_send()
        for n in range(per):
            y_sent(n).wait_send()
            y_own_copy(0, n).wait()
        from_all(tab_all, t_send, t_recv).wait_send()
        r = dg_all.at[pl.ds(0, group - 1)]
        others = remote(r, r, dg_send, dg_recv, mate)
        others.wait_recv()
        others.wait_send()
        dgain = dg_all[0]
        for j in range(1, group):
            dgain = dgain + dg_all[j]
        dgain_ref[...] = dgain.reshape(dim)

    def step(i, carry):
        def guarded(lag, fn):
            u = i - lag

            @pl.when(jnp.logical_and(u >= 0, u < n_all))
            def _():
                fn(u)

        def ag0(u):
            ag_all(u, 0).wait_recv()

        def ag1(u):
            ag_all(u, 1).wait_recv()
            ag_mate(u, True)

        def ag2(u):
            ag_all(u, 2).wait_recv()
            ag_start(u, 1)

            @pl.when(u >= NS)
            def _():
                ag_all(u, 0).wait_send()

            ag_mate(u, False)

        def ag3(u):
            ag_all(u, 3).wait_recv()
            ag_all(u, 3).wait_send()
            local_wait(u)
            ag_start(u, 2)

        def last(u):
            rs_finish(u, 3)
            local_start(u)
            ag_start(u, 3)

        def middle(t):
            def fn(u):
                rs_finish(u, t)
                rs_start(u, t + 1)
            return fn

        guarded(0, dw_tile)

        from_a, to_a = [n_early - 1 + jnp.where(k > 2, k - 1, 0) for k in (i, i + 1)]

        @pl.when(jnp.logical_and(i % 3 == 0, jnp.logical_and(i >= 3, i < first_out)))
        def _():
            first_seq(i // 3 + 1).start()

        @pl.when(i < first_out)
        def _():
            pl.loop(from_a, jnp.minimum(to_a, n_attn))(attn_step)

        for lag, fn in enumerate((middle(0), middle(1), middle(2), last, ag3, ag2, ag1, ag0)):
            guarded(lag + 1, fn)

        @pl.when(i == first_out)
        def _():
            attn_out_wait(n_attn - 2)
            attn_out_wait(n_attn - 1)
            for x in o_load(1):
                x.start()
            tile_start(per)

        def blocks(i):
            k = i - first_out
            return jnp.where(k <= seqs, jnp.maximum(3 * k - 1, 1), jnp.minimum(k + 2 * seqs, n_blocks))

        @pl.when(i >= first_out)
        def _():
            pl.loop(blocks(i), blocks(i + 1))(run_block)

        @pl.when(i == 3)
        def _():
            last_copy().wait()

        first_dh = first_dn + seqs

        @pl.when(i == first_dh)
        def _():
            pltpu.make_async_copy(dh_v, dh_hbm.at[:, 0], dh_sem.at[2]).wait()
            for j in range(1, group):
                remote(dg_all.at[me], dg_all.at[me], dg_send, dg_recv, flipped(me, j)).start()

        @pl.when(jnp.logical_and(i >= first_dh, i < first_dh + 4 * (seqs - by_xla)))
        def _():
            dh_send(i - first_dh)

        pl.when(i == n_all + 4)(settle)
        return carry

    lax.fori_loop(0, n_all + 8, step, 0)

    for q in range(4 * (seqs - by_xla)):
        dh_wait(q)
    for j in range(NS):
        u = n_all - NS + j
        for t in range(4):
            pl.semaphore_wait(credit.at[t, u % NS], 1 if t == 0 else 3)
            if t < 3:
                ag_all(u, t).wait_send()


BY_XLA = 2


def main_call(hidden, d_out, cos_tab, sin_tab, w_qkv, w_out, gain):
    n, loc, dim = hidden.shape
    group = 16
    rows = n * loc
    seqs = n // group
    seq = loc * group
    h = dim // 2
    n_all = 4 * dim // TW
    hbm = pl.BlockSpec(memory_space=pl.ANY)
    vmem = pl.BlockSpec(memory_space=pltpu.VMEM)
    D = pltpu.SemaphoreType.DMA
    S = jax.ShapeDtypeStruct
    V = pltpu.VMEM
    act = S((rows, dim), BF)
    return pl.pallas_call(
        functools.partial(main_kernel, 128 ** -0.5),
        in_specs=[hbm] * 2 + [vmem] * 2 + [hbm] * 2 + [vmem],
        out_specs=[hbm] * 11 + [vmem],
        out_shape=[S((dim, 4 * dim), F32), act, act, S((3, rows, dim), BF),
                   act, S((dim, rows), BF), S((3, rows, dim), BF), S((n, loc, dim), BF),
                   S((group, BY_XLA, loc, dim), BF), S((group, seqs - BY_XLA, loc, dim), BF), S((group, seqs - BY_XLA, loc, dim), BF), S((dim,), F32)],
        scratch_shapes=[
            V((dim, rows), BF), V((2, 3, rows, TW), BF), V((NB, dim, TW), F32),
            V((NS, h, TW), F32), V((NS, h >> 1, TW), F32), V((NS, h >> 2, TW), F32), V((NS, h >> 3, TW), F32),
            V((2, 3, seq, TW), BF), V((2, seq, TW), BF), V((2, seq, TW), BF), V((2, TW, seq), BF), V((seq, 256), F32), V((loc, 128), F32), V((seq, 128), F32),
            V((seq, dim), F32), V((seq, dim), BF), V((seq, dim), BF), V((group, loc, dim), BF), V((group, 1, dim), F32),
            V((2, dim, 512), BF), V((2, seq, 512), BF), V((2, seq // 2, dim), BF), V((dim // 512, group, loc, 512), BF),
            D, D, D((4, NS)), D((4, NS)), pltpu.SemaphoreType.REGULAR((4, NS)), D((NS,)), D((4, NS)), D((4, n_all)),
            D((2, 2)), D((3, 2)), D((3,)), D((3,)), D, D, D((2, 2)), D((2,)), D((2,)),
            D((seqs,)), D((seqs,)), D((seqs,)), D((seqs,)), D, D, D((2 * seqs,)), D((dim // 512,)), D((seqs,)), D((dim // 512,)), D((4 * (seqs - BY_XLA),)), D((4 * (seqs - BY_XLA),)),
        ],
        compiler_params=pltpu.CompilerParams(collective_id=0, has_side_effects=True, vmem_limit_bytes=67043328),
        cost_estimate=pl.CostEstimate(flops=28 * rows * dim * dim, bytes_accessed=90 * dim * dim, transcendentals=0),
        name="main",
    )(hidden, d_out, cos_tab, sin_tab, w_qkv, w_out, gain)


def place_kernel(y_in, b_in, y_out, dh_out):
    y_out[...] = y_in[...]
    dh_out[...] = b_in[...]


def place_call(y, b):
    n, loc, dim = y.shape
    group, k = b.shape[:2]
    seqs = n // group
    return pl.pallas_call(
        place_kernel,
        grid=(2,),
        in_specs=[pl.BlockSpec((n // 2, loc, dim), lambda j: (j, 0, 0)), pl.BlockSpec((group // 2, k, loc, dim), lambda j: (j, 0, 0, 0))],
        out_specs=[pl.BlockSpec((n // 2, loc, dim), lambda j: (j, 0, 0)), pl.BlockSpec((group // 2, k, loc, dim), lambda j: (j, seqs // k - 1, 0, 0))],
        out_shape=[jax.ShapeDtypeStruct((n, loc, dim), BF), jax.ShapeDtypeStruct((group, seqs, loc, dim), BF)],
        cost_estimate=pl.CostEstimate(flops=8 * n * loc * dim, bytes_accessed=6 * n * loc * dim, transcendentals=0),
        name="place",
    )(y, b)


def fill_kernel(a_in, dh_in, dh_out):
    dh_out[...] = a_in[...]


def fill_call(a, dh):
    group, k, loc, dim = a.shape
    return pl.pallas_call(
        fill_kernel,
        grid=(2,),
        in_specs=[pl.BlockSpec((group // 2, k, loc, dim), lambda j: (j, 0, 0, 0)), pl.BlockSpec(memory_space=pl.ANY)],
        out_specs=pl.BlockSpec((group // 2, k, loc, dim), lambda j: (j, 0, 0, 0)),
        out_shape=jax.ShapeDtypeStruct(dh.shape, BF),
        input_output_aliases={1: 0},
        name="fill",
    )(a, dh)


def solution(mesh):
    group = mesh.shape['sp']
    token_spec = P(None, 'sp', None)
    table_spec = P('sp', None)

    def device_step(hidden, norm_gain, w_qkv, w_out, cos_tab, sin_tab, d_out):
        num_seqs, local_len, dim = hidden.shape
        dw, _, _, _, _, _, _, y, dh_a, _, dh_b, dgain = main_call(hidden, d_out, cos_tab, sin_tab, w_qkv, w_out, norm_gain)
        dh_a = lax.all_to_all(dh_a, 'sp', split_axis=0, concat_axis=0, tiled=True)
        y, dh = place_call(y, dh_b)
        dh = fill_call(dh_a, dh).reshape(num_seqs, local_len, dim)
        return y, dh, dw[:, :3 * dim], dw[:, 3 * dim:], dgain

    return jax.shard_map(device_step, mesh=mesh, in_specs=(token_spec, P(), P(), P(), table_spec, table_spec, token_spec), out_specs=(token_spec, token_spec, P(), P(), P()), check_vma=False)
```
